32 devices in a mesh: gx: 16 (over z, y, x), gz: 2 (over core).
Axes of the slice: x: 2, y: 2, z: 4, core: 2. Of those that a mesh axis runs over, the one named last changes fastest.
Arguments:
- velocity: float32 [3, 256, 16, 256], P(None, 'gx', 'gz'), may hold values from -6 to 6
- pressure: float32 [256, 16, 256], P('gx', 'gz'), may hold values from 1 to 3
- stress_old: float32 [6, 256, 16, 256], P(None, 'gx', 'gz'), may hold values from -6 to 6
- plastic: float32 [256, 16, 256], P('gx', 'gz'), may hold values from 0 to 2
- viscosity: float32 [256, 16, 256], P('gx', 'gz'), may hold values from 1 to 30
- weak_seed: int32 [256, 16, 256], P('gx', 'gz'), may hold values 0 or 1
Outputs:
- velocity_out: float32 [3, 256, 16, 256], P(None, 'gx', 'gz')
- pressure_out: float32 [256, 16, 256], P('gx', 'gz')
- stress_out: float32 [6, 256, 16, 256], P(None, 'gx', 'gz')
- plastic_out: float32 [256, 16, 256], P('gx', 'gz')
- yield_peak: float32 [2], replicated
The draws below stay inside these ranges and needn't reach their ends.
All inputs are finite; a program needn't handle non-finite values. No bound on the sum of `weak_seed` on one device may be relied on, other than what follows from the above.
Results may differ from the reference program's by a relative error of at most 0.000059.
Values sent between devices are 32-bit elements; how exact they have to be, the bound alone decides.
A program may use at most 64 MiB of HBM per device.

```python
import math
import jax
import jax.numpy as jnp
from jax import lax

NY = 256
ITERS = 2
NX = 256
NZ = 16


def draw_viscosity(key, part):
    xpos = jnp.arange(NX, dtype=jnp.float32) / max(NX - 1, 1)
    ramp = jnp.exp(jnp.log(10.0) * xpos)[:, None, None]
    rough = jnp.exp(jax.random.uniform(key, (NX, NZ, NY), jnp.float32, 0.0, jnp.log(3.0)))
    return (ramp * rough).astype(jnp.float32)


def touch_ends(array, rng, least, largest):
    longest = array.shape.index(max(array.shape))
    spots = []
    for shift in (0, 1):
        where = [jax.random.randint(jax.random.fold_in(rng, axis), (), 0, length) for axis, length in enumerate(array.shape)]
        where[longest] = (where[longest] + shift) % array.shape[longest]
        spots.append(tuple(where))
    return array.at[spots[0]].set(least).at[spots[1]].set(largest)


def level_of(own_key, extent, cuts, smallest, high):
    factor_of, own = 1.0, jax.random.fold_in(own_key, 6)
    for position, shards_of in cuts:
        draws = jnp.exp(jax.random.uniform(jax.random.fold_in(own, position), (shards_of,), jnp.float32, smallest / len(cuts), high / len(cuts)))
        factor_of = factor_of * jnp.repeat(draws, extent[position] // shards_of).reshape([-1 if axis == position else 1 for axis in range(len(extent))])
    return factor_of


def bell_draw(own_key, extent, deviation, limit, cuts=(), held_as=jnp.bfloat16):
    result = deviation * jax.random.normal(own_key, extent, jnp.float32)
    if cuts:
        result = result * level_of(own_key, extent, cuts, -0.22, 0.18)
    return jnp.clip(result, -limit, limit).astype(held_as)


def setup_inputs(seed: int = 0) -> dict:
    key_of = jax.random.split(jax.random.key(seed), 7)
    velocity = bell_draw(key_of[0], (3, NX, NZ, NY), 1.0, 6.0, ((1, 16), (2, 2)), jnp.float32)
    pressure = jnp.clip(1.0 + 2.0 * jax.random.uniform(key_of[1], (NX, NZ, NY), jnp.float32) ** level_of(key_of[1], (NX, NZ, NY), ((0, 16), (1, 2)), -0.2, 0.2), 1.0, 3.0)
    stress_old = bell_draw(key_of[2], (6, NX, NZ, NY), 1.0, 6.0, ((1, 16), (2, 2)), jnp.float32)
    plastic = jnp.clip(2.0 * jax.random.uniform(key_of[3], (NX, NZ, NY), jnp.float32) ** level_of(key_of[3], (NX, NZ, NY), ((0, 16), (1, 2)), -0.2, 0.2), 0.0, 2.0)
    viscosity = draw_viscosity(jax.random.fold_in(key_of[6], 71), 0)
    weak_seed = touch_ends((jax.random.randint(key_of[5], (NX, NZ, NY), 0, 8) < 1).astype(jnp.int32), jax.random.fold_in(key_of[5], 1), 0, 1)
    return {"velocity": velocity, "pressure": pressure, "stress_old": stress_old, "plastic": plastic, "viscosity": viscosity, "weak_seed": weak_seed}


unnormalized_weights = [math.exp(-(k * k) / 18.0) for k in range(-6, 7)]
weight_total = sum(unnormalized_weights)
gauss_weights = [value / weight_total for value in unnormalized_weights]
shear_time_increment = 20.0

def smooth_axis(field, axis):
    count = field.shape[axis]
    widths = [(0, 0)] * field.ndim
    widths[axis] = (6, 6)
    padded = jnp.pad(field, widths)
    total = gauss_weights[0] * lax.slice_in_dim(padded, 0, count, axis=axis)
    for index in range(1, 13):
        total = total + gauss_weights[index] * lax.slice_in_dim(padded, index, index + count, axis=axis)
    return total

def y_matrix(length):
    places = jnp.arange(length)
    gap = (places[:, None] - places[None, :]).astype(jnp.float32)
    return jnp.where(jnp.abs(gap) <= 6.0, jnp.exp(-gap * gap / 18.0) / weight_total, 0.0).astype(jnp.float32)

def smooth_y(field):
    length = field.shape[-1]
    flat = field.reshape(-1, length)
    return jnp.dot(flat, y_matrix(length), precision=lax.Precision.HIGHEST).reshape(field.shape)

def diff_axis(field, axis):
    count = field.shape[axis]
    widths = [(0, 0)] * field.ndim
    widths[axis] = (1, 1)
    padded = jnp.pad(field, widths)
    return (lax.slice_in_dim(padded, 2, count + 2, axis=axis) - lax.slice_in_dim(padded, 0, count, axis=axis)) * 0.5

def return_map(velocity_x_spacing, velocity_z_spacing, dyv, stress_old, eta_ve, pres, cohesion_strength):
    divv = velocity_x_spacing[0] + velocity_z_spacing[1] + dyv[2]
    pres = pres - 0.25 * divv
    strain = jnp.stack([velocity_x_spacing[0] - divv / 3.0, velocity_z_spacing[1] - divv / 3.0, dyv[2] - divv / 3.0, 0.5 * (velocity_x_spacing[1] + velocity_z_spacing[0]), 0.5 * (velocity_x_spacing[2] + dyv[0]), 0.5 * (velocity_z_spacing[2] + dyv[1])])
    trial = 2.0 * eta_ve * (strain + stress_old / (2.0 * shear_time_increment))
    tau_ii = jnp.sqrt(0.5 * (trial[0] ** 2 + trial[1] ** 2 + trial[2] ** 2) + trial[3] ** 2 + trial[4] ** 2 + trial[5] ** 2)
    yield_f = tau_ii - 0.5 * jnp.maximum(pres, 0.0) - 0.8660254 * cohesion_strength
    dlam = jnp.maximum(yield_f, 0.0) / (eta_ve + 0.5)
    shrink = 1.0 - eta_ve * dlam / jnp.maximum(tau_ii, 0.5)
    return (pres, trial * shrink, shrink, yield_f, dlam)

def reference(velocity, pressure, stress_old, plastic, viscosity, weak_seed):
    smoothed = smooth_y(smooth_axis(smooth_axis(plastic, 0), 1))
    eta_ve = 1.0 / (1.0 / viscosity + 1.0 / shear_time_increment)
    seeded = weak_seed.astype(jnp.float32)
    cohesion_strength = (1.0 - 0.6 * seeded) / (1.0 + 2.0 * smoothed)
    pres = pressure
    plastic_sum = plastic
    peaks = []
    tau = stress_old
    for step_index in range(ITERS):
        velocity_x_spacing = diff_axis(velocity, 1)
        velocity_z_spacing = diff_axis(velocity, 2)
        dyv = diff_axis(velocity, 3)
        pres, tau, shrink, yield_f, dlam = return_map(velocity_x_spacing, velocity_z_spacing, dyv, stress_old, eta_ve, pres, cohesion_strength)
        plastic_sum = plastic_sum + dlam
        peaks.append(jnp.max(yield_f))
        step = 0.125 / jnp.max(eta_ve * shrink)
        sxx = tau[0] - pres
        szz = tau[1] - pres
        syy = tau[2] - pres
        rx = diff_axis(sxx, 0) + diff_axis(tau[3], 1) + diff_axis(tau[4], 2)
        rz = diff_axis(tau[3], 0) + diff_axis(szz, 1) + diff_axis(tau[5], 2)
        ry = diff_axis(tau[4], 0) + diff_axis(tau[5], 1) + diff_axis(syy, 2)
        velocity = velocity + step * jnp.stack([rx, rz, ry])
    return (velocity, pres, tau, plastic_sum, jnp.stack(peaks))
```

```python
import functools
import math

import jax
import jax.numpy as jnp
from jax import lax
from jax.experimental import pallas as pl
from jax.experimental.pallas import tpu as pltpu
from jax.sharding import PartitionSpec as P

ITERS = 2
REACH = 6
BLOCK = 8
UNROLL = 1
MESH = pl.DeviceIdType.MESH

unnormalized_weights = [math.exp(-(k * k) / 18.0) for k in range(-REACH, REACH + 1)]
weight_total = sum(unnormalized_weights)
gauss_weights = [value / weight_total for value in unnormalized_weights]
shear_time_increment = 20.0


def kernel(
    gx_count,
    gz_count,
    vel_in,
    pres_in,
    old_in,
    plas_in,
    visc_in,
    weak_in,
    VOUT,
    PR,
    TAU,
    PL,
    peak_out,
    V,
    PIN,
    OLD,
    PLX,
    VI,
    WK,
    ETA,
    COH,
    YM,
    GX,
    GZH,
    SM,
    VZE,
    VZH,
    SX,
    TZ,
    SZE,
    SZH,
    RP,
    RH,
    R,
    RZE,
    RZH,
    TB,
    PK,
    in_sem,
    send_sem,
    recv_sem,
    pk_send,
    pk_recv,
):
    rows, nz, ny = PR.shape
    gx = lax.axis_index("gx")
    gz = lax.axis_index("gz")
    me = gx * gz_count + gz
    total = gx_count * gz_count
    has = {
        "xl": gx > 0,
        "xh": gx < gx_count - 1,
        "zl": gz > 0,
        "zh": gz < gz_count - 1,
    }
    target = {
        "xl": (gx - 1, gz),
        "xh": (gx + 1, gz),
        "zl": (gx, gz - 1),
        "zh": (gx, gz + 1),
    }
    opposite = {"xl": "xh", "xh": "xl", "zl": "zh", "zh": "zl"}

    barrier = pltpu.get_barrier_semaphore()

    def to_others(act):
        for dz_ in range(gz_count):
            other_z = gz + dz_
            other_z = jnp.where(other_z >= gz_count, other_z - gz_count, other_z)

            def body(dx_, carry):
                other_x = gx + dx_
                act((jnp.where(other_x >= gx_count, other_x - gx_count, other_x), other_z))
                return carry

            lax.fori_loop(0 if dz_ else 1, gx_count, body, 0, unroll=UNROLL)

    loads = [
        pltpu.make_async_copy(plas_in, PLX.at[pl.ds(REACH, rows)], in_sem.at[0]),
        pltpu.make_async_copy(vel_in, V.at[:, pl.ds(1, rows)], in_sem.at[1]),
        pltpu.make_async_copy(visc_in, VI, in_sem.at[2]),
        pltpu.make_async_copy(weak_in, WK, in_sem.at[3]),
        pltpu.make_async_copy(old_in, OLD, in_sem.at[4]),
        pltpu.make_async_copy(pres_in, PIN, in_sem.at[5]),
    ]
    for copy in loads[:2]:
        copy.start()
    to_others(
        lambda place: pl.semaphore_signal(
            barrier, inc=1, device_id=place, device_id_type=MESH
        )
    )
    for copy in loads[2:]:
        copy.start()

    count = [0]

    def exchange(side, source, landing):
        slot = count[0]
        count[0] += 1
        copy = pltpu.make_async_remote_copy(
            src_ref=source,
            dst_ref=landing,
            send_sem=send_sem.at[slot],
            recv_sem=recv_sem.at[slot],
            device_id=target[side],
            device_id_type=MESH,
        )

        @pl.when(has[side])
        def _():
            copy.start()

        return side, copy

    def wait_sent(pair):
        side, copy = pair

        @pl.when(has[side])
        def _():
            copy.wait_send()

    def wait_got(pair):
        side, copy = pair

        @pl.when(has[opposite[side]])
        def _():
            copy.wait_recv()

    def zero_unless(side, ref):
        @pl.when(jnp.logical_not(has[side]))
        def _():
            ref[...] = jnp.zeros(ref.shape, ref.dtype)

    zero_unless("xl", PLX.at[pl.ds(0, REACH)])
    zero_unless("xh", PLX.at[pl.ds(rows + REACH, REACH)])
    zero_unless("xl", V.at[:, pl.ds(0, 1)])
    zero_unless("xh", V.at[:, pl.ds(rows + 1, 1)])
    zero_unless("zl", GZH.at[0])
    zero_unless("zh", GZH.at[1])
    for buf in (VZH.at[0], RZH.at[0], SZH.at[0, 0], SZH.at[1, 0]):
        zero_unless("zl", buf)
    for buf in (VZH.at[1], RZH.at[1], SZH.at[0, 1], SZH.at[1, 1]):
        zero_unless("zh", buf)
    for it in range(ITERS):
        zero_unless("xl", SX.at[it, :, pl.ds(0, 1)])
        zero_unless("xh", SX.at[it, :, pl.ds(rows + 1, 1)])

    loads[0].wait()
    loads[1].wait()

    def vel_edges(x, carry):
        for c in range(3):
            row = V[c, x + 1]
            VZE[0, c, x] = row[0:1]
            VZE[1, c, x] = row[nz - 1 : nz]
        return carry

    lax.fori_loop(0, rows, vel_edges, 0)
    pl.semaphore_wait(barrier, total - 1)
    plas_copies = [
        exchange("xh", PLX.at[pl.ds(rows, REACH)], PLX.at[pl.ds(0, REACH)]),
        exchange("xl", PLX.at[pl.ds(REACH, REACH)], PLX.at[pl.ds(rows + REACH, REACH)]),
    ]
    vel_copies = [
        exchange("xh", V.at[:, pl.ds(rows, 1)], V.at[:, pl.ds(0, 1)]),
        exchange("xl", V.at[:, pl.ds(1, 1)], V.at[:, pl.ds(rows + 1, 1)]),
    ]

    vz_copies = [
        exchange("zh", VZE.at[1], VZH.at[0]),
        exchange("zl", VZE.at[0], VZH.at[1]),
    ]

    places_a = lax.broadcasted_iota(jnp.int32, (ny, ny), 0)
    places_b = lax.broadcasted_iota(jnp.int32, (ny, ny), 1)
    gap = (places_a - places_b).astype(jnp.float32)
    YM[...] = jnp.where(
        jnp.abs(gap) <= float(REACH), jnp.exp(-gap * gap / 18.0) / weight_total, 0.0
    )
    for copy in loads[2:]:
        copy.wait()

    def prepare(x, carry):
        eta = VI[x]
        ETA[x] = shear_time_increment * eta / (eta + shear_time_increment)
        return carry

    lax.fori_loop(0, rows, prepare, 0)

    block = next(size for size in (BLOCK, 4, 2, 1) if rows % size == 0)
    many = (block, nz, ny)
    sub = lax.broadcasted_iota(jnp.int32, many, 1)
    lane = lax.broadcasted_iota(jnp.int32, many, 2)

    def over_rows(body, carry=0):
        return lax.fori_loop(0, rows // block, lambda i, state: body(i * block, state), carry)

    def at(x):
        return pl.ds(x, block)

    for pair in plas_copies:
        wait_got(pair)

    def smooth_x(x, carry):
        sum_ = gauss_weights[REACH] * PLX[at(x + REACH)]
        for k in range(1, REACH + 1):
            sum_ = sum_ + gauss_weights[REACH + k] * (PLX[at(x + REACH - k)] + PLX[at(x + REACH + k)])
        GX[at(x)] = sum_
        return carry

    over_rows(smooth_x)
    gz_copies = [
        exchange("zh", GX, GZH.at[0]),
        exchange("zl", GX, GZH.at[1]),
    ]
    for pair in vel_copies + vz_copies:
        wait_got(pair)

    def dy(f):
        up = jnp.where(lane < ny - 1, pltpu.roll(f, ny - 1, 2), 0.0)
        down = jnp.where(lane > 0, pltpu.roll(f, 1, 2), 0.0)
        return (up - down) * 0.5

    def dz(f, low, high):
        up = pltpu.roll(jnp.where(sub >= 1, f, jnp.broadcast_to(high, f.shape)), nz - 1, 1)
        down = pltpu.roll(jnp.where(sub < nz - 1, f, jnp.broadcast_to(low, f.shape)), 1, 1)
        return (up - down) * 0.5

    def trial_stress(x, pres):
        v = [V[c, at(x + 1)] for c in range(3)]
        dx_v = [(V[c, at(x + 2)] - V[c, at(x)]) * 0.5 for c in range(3)]
        dz_v = [dz(f, VZH[0, c, at(x)], VZH[1, c, at(x)]) for c, f in enumerate(v)]
        dy_v = [dy(f) for f in v]
        div = dx_v[0] + dz_v[1] + dy_v[2]
        third = div * (1.0 / 3.0)
        pres = pres - 0.25 * div
        PR[at(x)] = pres
        strain = (
            dx_v[0] - third,
            dz_v[1] - third,
            dy_v[2] - third,
            0.5 * (dx_v[1] + dz_v[0]),
            0.5 * (dx_v[2] + dy_v[0]),
            0.5 * (dz_v[2] + dy_v[1]),
        )
        twice = 2.0 * ETA[at(x)]
        trial = [
            twice * (strain[c] + OLD[c, at(x)] * (0.5 / shear_time_increment)) for c in range(6)
        ]
        tau_ii = jnp.sqrt(
            0.5 * (trial[0] * trial[0] + trial[1] * trial[1] + trial[2] * trial[2])
            + trial[3] * trial[3]
            + trial[4] * trial[4]
            + trial[5] * trial[5]
        )
        return pres, trial, tau_ii

    def first_trial(x, carry):
        _, trial, tau_ii = trial_stress(x, PIN[at(x)])
        for c in range(6):
            TAU[c, at(x)] = trial[c]
        TB[at(x)] = tau_ii
        return carry

    over_rows(first_trial)

    for pair in gz_copies:
        wait_got(pair)

    def smooth_z(x, carry):
        own, low, high = GX[at(x)], GZH[0, at(x)], GZH[1, at(x)]
        sum_ = gauss_weights[REACH] * own
        for k in range(1, REACH + 1):
            above = pltpu.roll(jnp.where(sub >= k, own, high), nz - k, 1)
            below = pltpu.roll(jnp.where(sub < nz - k, own, low), k, 1)
            sum_ = sum_ + gauss_weights[REACH + k] * (above + below)
        SM[at(x)] = sum_
        return carry

    over_rows(smooth_z)
    SM[...] = jnp.dot(
        SM[...].reshape(rows * nz, ny),
        YM[...],
        precision=lax.Precision.HIGHEST,
        preferred_element_type=jnp.float32,
    ).reshape(rows, nz, ny)

    half = ny // 2 if ny % 256 == 0 else ny
    tops = []
    for it in range(ITERS):
        last = it == ITERS - 1

        def stress_row(x, carry, it=it, last=last):
            most_f, most_eta = carry
            if it == 0:
                pres, trial, tau_ii = PR[at(x)], [TAU[c, at(x)] for c in range(6)], TB[at(x)]
                seeded = WK[at(x)].astype(jnp.float32)
                strength = 0.8660254 * ((1.0 - 0.6 * seeded) / (1.0 + 2.0 * SM[at(x)]))
                COH[at(x)] = strength
                plas = PLX[at(x + REACH)]
            else:
                pres, trial, tau_ii = trial_stress(x, PR[at(x)])
                strength = COH[at(x)]
                plas = PL[at(x)]
            eta = ETA[at(x)]
            yield_f = tau_ii - 0.5 * jnp.maximum(pres, 0.0) - strength
            dlam = jnp.maximum(yield_f, 0.0) / (eta + 0.5)
            shrink = 1.0 - eta * dlam / jnp.maximum(tau_ii, 0.5)
            tau = [shrink * value for value in trial]
            PL[at(x)] = plas + dlam
            if last:
                for c in range(6):
                    TAU[c, at(x)] = tau[c]
            SX[it, 0, at(x + 1)] = tau[0] - pres
            SX[it, 1, at(x + 1)] = tau[3]
            SX[it, 2, at(x + 1)] = tau[4]
            szz = tau[1] - pres
            TZ[0, at(x)] = szz
            TZ[1, at(x)] = tau[5]
            TZ[2, at(x)] = tau[2] - pres
            for c, f in enumerate((tau[3], szz, tau[5])):
                SZE[it, 0, c, at(x)] = f[:, 0:1]
                SZE[it, 1, c, at(x)] = f[:, nz - 1 : nz]
            return jnp.maximum(most_f, yield_f), jnp.maximum(most_eta, eta * shrink)

        start = jnp.full(many, -jnp.inf, jnp.float32)
        most_f, most_eta = over_rows(stress_row, (start, start))
        sx_copies = [
            exchange("xh", SX.at[it, :, pl.ds(rows, 1)], SX.at[it, :, pl.ds(0, 1)]),
            exchange("xl", SX.at[it, :, pl.ds(1, 1)], SX.at[it, :, pl.ds(rows + 1, 1)]),
        ]
        sz_copies = [
            exchange("zh", SZE.at[it, 1], SZH.at[it, 0]),
            exchange("zl", SZE.at[it, 0], SZH.at[it, 1]),
        ]

        def folded(most):
            most = jnp.max(jnp.max(most, axis=0), axis=0, keepdims=True)
            return jnp.maximum(most[:, :half], most[:, ny - half :])

        PK[it, me] = jnp.concatenate([folded(most_f), folded(most_eta)], axis=0)

        def tell(place, it=it):
            pltpu.make_async_remote_copy(
                src_ref=PK.at[it, me],
                dst_ref=PK.at[it, me],
                send_sem=pk_send.at[it],
                recv_sem=pk_recv.at[it],
                device_id=place,
                device_id_type=MESH,
            ).start()

        to_others(tell)
        for pair in sz_copies:
            wait_got(pair)

        def inner_row(x, carry, it=it):
            txz, txy = SX[it, 1, at(x + 1)], SX[it, 2, at(x + 1)]
            szz, tzy, syy = TZ[0, at(x)], TZ[1, at(x)], TZ[2, at(x)]
            z_terms = [
                dz(f, SZH[it, 0, c, at(x)], SZH[it, 1, c, at(x)])
                for c, f in enumerate((txz, szz, tzy))
            ]
            y_terms = [dy(f) for f in (txy, tzy, syy)]
            for c in range(3):
                R[c, at(x)] = z_terms[c] + y_terms[c]
            return carry

        def add_x(low, high, it=it):
            for c in range(3):
                R[c, low:high] = R[c, low:high] + 0.5 * (
                    SX[it, c, low + 2 : high + 2] - SX[it, c, low:high]
                )

        r_copies = []
        if not last:
            inner_row(0, 0)
            inner_row(rows - block, 0)
            for c in range(3):
                RP[0, c] = R[c, 0] + 0.5 * SX[it, c, 2]
                RP[1, c] = R[c, rows - 1] - 0.5 * SX[it, c, rows - 1]
            r_copies += [
                exchange("xh", RP.at[1], RH.at[0]),
                exchange("xl", RP.at[0], RH.at[1]),
            ]
        over_rows(inner_row)
        add_x(1, rows - 1)
        for pair in sx_copies:
            wait_got(pair)
        add_x(0, 1)
        add_x(rows - 1, rows)
        if not last:

            def edges(x, carry):
                for c in range(3):
                    value = R[c, at(x)]
                    RZE[0, c, at(x)] = value[:, 0:1]
                    RZE[1, c, at(x)] = value[:, nz - 1 : nz]
                return carry

            over_rows(edges)
            r_copies += [
                exchange("zh", RZE.at[1], RZH.at[0]),
                exchange("zl", RZE.at[0], RZH.at[1]),
            ]
            for pair in vel_copies:
                wait_sent(pair)
            for pair in r_copies:
                wait_got(pair)

        others = PK.at[it, pl.ds(0, total - 1)]
        arrived = pltpu.make_async_copy(others, others, pk_recv.at[it])
        arrived.wait()
        peaks = jnp.max(PK[it], axis=0)
        step = 0.125 / jnp.max(peaks[1:2], axis=1, keepdims=True)

        def velocity_row(x, carry):
            for c in range(3):
                value = V[c, at(x + 1)] + step * R[c, at(x)]
                if last:
                    VOUT[c, at(x)] = value
                else:
                    V[c, at(x + 1)] = value
            return carry

        over_rows(velocity_row)
        if not last:

            @pl.when(has["xl"])
            def _(it=it, step=step):
                for c in range(3):
                    V[c, 0] = V[c, 0] + step * (RH[0, c] + 0.5 * SX[it, c, 1])

            @pl.when(has["xh"])
            def _(it=it, step=step):
                for c in range(3):
                    V[c, rows + 1] = V[c, rows + 1] + step * (RH[1, c] - 0.5 * SX[it, c, rows])

            VZH[...] = VZH[...] + step * RZH[...]
        tops.append(jnp.max(peaks[0:1], axis=1, keepdims=True))
        for pair in sx_copies + sz_copies + r_copies:
            wait_sent(pair)
        pltpu.make_async_copy(others, others, pk_send.at[it]).wait()

    peak_out[...] = jnp.concatenate(tops, axis=1)[0]
    for pair in plas_copies + vz_copies + gz_copies:
        wait_sent(pair)


def store_kernel(*refs):
    held, out, sem = refs[:5], refs[5:10], refs[10]
    copies = [pltpu.make_async_copy(a, b, sem.at[i]) for i, (a, b) in enumerate(zip(held, out))]
    for copy in copies:
        copy.start()
    for copy in copies:
        copy.wait()


def solution(mesh):
    gx_count, gz_count = mesh.shape["gx"], mesh.shape["gz"]
    total = gx_count * gz_count

    def per_device(velocity, pressure, stress_old, plastic, viscosity, weak_seed):
        rows, nz, ny = pressure.shape
        cells = (rows, nz, ny)
        f32 = jnp.float32
        vm = lambda *shape: pltpu.VMEM(shape, f32)
        copies = 6 + 2 + 4 * ITERS + 4 * (ITERS - 1)
        anywhere = pl.BlockSpec(memory_space=pl.ANY)
        shapes = (velocity.shape, pressure.shape, stress_old.shape, plastic.shape)
        held = pl.pallas_call(
            functools.partial(kernel, gx_count, gz_count),
            out_shape=tuple(vm(*shape) for shape in shapes + ((ITERS,),)),
            in_specs=[anywhere] * 6,
            out_specs=(pl.BlockSpec(memory_space=pltpu.VMEM),) * 5,
            scratch_shapes=[
                vm(3, rows + 2, nz, ny),
                vm(*cells),
                vm(6, *cells),
                vm(rows + 2 * REACH, nz, ny),
                vm(*cells),
                pltpu.VMEM(cells, jnp.int32),
                vm(*cells),
                vm(*cells),
                vm(ny, ny),
                vm(*cells),
                vm(2, *cells),
                vm(*cells),
                vm(2, 3, rows, 1, ny),
                vm(2, 3, rows, 1, ny),
                vm(ITERS, 3, rows + 2, nz, ny),
                vm(3, *cells),
                vm(ITERS, 2, 3, rows, 1, ny),
                vm(ITERS, 2, 3, rows, 1, ny),
                vm(2, 3, nz, ny),
                vm(2, 3, nz, ny),
                vm(3, *cells),
                vm(2, 3, rows, 1, ny),
                vm(2, 3, rows, 1, ny),
                vm(*cells),
                vm(ITERS, total, 2, ny // 2 if ny % 256 == 0 else ny),
                pltpu.SemaphoreType.DMA((6,)),
                pltpu.SemaphoreType.DMA((copies,)),
                pltpu.SemaphoreType.DMA((copies,)),
                pltpu.SemaphoreType.DMA((ITERS,)),
                pltpu.SemaphoreType.DMA((ITERS,)),
            ],
            compiler_params=pltpu.CompilerParams(collective_id=0, has_side_effects=True),
        )(velocity, pressure, stress_old, plastic, viscosity, weak_seed)
        held = [pltpu.with_memory_space_constraint(array, pltpu.VMEM) for array in held]
        return pl.pallas_call(
            store_kernel,
            out_shape=tuple(jax.ShapeDtypeStruct(shape, f32) for shape in shapes)
            + (jax.ShapeDtypeStruct((ITERS,), f32),),
            in_specs=[anywhere] * 5,
            out_specs=(anywhere,) * 5,
            scratch_shapes=[pltpu.SemaphoreType.DMA((5,))],
        )(*held)

    in_specs = (
        P(None, "gx", "gz", None),
        P("gx", "gz", None),
        P(None, "gx", "gz", None),
        P("gx", "gz", None),
        P("gx", "gz", None),
        P("gx", "gz", None),
    )
    out_specs = (
        P(None, "gx", "gz", None),
        P("gx", "gz", None),
        P(None, "gx", "gz", None),
        P("gx", "gz", None),
        P(),
    )
    return jax.shard_map(
        per_device, mesh=mesh, in_specs=in_specs, out_specs=out_specs, check_vma=False
    )
```

```python
import functools
import math

import jax
import jax.numpy as jnp
from jax import lax
from jax.experimental import pallas as pl
from jax.experimental.pallas import tpu as pltpu
from jax.sharding import PartitionSpec as P

ITERS = 2
REACH = 6
BLOCK = 8
PLANE = 4
MESH = pl.DeviceIdType.MESH

unnormalized_weights = [math.exp(-(k * k) / 18.0) for k in range(-REACH, REACH + 1)]
weight_total = sum(unnormalized_weights)
gauss_weights = [value / weight_total for value in unnormalized_weights]
shear_time_increment = 20.0


def bits_of(count):
    assert count & (count - 1) == 0
    return [1 << bit for bit in range(count.bit_length() - 1)]


def kernel(
    gx_count,
    gz_count,
    vel_in,
    pres_in,
    old_in,
    plas_in,
    visc_in,
    weak_in,
    VOUT,
    PR,
    TAU,
    PL,
    peak_out,
    V,
    IN,
    WK,
    PLZ,
    PZH,
    ETA,
    INV,
    COH,
    YM,
    GX,
    GXH,
    SM,
    VZE,
    VZH,
    SX,
    TZ,
    SE,
    ZH,
    XS,
    XH,
    CE,
    CH,
    SEL,
    ZHL,
    XHL,
    RF,
    RZF,
    TR,
    DV,
    TB,
    PK,
    in_sem,
    send_sem,
    recv_sem,
    pk_send,
    pk_recv,
    pair_sem,
    hop_sem,
):
    rows, nz, ny = PR.shape
    gx = lax.axis_index("gx")
    gz = lax.axis_index("gz")
    me = gx * gz_count + gz
    total = gx_count * gz_count
    has = {
        "xl": gx > 0,
        "xh": gx < gx_count - 1,
        "zl": gz > 0,
        "zh": gz < gz_count - 1,
    }
    target = {
        "xl": (gx - 1, gz),
        "xh": (gx + 1, gz),
        "zl": (gx, gz - 1),
        "zh": (gx, gz + 1),
    }
    opposite = {"xl": "xh", "xh": "xl", "zl": "zh", "zh": "zl"}
    corners = [(a, b) for a in ("xl", "xh") for b in ("zl", "zh")]
    for a, b in corners:
        has[a + b] = jnp.logical_and(has[a], has[b])
        target[a + b] = (target[a][0], target[b][1])
        opposite[a + b] = opposite[a] + opposite[b]
    barrier = pltpu.get_barrier_semaphore()

    side_of = gz % 2
    odd = side_of == 1
    even = side_of == 0
    lead = gz + 1 - side_of
    couple = gz // 2

    def flipped(index, bit):
        return index + bit * (1 - 2 * ((index // bit) % 2))

    always = gx >= 0
    rounds = [[(flipped(gx, bit), gz, always)] for bit in bits_of(min(PLANE, gx_count))]
    rounds += [
        [(gx - far, gz, gx >= far), (gx + far, gz, gx < gx_count - far)]
        for far in bits_of(gx_count)
        if far >= PLANE
    ]
    rounds += [[(gx, 2 * flipped(couple, bit) + 1, always)] for bit in bits_of(gz_count // 2)]
    along_gx = len(bits_of(gx_count))
    met = [place for far in rounds[1:3] + rounds[max(along_gx, 3) :] for place in far]

    def signal(sem, place):
        pl.semaphore_signal(sem, inc=1, device_id=place, device_id_type=MESH)

    def one_if(flag):
        return jnp.where(flag, 1, 0)

    VI, PIN = IN.at[0], IN.at[1]
    plas_load = pltpu.make_async_copy(plas_in, PLZ, in_sem.at[0])
    vel_load = pltpu.make_async_copy(vel_in, V.at[:, pl.ds(1, rows)], in_sem.at[1])
    weak_load = pltpu.make_async_copy(weak_in, WK, in_sem.at[2])
    rest_loads = [
        pltpu.make_async_copy(visc_in, VI, in_sem.at[3]),
        pltpu.make_async_copy(pres_in, PIN, in_sem.at[3]),
        pltpu.make_async_copy(old_in, IN.at[pl.ds(2, 6)], in_sem.at[3]),
    ]
    all_rest = pltpu.make_async_copy(IN, IN, in_sem.at[3])

    @pl.when(odd)
    def _():
        signal(barrier, (gx, gz - 1))

        @pl.when(has["zh"])
        def _():
            signal(barrier, (gx, gz + 1))

    for side in ("xl", "xh"):

        @pl.when(has[side])
        def _(side=side):
            signal(barrier, (target[side][0], lead))

    plas_load.start()

    @pl.when(odd)
    def _():
        for x_place, z_place, there in met:

            @pl.when(there)
            def _(x_place=x_place, z_place=z_place):
                signal(barrier, (x_place, z_place))

    def described(side, source, landing, got, sent):
        number = {"xl": 0, "xh": 1, "zl": 0, "zh": 1}.get(side, 0)
        return pltpu.make_async_remote_copy(
            src_ref=source,
            dst_ref=landing,
            send_sem=send_sem.at[2 * sent + number],
            recv_sem=recv_sem.at[2 * got + number],
            device_id=target[side],
            device_id_type=MESH,
        )

    def start(pairs):
        for side, copy in pairs:

            @pl.when(has[side])
            def _(copy=copy):
                copy.start()

    def start_ordered(pairs):
        gx_odd = gx % 2 == 1

        @pl.when(gx_odd)
        def _():
            start([pair for pair in pairs if pair[0] == "xh"])
            start([pair for pair in pairs if pair[0] == "xl"])

        @pl.when(jnp.logical_not(gx_odd))
        def _():
            start([pair for pair in pairs if pair[0] == "xl"])
            start([pair for pair in pairs if pair[0] == "xh"])

    def wait_sent(pairs):
        for side, copy in pairs:

            @pl.when(has[side])
            def _(copy=copy):
                copy.wait_send()

    def wait_got(pairs):
        for side, copy in pairs:

            @pl.when(has[opposite[side]])
            def _(copy=copy):
                copy.wait_recv()

    def zero(ref):
        ref[...] = jnp.zeros(ref.shape, ref.dtype)

    def zero_unless(side, *refs):
        @pl.when(jnp.logical_not(has[side]))
        def _():
            for ref in refs:
                zero(ref)

    @pl.when(even)
    def _():
        pl.semaphore_wait(barrier, 1 + one_if(has["zl"]))
        signal(pair_sem, (gx, gz + 1))

        @pl.when(has["zl"])
        def _():
            signal(pair_sem, (gx, gz - 1))

    @pl.when(odd)
    def _():
        pl.semaphore_wait(pair_sem, 1 + one_if(has["zh"]))

    pz_copies = [
        ("zh", described("zh", plas_in, PZH.at[0], 0, 0)),
        ("zl", described("zl", plas_in, PZH.at[1], 0, 0)),
    ]
    start(pz_copies)
    vel_load.start()
    for copy in rest_loads:
        copy.start()
    weak_load.start()

    places_a = lax.broadcasted_iota(jnp.int32, (ny, ny), 0)
    places_b = lax.broadcasted_iota(jnp.int32, (ny, ny), 1)
    gap = (places_a - places_b).astype(jnp.float32)
    YM[...] = jnp.where(
        jnp.abs(gap) <= float(REACH), jnp.exp(-gap * gap / 18.0) / weight_total, 0.0
    )
    zero_unless("zl", PZH.at[0])
    zero_unless("zh", PZH.at[1])
    zero_unless("xl", V.at[:, pl.ds(0, 1)], GXH.at[0], XH.at[0], XHL.at[0], RF.at[:, pl.ds(0, 1)])
    zero_unless("xh", V.at[:, pl.ds(rows + 1, 1)], GXH.at[1], XH.at[1], XHL.at[1])
    zero_unless("xh", RF.at[:, pl.ds(rows + 1, 1)])
    zero_unless("zl", VZH.at[0], ZH.at[0], ZHL.at[0], RZF.at[0])
    zero_unless("zh", VZH.at[1], ZH.at[1], ZHL.at[1], RZF.at[1])
    for number, (a, b) in enumerate(corners):
        zero_unless(a + b, CH.at[number])
    for it in range(ITERS):
        zero(SX.at[it, :, pl.ds(0, 1)])
        zero(SX.at[it, :, pl.ds(rows + 1, 1)])

    @pl.when(odd)
    def _():
        greeters = 2 * (one_if(has["xl"]) + one_if(has["xh"]))
        for _, _, there in met:
            greeters = greeters + one_if(there)
        pl.semaphore_wait(barrier, greeters)
        signal(pair_sem, (gx, gz - 1))

    @pl.when(even)
    def _():
        pl.semaphore_wait(pair_sem, 1)

    vel_copies = [
        ("xh", described("xh", vel_in.at[:, pl.ds(rows - 1, 1)], V.at[:, pl.ds(0, 1)], 2, 2)),
        ("xl", described("xl", vel_in.at[:, pl.ds(0, 1)], V.at[:, pl.ds(rows + 1, 1)], 2, 2)),
    ]
    start_ordered(vel_copies)

    def hop_send(k):
        if k < len(rounds):

            @pl.when(odd)
            def _():
                for x_place, z_place, there in rounds[k]:

                    @pl.when(there)
                    def _(x_place=x_place, z_place=z_place):
                        signal(hop_sem.at[k], (x_place, z_place))

    def hop_wait(k):
        if k < len(rounds):

            @pl.when(odd)
            def _():
                expected = 0
                for _, _, there in rounds[k]:
                    expected = expected + one_if(there)
                pl.semaphore_wait(hop_sem.at[k], expected)

    hop_send(0)

    block = next(size for size in (BLOCK, 4, 2, 1) if rows % size == 0)
    many = (block, nz, ny)

    def over_rows(body, carry=0):
        return lax.fori_loop(0, rows // block, lambda i, state: body(i * block, state), carry)

    def at(x):
        return pl.ds(x, block)

    vel_load.wait()

    def vel_edges(x, carry):
        for c in range(3):
            row = V[c, at(x + 1)]
            VZE[0, c, at(x)] = row[:, 0:1]
            VZE[1, c, at(x)] = row[:, nz - 1 : nz]
        return carry

    over_rows(vel_edges)
    plas_load.wait()
    wait_got(pz_copies)
    vz_copies = [
        ("zh", described("zh", VZE.at[1], VZH.at[0], 1, 1)),
        ("zl", described("zl", VZE.at[0], VZH.at[1], 1, 1)),
    ]
    start(vz_copies)

    def smooth_z(x, carry):
        own, low, high = PLZ[at(x)], PZH[0, at(x)], PZH[1, at(x)]
        sub = lax.broadcasted_iota(jnp.int32, many, 1)
        sum_ = gauss_weights[REACH] * own
        for k in range(1, REACH + 1):
            above = pltpu.roll(jnp.where(sub >= k, own, high), nz - k, 1)
            below = pltpu.roll(jnp.where(sub < nz - k, own, low), k, 1)
            sum_ = sum_ + gauss_weights[REACH + k] * (above + below)
        SM[at(x)] = sum_
        return carry

    over_rows(smooth_z)
    GX[...] = jnp.dot(
        SM[...].reshape(rows * nz, ny),
        YM[...],
        precision=lax.Precision.HIGHEST,
        preferred_element_type=jnp.float32,
    ).reshape(rows, nz, ny)
    plas_copies = [
        ("xh", described("xh", GX.at[pl.ds(rows - REACH, REACH)], GXH.at[0], 3, 3)),
        ("xl", described("xl", GX.at[pl.ds(0, REACH)], GXH.at[1], 3, 3)),
    ]
    start_ordered(plas_copies)
    hop_wait(0)
    hop_send(1)

    all_rest.wait()
    weak_load.wait()

    def prepare(x, carry):
        eta = VI[at(x)]
        eta = shear_time_increment * eta / (eta + shear_time_increment)
        ETA[at(x)] = eta
        INV[at(x)] = 1.0 / (eta + 0.5)
        COH[at(x)] = 0.8660254 - (0.8660254 * 0.6) * WK[at(x)].astype(jnp.float32)
        return carry

    over_rows(prepare)
    for row in range(rows):
        sum_ = gauss_weights[REACH] * GX[row]
        for k in range(1, REACH + 1):
            for other in (row - k, row + k):
                if 0 <= other < rows:
                    sum_ = sum_ + gauss_weights[REACH + k] * GX[other]
        SM[row] = sum_
    for k in range(1, len(rounds) - 1):
        hop_wait(k)
        hop_send(k + 1)

    wait_got(vz_copies)
    wait_got(vel_copies)

    def dy(f):
        lane = lax.broadcasted_iota(jnp.int32, f.shape, 2)
        up = jnp.where(lane < ny - 1, pltpu.roll(f, ny - 1, 2), 0.0)
        down = jnp.where(lane > 0, pltpu.roll(f, 1, 2), 0.0)
        return (up - down) * 0.5

    def dz(f, low, high):
        sub = lax.broadcasted_iota(jnp.int32, f.shape, 1)
        up = pltpu.roll(jnp.where(sub >= 1, f, jnp.broadcast_to(high, f.shape)), nz - 1, 1)
        down = pltpu.roll(jnp.where(sub < nz - 1, f, jnp.broadcast_to(low, f.shape)), 1, 1)
        return (up - down) * 0.5

    def dz_inside(f):
        sub = lax.broadcasted_iota(jnp.int32, f.shape, 1)
        up = jnp.where(sub < nz - 1, pltpu.roll(f, nz - 1, 1), 0.0)
        down = jnp.where(sub >= 1, pltpu.roll(f, 1, 1), 0.0)
        return (up - down) * 0.5

    def strains(field, halo, x, size):
        v = [field[c, pl.ds(x + 1, size)] for c in range(3)]
        dx_v = [(field[c, pl.ds(x + 2, size)] - field[c, pl.ds(x, size)]) * 0.5 for c in range(3)]
        dz_v = [dz(f, halo[0, c, pl.ds(x, size)], halo[1, c, pl.ds(x, size)]) for c, f in enumerate(v)]
        dy_v = [dy(f) for f in v]
        div = dx_v[0] + dz_v[1] + dy_v[2]
        third = div * (1.0 / 3.0)
        return (
            dx_v[0] - third,
            dz_v[1] - third,
            dy_v[2] - third,
            0.5 * (dx_v[1] + dz_v[0]),
            0.5 * (dx_v[2] + dy_v[0]),
            0.5 * (dz_v[2] + dy_v[1]),
        ), div

    def second_invariant(trial):
        return jnp.sqrt(
            0.5 * (trial[0] * trial[0] + trial[1] * trial[1] + trial[2] * trial[2])
            + trial[3] * trial[3]
            + trial[4] * trial[4]
            + trial[5] * trial[5]
        )

    def first_trial(x, carry):
        strain, div = strains(V, VZH, x, block)
        quarter = 0.25 * div
        pres = PIN[at(x)] - quarter
        PR[at(x)] = pres
        PIN[at(x)] = pres - quarter
        twice = 2.0 * ETA[at(x)]
        trial = [
            twice * (strain[c] + IN[2 + c, at(x)] * (0.5 / shear_time_increment)) for c in range(6)
        ]
        for c in range(6):
            TAU[c, at(x)] = trial[c]
        TB[at(x)] = second_invariant(trial)
        return carry

    over_rows(first_trial)
    if len(rounds) > 1:
        hop_wait(len(rounds) - 1)

    @pl.when(odd)
    def _():
        signal(pair_sem, (gx, gz - 1))

    wait_got(plas_copies)
    for row in range(min(REACH, rows)):
        low, high = SM[row], SM[rows - 1 - row]
        for k in range(row + 1, REACH + 1):
            low = low + gauss_weights[REACH + k] * GXH[0, REACH + row - k]
            high = high + gauss_weights[REACH + k] * GXH[1, k - 1 - row]
        SM[row] = low
        SM[rows - 1 - row] = high

    half = ny // 2 if ny % 256 == 0 else ny

    def stress_rows(it, x, carry, pres, trial, tau_ii, strength, plas, edge):
        last = it == ITERS - 1
        most_f, most_eta = carry
        eta, inv = ETA[at(x)], INV[at(x)]
        yield_f = tau_ii - 0.5 * jnp.maximum(pres, 0.0) - strength
        dlam = jnp.maximum(yield_f, 0.0) * inv
        shrink = 1.0 - eta * dlam / jnp.maximum(tau_ii, 0.5)
        tau = [shrink * value for value in trial]
        PL[at(x)] = plas + dlam
        if last:
            for c in range(6):
                TAU[c, at(x)] = tau[c]
        SX[it, 0, at(x + 1)] = tau[0] - pres
        SX[it, 1, at(x + 1)] = tau[3]
        SX[it, 2, at(x + 1)] = tau[4]
        szz = tau[1] - pres
        TZ[0, at(x)] = szz
        TZ[1, at(x)] = tau[5]
        TZ[2, at(x)] = tau[2] - pres
        for c, f in enumerate((tau[3], szz, tau[5])):
            edge[0, c, at(x)] = f[:, 0:1]
            edge[1, c, at(x)] = f[:, nz - 1 : nz]
        return jnp.maximum(most_f, yield_f), jnp.maximum(most_eta, eta * shrink)

    def forces(it, x, size, diff_z):
        s = [SX[it, c, pl.ds(x + 1, size)] for c in range(3)]
        t = [TZ[c, pl.ds(x, size)] for c in range(3)]
        along_x = [0.5 * (SX[it, c, pl.ds(x + 2, size)] - SX[it, c, pl.ds(x, size)]) for c in range(3)]
        along_z = [diff_z(c, f) for c, f in enumerate((s[1], t[0], t[1]))]
        along_y = [dy(f) for f in (s[2], t[1], t[2])]
        return [along_x[c] + along_z[c] + along_y[c] for c in range(3)]

    def folded(most):
        most = jnp.max(jnp.max(most, axis=0), axis=0, keepdims=True)
        return jnp.maximum(most[:, :half], most[:, ny - half :])

    def tell(it, place):
        pltpu.make_async_remote_copy(
            src_ref=PK.at[it, me],
            dst_ref=PK.at[it, me],
            send_sem=pk_send,
            recv_sem=pk_recv.at[it],
            device_id=place,
            device_id_type=MESH,
        ).start()

    def tell_all(it, most_f, most_eta):
        PK[it, me] = jnp.concatenate([folded(most_f), folded(most_eta)], axis=0)
        for dz_ in range(gz_count):
            other_z = gz + dz_
            other_z = jnp.where(other_z >= gz_count, other_z - gz_count, other_z)

            def one(dx_, carry, other_z=other_z):
                other_x = gx + dx_
                tell(it, (jnp.where(other_x >= gx_count, other_x - gx_count, other_x), other_z))
                return carry

            first = 0 if dz_ else 1
            if gx_count <= 16 and gz_count <= 2:
                for dx_ in range(first, gx_count):
                    one(dx_, 0)
            else:
                lax.fori_loop(first, gx_count, one, 0)

    def told(it):
        others = PK.at[it, pl.ds(0, total - 1)]
        pltpu.make_async_copy(others, others, pk_recv.at[it]).wait()
        peaks = jnp.max(PK[it], axis=0)
        step = 0.125 / jnp.max(peaks[1:2], axis=1, keepdims=True)
        return step, jnp.max(peaks[0:1], axis=1, keepdims=True)

    def tell_sent():
        others = PK.at[0, pl.ds(0, total - 1)]
        pltpu.make_async_copy(others, others, pk_send).wait()

    lowest = jnp.full(many, -jnp.inf, jnp.float32)

    def first_stress(x, carry):
        strength = COH[at(x)] / (1.0 + 2.0 * SM[at(x)])
        COH[at(x)] = strength
        trial = [TAU[c, at(x)] for c in range(6)]
        return stress_rows(0, x, carry, PR[at(x)], trial, TB[at(x)], strength, PLZ[at(x)], SE)

    most_f, most_eta = over_rows(first_stress, (lowest, lowest))

    @pl.when(even)
    def _():
        pl.semaphore_wait(pair_sem, 1)

    tell_all(0, most_f, most_eta)
    wait_sent(vel_copies)
    for number, row in ((0, 0), (1, rows - 1)):
        force = forces(0, row, 1, lambda c, f: dz_inside(f))
        for c in range(3):
            XS[number, c] = SX[0, c, row + 1]
            XS[number, 3 + c] = force[c][0]
        for layer in range(2):
            where = 2 * number + layer
            place = (nz - 1) * layer
            for c in range(3):
                CE[where, c] = SX[0, c, row + 1, place : place + 1]
                CE[where, 3 + c] = SE[layer, c, row]
    x_copies = [
        ("xh", described("xh", XS.at[1], XH.at[0], 4, 2)),
        ("xl", described("xl", XS.at[0], XH.at[1], 4, 2)),
    ]
    start_ordered(x_copies)
    corner_copies = []
    for number, (a, b) in enumerate(corners):
        there = corners.index((opposite[a], opposite[b]))
        corner_copies.append(
            (
                a + b,
                pltpu.make_async_remote_copy(
                    src_ref=CE.at[number],
                    dst_ref=CH.at[there],
                    send_sem=send_sem.at[8 + number],
                    recv_sem=recv_sem.at[10 + number],
                    device_id=target[a + b],
                    device_id_type=MESH,
                ),
            )
        )
    start(corner_copies)

    def own_force(x, carry):
        force = forces(0, x, block, lambda c, f: dz_inside(f))
        for c in range(3):
            RF[c, at(x + 1)] = force[c]
            SE[0, 3 + c, at(x)] = force[c][:, 0:1]
            SE[1, 3 + c, at(x)] = force[c][:, nz - 1 : nz]
        return carry

    over_rows(own_force)
    wait_sent(pz_copies)
    z_copies = [
        ("zh", described("zh", SE.at[1], ZH.at[0], 0, 0)),
        ("zl", described("zl", SE.at[0], ZH.at[1], 0, 0)),
    ]
    start(z_copies)
    wait_got(z_copies)

    def add_z(x, carry):
        sub = lax.broadcasted_iota(jnp.int32, many, 1)
        for c in range(3):
            high = jnp.where(sub == nz - 1, jnp.broadcast_to(ZH[1, c, at(x)], many), 0.0)
            low = jnp.where(sub == 0, jnp.broadcast_to(ZH[0, c, at(x)], many), 0.0)
            RF[c, at(x + 1)] = RF[c, at(x + 1)] + 0.5 * (high - low)
        return carry

    def second_trial(x, size):
        strain, div = strains(RF, RZF, x, size)
        twice = 2.0 * ETA[pl.ds(x, size)]
        for c in range(6):
            TR[c, pl.ds(x, size)] = twice * strain[c]
        DV[pl.ds(x, size)] = 0.25 * div

    over_rows(add_z)

    @pl.when(has["zl"])
    def _():
        RZF[0] = ZH[0, 3:6] + 0.5 * SE[0, 0:3]

    @pl.when(has["zh"])
    def _():
        RZF[1] = ZH[1, 3:6] - 0.5 * SE[1, 0:3]

    inside = rows - 4
    if inside > 0:
        size = next(size for size in (6, 4, 3, 2, 1) if inside % size == 0)

        def inside_trial(i, carry):
            second_trial(2 + i * size, size)
            return carry

        lax.fori_loop(0, inside // size, inside_trial, 0)

    wait_got(x_copies)
    wait_got(corner_copies)
    for number, side, row in ((0, "xl", 0), (1, "xh", rows - 1)):
        sign = 0.5 - number
        beyond = row + 2 * number
        for c in range(3):
            RF[c, row + 1] = RF[c, row + 1] - sign * XH[number, c]

        @pl.when(has[side])
        def _(number=number, sign=sign, row=row, beyond=beyond):
            sub = lax.broadcasted_iota(jnp.int32, (nz, ny), 0)
            for c in range(3):
                low = jnp.where(sub == 0, jnp.broadcast_to(CH[2 * number, 3 + c], (nz, ny)), 0.0)
                high = jnp.where(sub == nz - 1, jnp.broadcast_to(CH[2 * number + 1, 3 + c], (nz, ny)), 0.0)
                RF[c, beyond] = XH[number, 3 + c] + sign * SX[0, c, row + 1] + 0.5 * (high - low)

        for layer in range(2):
            for c in range(3):
                RZF[layer, c, row] = RZF[layer, c, row] - sign * CH[2 * number + layer, c]
    if inside > 0:
        second_trial(0, 2)
        second_trial(rows - 2, 2)
    else:
        second_trial(0, rows)

    step, top = told(0)
    tell_sent()
    tops = [top]

    def second_stress(x, carry):
        pres = PIN[at(x)] - step * DV[at(x)]
        PR[at(x)] = pres
        trial = [TAU[c, at(x)] + step * TR[c, at(x)] for c in range(6)]
        return stress_rows(
            1, x, carry, pres, trial, second_invariant(trial), COH[at(x)], PL[at(x)], SEL
        )

    most_f, most_eta = over_rows(second_stress, (lowest, lowest))
    tell_all(1, most_f, most_eta)
    wait_sent(plas_copies)
    wait_sent(vz_copies)
    sx_copies = [
        ("xh", described("xh", SX.at[1, :, pl.ds(rows, 1)], XHL.at[0], 2, 3)),
        ("xl", described("xl", SX.at[1, :, pl.ds(1, 1)], XHL.at[1], 2, 3)),
    ]
    start_ordered(sx_copies)
    sz_copies = [
        ("zh", described("zh", SEL.at[1], ZHL.at[0], 1, 1)),
        ("zl", described("zl", SEL.at[0], ZHL.at[1], 1, 1)),
    ]
    start(sz_copies)

    def moved(x, carry):
        for c in range(3):
            V[c, at(x + 1)] = V[c, at(x + 1)] + step * RF[c, at(x + 1)]
        return carry

    over_rows(moved)
    wait_got(sz_copies)

    def last_force(x, carry):
        def diff_z(c, f):
            return dz(f, ZHL[0, c, at(x)], ZHL[1, c, at(x)])

        force = forces(1, x, block, diff_z)
        for c in range(3):
            RF[c, at(x + 1)] = force[c]
        return carry

    over_rows(last_force)
    wait_got(sx_copies)
    for c in range(3):
        RF[c, 1] = RF[c, 1] - 0.5 * XHL[0, c, 0]
        RF[c, rows] = RF[c, rows] + 0.5 * XHL[1, c, 0]
    step, top = told(1)
    tops.append(top)

    def last_velocity(x, carry):
        for c in range(3):
            VOUT[c, at(x)] = V[c, at(x + 1)] + step * RF[c, at(x + 1)]
        return carry

    over_rows(last_velocity)
    peak_out[...] = jnp.concatenate(tops, axis=1)[0]
    wait_sent(x_copies + corner_copies + z_copies + sx_copies + sz_copies)
    tell_sent()


def store_kernel(*refs):
    held, out, sem = refs[:5], refs[5:10], refs[10]
    copies = [pltpu.make_async_copy(a, b, sem.at[i]) for i, (a, b) in enumerate(zip(held, out))]
    for copy in copies:
        copy.start()
    for copy in copies:
        copy.wait()


def solution(mesh):
    gx_count, gz_count = mesh.shape["gx"], mesh.shape["gz"]
    total = gx_count * gz_count

    def per_device(velocity, pressure, stress_old, plastic, viscosity, weak_seed):
        rows, nz, ny = pressure.shape
        cells = (rows, nz, ny)
        f32 = jnp.float32
        vm = lambda *shape: pltpu.VMEM(shape, f32)
        hops = len(bits_of(gx_count)) + len(bits_of(gz_count // 2))
        anywhere = pl.BlockSpec(memory_space=pl.ANY)
        shapes = (velocity.shape, pressure.shape, stress_old.shape, plastic.shape)
        held = pl.pallas_call(
            functools.partial(kernel, gx_count, gz_count),
            out_shape=tuple(vm(*shape) for shape in shapes + ((ITERS,),)),
            in_specs=[anywhere] * 6,
            out_specs=(pl.BlockSpec(memory_space=pltpu.VMEM),) * 5,
            scratch_shapes=[
                vm(3, rows + 2, nz, ny),
                vm(8, *cells),
                pltpu.VMEM(cells, jnp.int32),
                vm(*cells),
                vm(2, *cells),
                vm(*cells),
                vm(*cells),
                vm(*cells),
                vm(ny, ny),
                vm(*cells),
                vm(2, REACH, nz, ny),
                vm(*cells),
                vm(2, 3, rows, 1, ny),
                vm(2, 3, rows, 1, ny),
                vm(ITERS, 3, rows + 2, nz, ny),
                vm(3, *cells),
                vm(2, 6, rows, 1, ny),
                vm(2, 6, rows, 1, ny),
                vm(2, 6, nz, ny),
                vm(2, 6, nz, ny),
                vm(4, 6, 1, ny),
                vm(4, 6, 1, ny),
                vm(2, 3, rows, 1, ny),
                vm(2, 3, rows, 1, ny),
                vm(2, 3, 1, nz, ny),
                vm(3, rows + 2, nz, ny),
                vm(2, 3, rows, 1, ny),
                vm(6, *cells),
                vm(*cells),
                vm(*cells),
                vm(ITERS, total, 2, ny // 2 if ny % 256 == 0 else ny),
                pltpu.SemaphoreType.DMA((4,)),
                pltpu.SemaphoreType.DMA((12,)),
                pltpu.SemaphoreType.DMA((14,)),
                pltpu.SemaphoreType.DMA,
                pltpu.SemaphoreType.DMA((ITERS,)),
                pltpu.SemaphoreType.REGULAR,
                pltpu.SemaphoreType.REGULAR((hops,)),
            ],
            compiler_params=pltpu.CompilerParams(collective_id=0, has_side_effects=True),
        )(velocity, pressure, stress_old, plastic, viscosity, weak_seed)
        held = [pltpu.with_memory_space_constraint(array, pltpu.VMEM) for array in held]
        return pl.pallas_call(
            store_kernel,
            out_shape=tuple(jax.ShapeDtypeStruct(shape, f32) for shape in shapes)
            + (jax.ShapeDtypeStruct((ITERS,), f32),),
            in_specs=[anywhere] * 5,
            out_specs=(anywhere,) * 5,
            scratch_shapes=[pltpu.SemaphoreType.DMA((5,))],
        )(*held)

    in_specs = (
        P(None, "gx", "gz", None),
        P("gx", "gz", None),
        P(None, "gx", "gz", None),
        P("gx", "gz", None),
        P("gx", "gz", None),
        P("gx", "gz", None),
    )
    out_specs = (
        P(None, "gx", "gz", None),
        P("gx", "gz", None),
        P(None, "gx", "gz", None),
        P("gx", "gz", None),
        P(),
    )
    return jax.shard_map(
        per_device, mesh=mesh, in_specs=in_specs, out_specs=out_specs, check_vma=False
    )
```

```python
import functools
import math

import jax
import jax.numpy as jnp
from jax import lax
from jax.experimental import pallas as pl
from jax.experimental.pallas import tpu as pltpu
from jax.sharding import PartitionSpec as P

ITERS = 2
REACH = 6
PLANE = 4
MESH = pl.DeviceIdType.MESH

unnormalized_weights = [math.exp(-(k * k) / 18.0) for k in range(-REACH, REACH + 1)]
weight_total = sum(unnormalized_weights)
gauss_weights = [value / weight_total for value in unnormalized_weights]
shear_time_increment = 20.0


def bits_of(count):
    assert count & (count - 1) == 0
    return [1 << bit for bit in range(count.bit_length() - 1)]


def kernel(
    gx_count,
    gz_count,
    vel_in,
    pres_in,
    old_in,
    plas_in,
    visc_in,
    weak_in,
    VOUT,
    PR,
    TAU,
    PL,
    peak_out,
    V,
    IN,
    WK,
    PLZ,
    PZH,
    ETA,
    INV,
    COH,
    YM,
    GX,
    GXH,
    SM,
    VZE,
    VZH,
    SX,
    TZ,
    SE,
    ZH,
    XS,
    XH,
    CE,
    CH,
    SEL,
    ZHL,
    XHL,
    RF,
    RZF,
    TR,
    DV,
    TB,
    MOST,
    PK,
    in_sem,
    send_sem,
    recv_sem,
    pk_send,
    pk_recv,
    pair_sem,
    hop_sem,
):
    rows, nz, ny = PR.shape
    gx = lax.axis_index("gx")
    gz = lax.axis_index("gz")
    me = gx * gz_count + gz
    total = gx_count * gz_count
    has = {
        "xl": gx > 0,
        "xh": gx < gx_count - 1,
        "zl": gz > 0,
        "zh": gz < gz_count - 1,
    }
    target = {
        "xl": (gx - 1, gz),
        "xh": (gx + 1, gz),
        "zl": (gx, gz - 1),
        "zh": (gx, gz + 1),
    }
    opposite = {"xl": "xh", "xh": "xl", "zl": "zh", "zh": "zl"}
    corners = [(a, b) for a in ("xl", "xh") for b in ("zl", "zh")]
    for a, b in corners:
        has[a + b] = jnp.logical_and(has[a], has[b])
        target[a + b] = (target[a][0], target[b][1])
        opposite[a + b] = opposite[a] + opposite[b]
    barrier = pltpu.get_barrier_semaphore()

    side_of = gz % 2
    odd = side_of == 1
    even = side_of == 0
    lead = gz + 1 - side_of
    couple = gz // 2

    def flipped(index, bit):
        return index + bit * (1 - 2 * ((index // bit) % 2))

    always = gx >= 0
    rounds = [[(flipped(gx, bit), gz, always)] for bit in bits_of(min(PLANE, gx_count))]
    rounds += [
        [(gx - far, gz, gx >= far), (gx + far, gz, gx < gx_count - far)]
        for far in bits_of(gx_count)
        if far >= PLANE
    ]
    rounds += [[(gx, 2 * flipped(couple, bit) + 1, always)] for bit in bits_of(gz_count // 2)]
    along_gx = len(bits_of(gx_count))
    met = [place for far in rounds[1:3] + rounds[max(along_gx, 3) :] for place in far]

    def signal(sem, place):
        pl.semaphore_signal(sem, inc=1, device_id=place, device_id_type=MESH)

    def one_if(flag):
        return jnp.where(flag, 1, 0)

    VI, PIN = IN.at[0], IN.at[1]
    plas_load = pltpu.make_async_copy(plas_in, PLZ, in_sem.at[0])
    vel_load = pltpu.make_async_copy(vel_in, V.at[:, pl.ds(1, rows)], in_sem.at[1])
    weak_load = pltpu.make_async_copy(weak_in, WK, in_sem.at[2])
    rest_loads = [
        pltpu.make_async_copy(visc_in, VI, in_sem.at[3]),
        pltpu.make_async_copy(pres_in, PIN, in_sem.at[3]),
        pltpu.make_async_copy(old_in, IN.at[pl.ds(2, 6)], in_sem.at[3]),
    ]
    all_rest = pltpu.make_async_copy(IN, IN, in_sem.at[3])

    @pl.when(odd)
    def _():
        signal(barrier, (gx, gz - 1))

        @pl.when(has["zh"])
        def _():
            signal(barrier, (gx, gz + 1))

    for side in ("xl", "xh"):

        @pl.when(has[side])
        def _(side=side):
            signal(barrier, (target[side][0], lead))

    plas_load.start()

    @pl.when(odd)
    def _():
        for x_place, z_place, there in met:

            @pl.when(there)
            def _(x_place=x_place, z_place=z_place):
                signal(barrier, (x_place, z_place))

    def described(side, source, landing, got, sent):
        number = {"xl": 0, "xh": 1, "zl": 0, "zh": 1}.get(side, 0)
        return pltpu.make_async_remote_copy(
            src_ref=source,
            dst_ref=landing,
            send_sem=send_sem.at[2 * sent + number],
            recv_sem=recv_sem.at[2 * got + number],
            device_id=target[side],
            device_id_type=MESH,
        )

    def start(pairs):
        for side, copy in pairs:

            @pl.when(has[side])
            def _(copy=copy):
                copy.start()

    gx_odd = gx % 2 == 1
    gx_even = gx % 2 == 0

    def start_far(pairs):
        for place, side in ((gx_odd, "xh"), (gx_even, "xl")):

            @pl.when(place)
            def _(side=side):
                start([pair for pair in pairs if pair[0] == side])

    def start_near(pairs):
        for place, side in ((gx_odd, "xl"), (gx_even, "xh")):

            @pl.when(place)
            def _(side=side):
                start([pair for pair in pairs if pair[0] == side])

    has_far = jnp.logical_or(
        jnp.logical_and(gx_odd, has["xh"]), jnp.logical_and(gx_even, has["xl"])
    )

    def wait_sent(pairs):
        for side, copy in pairs:

            @pl.when(has[side])
            def _(copy=copy):
                copy.wait_send()

    def wait_got(pairs):
        for side, copy in pairs:

            @pl.when(has[opposite[side]])
            def _(copy=copy):
                copy.wait_recv()

    def zero(ref):
        ref[...] = jnp.zeros(ref.shape, ref.dtype)

    def zero_unless(side, *refs):
        @pl.when(jnp.logical_not(has[side]))
        def _():
            for ref in refs:
                zero(ref)

    @pl.when(even)
    def _():
        pl.semaphore_wait(barrier, 1 + one_if(has["zl"]))
        signal(pair_sem, (gx, gz + 1))

        @pl.when(has["zl"])
        def _():
            signal(pair_sem, (gx, gz - 1))

    @pl.when(odd)
    def _():
        pl.semaphore_wait(pair_sem, 1 + one_if(has["zh"]))

    pz_copies = [
        ("zh", described("zh", plas_in, PZH.at[0], 0, 0)),
        ("zl", described("zl", plas_in, PZH.at[1], 0, 0)),
    ]
    start(pz_copies)
    vel_load.start()
    for copy in rest_loads:
        copy.start()
    weak_load.start()

    places_a = lax.broadcasted_iota(jnp.int32, (ny, ny), 0)
    places_b = lax.broadcasted_iota(jnp.int32, (ny, ny), 1)
    gap = (places_a - places_b).astype(jnp.float32)
    YM[...] = jnp.where(
        jnp.abs(gap) <= float(REACH), jnp.exp(-gap * gap / 18.0) / weight_total, 0.0
    )
    zero_unless("zl", PZH.at[0])
    zero_unless("zh", PZH.at[1])
    zero_unless("xl", V.at[:, pl.ds(0, 1)], GXH.at[0], XH.at[0], XHL.at[0], RF.at[:, pl.ds(0, 1)])
    zero_unless("xh", V.at[:, pl.ds(rows + 1, 1)], GXH.at[1], XH.at[1], XHL.at[1])
    zero_unless("xh", RF.at[:, pl.ds(rows + 1, 1)])
    zero_unless("zl", VZH.at[0], ZH.at[0], ZHL.at[0], RZF.at[0])
    zero_unless("zh", VZH.at[1], ZH.at[1], ZHL.at[1], RZF.at[1])
    for number, (a, b) in enumerate(corners):
        zero_unless(a + b, CH.at[number])
    for it in range(ITERS):
        zero(SX.at[it, :, pl.ds(0, 1)])
        zero(SX.at[it, :, pl.ds(rows + 1, 1)])

    @pl.when(odd)
    def _():
        greeters = 2 * (one_if(has["xl"]) + one_if(has["xh"]))
        for _, _, there in met:
            greeters = greeters + one_if(there)
        pl.semaphore_wait(barrier, greeters)
        signal(pair_sem, (gx, gz - 1))

    @pl.when(even)
    def _():
        pl.semaphore_wait(pair_sem, 1)

    vel_copies = [
        ("xh", described("xh", vel_in.at[:, pl.ds(rows - 1, 1)], V.at[:, pl.ds(0, 1)], 2, 2)),
        ("xl", described("xl", vel_in.at[:, pl.ds(0, 1)], V.at[:, pl.ds(rows + 1, 1)], 2, 2)),
    ]
    start_far(vel_copies)

    @pl.when(jnp.logical_not(has_far))
    def _():
        start_near(vel_copies)


    def hop_send(k):
        if k < len(rounds):

            @pl.when(odd)
            def _():
                for x_place, z_place, there in rounds[k]:

                    @pl.when(there)
                    def _(x_place=x_place, z_place=z_place):
                        signal(hop_sem.at[k], (x_place, z_place))

    def hop_wait(k):
        if k < len(rounds):

            @pl.when(odd)
            def _():
                expected = 0
                for _, _, there in rounds[k]:
                    expected = expected + one_if(there)
                pl.semaphore_wait(hop_sem.at[k], expected)

    hop_send(0)

    block = rows // 2
    many = (block, nz, ny)

    def over_rows(body, carry=0):
        return lax.fori_loop(0, rows // block, lambda i, state: body(i * block, state), carry)

    def at(x):
        return pl.ds(x, block)

    vel_load.wait()

    def vel_edges(x, carry):
        for c in range(3):
            row = V[c, at(x + 1)]
            VZE[0, c, at(x)] = row[:, 0:1]
            VZE[1, c, at(x)] = row[:, nz - 1 : nz]
        return carry

    over_rows(vel_edges)
    plas_load.wait()
    wait_got(pz_copies)
    vz_copies = [
        ("zh", described("zh", VZE.at[1], VZH.at[0], 1, 1)),
        ("zl", described("zl", VZE.at[0], VZH.at[1], 1, 1)),
    ]
    start(vz_copies)

    def smooth_z(x, carry):
        own, low, high = PLZ[at(x)], PZH[0, at(x)], PZH[1, at(x)]
        sub = lax.broadcasted_iota(jnp.int32, many, 1)
        sum_ = gauss_weights[REACH] * own
        for k in range(1, REACH + 1):
            above = pltpu.roll(jnp.where(sub >= k, own, high), nz - k, 1)
            below = pltpu.roll(jnp.where(sub < nz - k, own, low), k, 1)
            sum_ = sum_ + gauss_weights[REACH + k] * (above + below)
        SM[at(x)] = sum_
        return carry

    over_rows(smooth_z)
    GX[...] = jnp.dot(
        SM[...].reshape(rows * nz, ny),
        YM[...],
        precision=lax.Precision.HIGHEST,
        preferred_element_type=jnp.float32,
    ).reshape(rows, nz, ny)
    plas_copies = [
        ("xh", described("xh", GX.at[pl.ds(rows - REACH, REACH)], GXH.at[0], 3, 3)),
        ("xl", described("xl", GX.at[pl.ds(0, REACH)], GXH.at[1], 3, 3)),
    ]
    start_far(plas_copies)

    @pl.when(has_far)
    def _():
        start_near(vel_copies)

    start_near(plas_copies)
    hop_wait(0)
    hop_send(1)

    all_rest.wait()
    weak_load.wait()

    def prepare(x, carry):
        eta = VI[at(x)]
        eta = shear_time_increment * eta / (eta + shear_time_increment)
        ETA[at(x)] = eta
        INV[at(x)] = 1.0 / (eta + 0.5)
        COH[at(x)] = 0.8660254 - (0.8660254 * 0.6) * WK[at(x)].astype(jnp.float32)
        return carry

    over_rows(prepare)
    for row in range(rows):
        sum_ = gauss_weights[REACH] * GX[row]
        for k in range(1, REACH + 1):
            for other in (row - k, row + k):
                if 0 <= other < rows:
                    sum_ = sum_ + gauss_weights[REACH + k] * GX[other]
        SM[row] = sum_
    for k in range(1, len(rounds) - 1):
        hop_wait(k)
        hop_send(k + 1)

    wait_got(vz_copies)

    def dy(f):
        lane = lax.broadcasted_iota(jnp.int32, f.shape, 2)
        up = jnp.where(lane < ny - 1, pltpu.roll(f, ny - 1, 2), 0.0)
        down = jnp.where(lane > 0, pltpu.roll(f, 1, 2), 0.0)
        return (up - down) * 0.5

    def dz(f, low, high):
        sub = lax.broadcasted_iota(jnp.int32, f.shape, 1)
        up = pltpu.roll(jnp.where(sub >= 1, f, jnp.broadcast_to(high, f.shape)), nz - 1, 1)
        down = pltpu.roll(jnp.where(sub < nz - 1, f, jnp.broadcast_to(low, f.shape)), 1, 1)
        return (up - down) * 0.5

    def dz_inside(f):
        sub = lax.broadcasted_iota(jnp.int32, f.shape, 1)
        up = jnp.where(sub < nz - 1, pltpu.roll(f, nz - 1, 1), 0.0)
        down = jnp.where(sub >= 1, pltpu.roll(f, 1, 1), 0.0)
        return (up - down) * 0.5

    def strains(field, halo, x, size):
        v = [field[c, pl.ds(x + 1, size)] for c in range(3)]
        dx_v = [(field[c, pl.ds(x + 2, size)] - field[c, pl.ds(x, size)]) * 0.5 for c in range(3)]
        dz_v = [dz(f, halo[0, c, pl.ds(x, size)], halo[1, c, pl.ds(x, size)]) for c, f in enumerate(v)]
        dy_v = [dy(f) for f in v]
        div = dx_v[0] + dz_v[1] + dy_v[2]
        third = div * (1.0 / 3.0)
        return (
            dx_v[0] - third,
            dz_v[1] - third,
            dy_v[2] - third,
            0.5 * (dx_v[1] + dz_v[0]),
            0.5 * (dx_v[2] + dy_v[0]),
            0.5 * (dz_v[2] + dy_v[1]),
        ), div

    def second_invariant(trial):
        return jnp.sqrt(
            0.5 * (trial[0] * trial[0] + trial[1] * trial[1] + trial[2] * trial[2])
            + trial[3] * trial[3]
            + trial[4] * trial[4]
            + trial[5] * trial[5]
        )

    def first_trial(x):
        strain, div = strains(V, VZH, x, block)
        quarter = 0.25 * div
        pres = PIN[at(x)] - quarter
        PR[at(x)] = pres
        PIN[at(x)] = pres - quarter
        twice = 2.0 * ETA[at(x)]
        trial = [
            twice * (strain[c] + IN[2 + c, at(x)] * (0.5 / shear_time_increment)) for c in range(6)
        ]
        for c in range(6):
            TAU[c, at(x)] = trial[c]
        TB[at(x)] = second_invariant(trial)

    def in_order(act):
        for place, numbers in ((gx_odd, (1, 0)), (gx_even, (0, 1))):

            @pl.when(place)
            def _(numbers=numbers):
                for number in numbers:
                    act(number, number == numbers[0])

    def one_trial(number, far):
        wait_got(vel_copies[number : number + 1])
        first_trial(number * block)

    in_order(one_trial)
    if len(rounds) > 1:
        hop_wait(len(rounds) - 1)

    @pl.when(odd)
    def _():
        signal(pair_sem, (gx, gz - 1))

    half = ny // 2 if ny % 256 == 0 else ny

    def stress_rows(it, x, pres, trial, tau_ii, strength, plas, edge):
        last = it == ITERS - 1
        eta, inv = ETA[at(x)], INV[at(x)]
        yield_f = tau_ii - 0.5 * jnp.maximum(pres, 0.0) - strength
        dlam = jnp.maximum(yield_f, 0.0) * inv
        shrink = 1.0 - eta * dlam / jnp.maximum(tau_ii, 0.5)
        tau = [shrink * value for value in trial]
        PL[at(x)] = plas + dlam
        if last:
            for c in range(6):
                TAU[c, at(x)] = tau[c]
        SX[it, 0, at(x + 1)] = tau[0] - pres
        SX[it, 1, at(x + 1)] = tau[3]
        SX[it, 2, at(x + 1)] = tau[4]
        szz = tau[1] - pres
        TZ[0, at(x)] = szz
        TZ[1, at(x)] = tau[5]
        TZ[2, at(x)] = tau[2] - pres
        for c, f in enumerate((tau[3], szz, tau[5])):
            edge[0, c, at(x)] = f[:, 0:1]
            edge[1, c, at(x)] = f[:, nz - 1 : nz]
        return yield_f, eta * shrink

    def forces(it, x, size, diff_z):
        s = [SX[it, c, pl.ds(x + 1, size)] for c in range(3)]
        t = [TZ[c, pl.ds(x, size)] for c in range(3)]
        along_x = [0.5 * (SX[it, c, pl.ds(x + 2, size)] - SX[it, c, pl.ds(x, size)]) for c in range(3)]
        along_z = [diff_z(c, f) for c, f in enumerate((s[1], t[0], t[1]))]
        along_y = [dy(f) for f in (s[2], t[1], t[2])]
        return [along_x[c] + along_z[c] + along_y[c] for c in range(3)]

    def folded(most):
        most = jnp.max(jnp.max(most, axis=0), axis=0, keepdims=True)
        return jnp.maximum(most[:, :half], most[:, ny - half :])

    def tell(it, place):
        pltpu.make_async_remote_copy(
            src_ref=PK.at[it, me],
            dst_ref=PK.at[it, me],
            send_sem=pk_send,
            recv_sem=pk_recv.at[it],
            device_id=place,
            device_id_type=MESH,
        ).start()

    def tell_all(it):
        most = [folded(jnp.maximum(MOST[0, k], MOST[1, k])) for k in range(2)]
        PK[it, me] = jnp.concatenate(most, axis=0)
        for dz_ in range(gz_count):
            other_z = gz + dz_
            other_z = jnp.where(other_z >= gz_count, other_z - gz_count, other_z)

            def one(dx_, carry, other_z=other_z):
                other_x = gx + dx_
                tell(it, (jnp.where(other_x >= gx_count, other_x - gx_count, other_x), other_z))
                return carry

            first = 0 if dz_ else 1
            if gx_count <= 16 and gz_count <= 2:
                for dx_ in range(first, gx_count):
                    one(dx_, 0)
            else:
                lax.fori_loop(first, gx_count, one, 0)

    def told(it):
        others = PK.at[it, pl.ds(0, total - 1)]
        pltpu.make_async_copy(others, others, pk_recv.at[it]).wait()
        peaks = jnp.max(PK[it], axis=0)
        step = 0.125 / jnp.max(peaks[1:2], axis=1, keepdims=True)
        return step, jnp.max(peaks[0:1], axis=1, keepdims=True)

    def tell_sent():
        others = PK.at[0, pl.ds(0, total - 1)]
        pltpu.make_async_copy(others, others, pk_send).wait()

    def first_stress(x):
        strength = COH[at(x)] / (1.0 + 2.0 * SM[at(x)])
        COH[at(x)] = strength
        trial = [TAU[c, at(x)] for c in range(6)]
        return stress_rows(0, x, PR[at(x)], trial, TB[at(x)], strength, PLZ[at(x)], SE)

    x_copies = [
        ("xh", described("xh", XS.at[1], XH.at[0], 4, 2)),
        ("xl", described("xl", XS.at[0], XH.at[1], 4, 2)),
    ]
    corner_copies = []
    for number, (a, b) in enumerate(corners):
        there = corners.index((opposite[a], opposite[b]))
        corner_copies.append(
            (
                a + b,
                pltpu.make_async_remote_copy(
                    src_ref=CE.at[number],
                    dst_ref=CH.at[there],
                    send_sem=send_sem.at[8 + number],
                    recv_sem=recv_sem.at[10 + number],
                    device_id=target[a + b],
                    device_id_type=MESH,
                ),
            )
        )

    def one_side(number, far):
        row = (rows - 1) * number
        wait_got(plas_copies[number : number + 1])
        for beside in range(min(REACH, block)):
            here = beside if number == 0 else rows - 1 - beside
            sum_ = SM[here]
            for k in range(beside + 1, REACH + 1):
                place = REACH + beside - k if number == 0 else k - 1 - beside
                sum_ = sum_ + gauss_weights[REACH + k] * GXH[number, place]
            SM[here] = sum_
        MOST[number, 0], MOST[number, 1] = first_stress(number * block)
        force = forces(0, row, 1, lambda c, f: dz_inside(f))
        for c in range(3):
            XS[number, c] = SX[0, c, row + 1]
            XS[number, 3 + c] = force[c][0]
        for layer in range(2):
            where = 2 * number + layer
            place = (nz - 1) * layer
            for c in range(3):
                CE[where, c] = SX[0, c, row + 1, place : place + 1]
                CE[where, 3 + c] = SE[layer, c, row]
        if far:
            wait_sent(vel_copies)
            start(x_copies[1 - number : 2 - number])

    in_order(one_side)
    @pl.when(even)
    def _():
        pl.semaphore_wait(pair_sem, 1)

    tell_all(0)
    start_near(x_copies)
    start(corner_copies)

    def own_force(x, carry):
        force = forces(0, x, block, lambda c, f: dz_inside(f))
        for c in range(3):
            RF[c, at(x + 1)] = force[c]
            SE[0, 3 + c, at(x)] = force[c][:, 0:1]
            SE[1, 3 + c, at(x)] = force[c][:, nz - 1 : nz]
        return carry

    over_rows(own_force)
    wait_sent(pz_copies)
    z_copies = [
        ("zh", described("zh", SE.at[1], ZH.at[0], 0, 0)),
        ("zl", described("zl", SE.at[0], ZH.at[1], 0, 0)),
    ]
    start(z_copies)
    wait_got(z_copies)

    def add_z(x, carry):
        sub = lax.broadcasted_iota(jnp.int32, many, 1)
        for c in range(3):
            high = jnp.where(sub == nz - 1, jnp.broadcast_to(ZH[1, c, at(x)], many), 0.0)
            low = jnp.where(sub == 0, jnp.broadcast_to(ZH[0, c, at(x)], many), 0.0)
            RF[c, at(x + 1)] = RF[c, at(x + 1)] + 0.5 * (high - low)
        return carry

    def second_trial(x, size):
        strain, div = strains(RF, RZF, x, size)
        twice = 2.0 * ETA[pl.ds(x, size)]
        for c in range(6):
            TR[c, pl.ds(x, size)] = twice * strain[c]
        DV[pl.ds(x, size)] = 0.25 * div

    over_rows(add_z)

    @pl.when(has["zl"])
    def _():
        RZF[0] = ZH[0, 3:6] + 0.5 * SE[0, 0:3]

    @pl.when(has["zh"])
    def _():
        RZF[1] = ZH[1, 3:6] - 0.5 * SE[1, 0:3]

    inside = rows - 4
    if inside > 0:
        size = next(size for size in (6, 4, 3, 2, 1) if inside % size == 0)

        def inside_trial(i, carry):
            second_trial(2 + i * size, size)
            return carry

        lax.fori_loop(0, inside // size, inside_trial, 0)

    wait_got(x_copies)
    wait_got(corner_copies)
    for number, side, row in ((0, "xl", 0), (1, "xh", rows - 1)):
        sign = 0.5 - number
        beyond = row + 2 * number
        for c in range(3):
            RF[c, row + 1] = RF[c, row + 1] - sign * XH[number, c]

        @pl.when(has[side])
        def _(number=number, sign=sign, row=row, beyond=beyond):
            sub = lax.broadcasted_iota(jnp.int32, (nz, ny), 0)
            for c in range(3):
                low = jnp.where(sub == 0, jnp.broadcast_to(CH[2 * number, 3 + c], (nz, ny)), 0.0)
                high = jnp.where(sub == nz - 1, jnp.broadcast_to(CH[2 * number + 1, 3 + c], (nz, ny)), 0.0)
                RF[c, beyond] = XH[number, 3 + c] + sign * SX[0, c, row + 1] + 0.5 * (high - low)

        for layer in range(2):
            for c in range(3):
                RZF[layer, c, row] = RZF[layer, c, row] - sign * CH[2 * number + layer, c]
    if inside > 0:
        second_trial(0, 2)
        second_trial(rows - 2, 2)
    else:
        second_trial(0, rows)

    step, top = told(0)
    tell_sent()
    tops = [top]

    def second_stress(i, carry):
        x = i * block
        pres = PIN[at(x)] - step * DV[at(x)]
        PR[at(x)] = pres
        trial = [TAU[c, at(x)] + step * TR[c, at(x)] for c in range(6)]
        MOST[i, 0], MOST[i, 1] = stress_rows(
            1, x, pres, trial, second_invariant(trial), COH[at(x)], PL[at(x)], SEL
        )
        return carry

    lax.fori_loop(0, 2, second_stress, 0)
    tell_all(1)
    wait_sent(plas_copies)
    wait_sent(vz_copies)
    sx_copies = [
        ("xh", described("xh", SX.at[1, :, pl.ds(rows, 1)], XHL.at[0], 2, 3)),
        ("xl", described("xl", SX.at[1, :, pl.ds(1, 1)], XHL.at[1], 2, 3)),
    ]
    start_far(sx_copies)
    start_near(sx_copies)
    sz_copies = [
        ("zh", described("zh", SEL.at[1], ZHL.at[0], 1, 1)),
        ("zl", described("zl", SEL.at[0], ZHL.at[1], 1, 1)),
    ]
    start(sz_copies)

    def moved(x, carry):
        for c in range(3):
            V[c, at(x + 1)] = V[c, at(x + 1)] + step * RF[c, at(x + 1)]
        return carry

    over_rows(moved)
    wait_got(sz_copies)

    def last_force(x, carry):
        def diff_z(c, f):
            return dz(f, ZHL[0, c, at(x)], ZHL[1, c, at(x)])

        force = forces(1, x, block, diff_z)
        for c in range(3):
            RF[c, at(x + 1)] = force[c]
        return carry

    over_rows(last_force)
    wait_got(sx_copies)
    for c in range(3):
        RF[c, 1] = RF[c, 1] - 0.5 * XHL[0, c, 0]
        RF[c, rows] = RF[c, rows] + 0.5 * XHL[1, c, 0]
    step, top = told(1)
    tops.append(top)

    def last_velocity(x, carry):
        for c in range(3):
            VOUT[c, at(x)] = V[c, at(x + 1)] + step * RF[c, at(x + 1)]
        return carry

    over_rows(last_velocity)
    peak_out[...] = jnp.concatenate(tops, axis=1)[0]
    wait_sent(x_copies + corner_copies + z_copies + sx_copies + sz_copies)
    tell_sent()


def store_kernel(*refs):
    held, out, sem = refs[:5], refs[5:10], refs[10]
    copies = [pltpu.make_async_copy(a, b, sem.at[i]) for i, (a, b) in enumerate(zip(held, out))]
    for copy in copies:
        copy.start()
    for copy in copies:
        copy.wait()


def solution(mesh):
    gx_count, gz_count = mesh.shape["gx"], mesh.shape["gz"]
    total = gx_count * gz_count

    def per_device(velocity, pressure, stress_old, plastic, viscosity, weak_seed):
        rows, nz, ny = pressure.shape
        cells = (rows, nz, ny)
        f32 = jnp.float32
        vm = lambda *shape: pltpu.VMEM(shape, f32)
        hops = len(bits_of(gx_count)) + len(bits_of(gz_count // 2))
        anywhere = pl.BlockSpec(memory_space=pl.ANY)
        shapes = (velocity.shape, pressure.shape, stress_old.shape, plastic.shape)
        held = pl.pallas_call(
            functools.partial(kernel, gx_count, gz_count),
            out_shape=tuple(vm(*shape) for shape in shapes + ((ITERS,),)),
            in_specs=[anywhere] * 6,
            out_specs=(pl.BlockSpec(memory_space=pltpu.VMEM),) * 5,
            scratch_shapes=[
                vm(3, rows + 2, nz, ny),
                vm(8, *cells),
                pltpu.VMEM(cells, jnp.int32),
                vm(*cells),
                vm(2, *cells),
                vm(*cells),
                vm(*cells),
                vm(*cells),
                vm(ny, ny),
                vm(*cells),
                vm(2, REACH, nz, ny),
                vm(*cells),
                vm(2, 3, rows, 1, ny),
                vm(2, 3, rows, 1, ny),
                vm(ITERS, 3, rows + 2, nz, ny),
                vm(3, *cells),
                vm(2, 6, rows, 1, ny),
                vm(2, 6, rows, 1, ny),
                vm(2, 6, nz, ny),
                vm(2, 6, nz, ny),
                vm(4, 6, 1, ny),
                vm(4, 6, 1, ny),
                vm(2, 3, rows, 1, ny),
                vm(2, 3, rows, 1, ny),
                vm(2, 3, 1, nz, ny),
                vm(3, rows + 2, nz, ny),
                vm(2, 3, rows, 1, ny),
                vm(6, *cells),
                vm(*cells),
                vm(*cells),
                vm(2, 2, rows // 2, nz, ny),
                vm(ITERS, total, 2, ny // 2 if ny % 256 == 0 else ny),
                pltpu.SemaphoreType.DMA((4,)),
                pltpu.SemaphoreType.DMA((12,)),
                pltpu.SemaphoreType.DMA((14,)),
                pltpu.SemaphoreType.DMA,
                pltpu.SemaphoreType.DMA((ITERS,)),
                pltpu.SemaphoreType.REGULAR,
                pltpu.SemaphoreType.REGULAR((hops,)),
            ],
            compiler_params=pltpu.CompilerParams(collective_id=0, has_side_effects=True),
        )(velocity, pressure, stress_old, plastic, viscosity, weak_seed)
        held = [pltpu.with_memory_space_constraint(array, pltpu.VMEM) for array in held]
        return pl.pallas_call(
            store_kernel,
            out_shape=tuple(jax.ShapeDtypeStruct(shape, f32) for shape in shapes)
            + (jax.ShapeDtypeStruct((ITERS,), f32),),
            in_specs=[anywhere] * 5,
            out_specs=(anywhere,) * 5,
            scratch_shapes=[pltpu.SemaphoreType.DMA((5,))],
        )(*held)

    in_specs = (
        P(None, "gx", "gz", None),
        P("gx", "gz", None),
        P(None, "gx", "gz", None),
        P("gx", "gz", None),
        P("gx", "gz", None),
        P("gx", "gz", None),
    )
    out_specs = (
        P(None, "gx", "gz", None),
        P("gx", "gz", None),
        P(None, "gx", "gz", None),
        P("gx", "gz", None),
        P(),
    )
    return jax.shard_map(
        per_device, mesh=mesh, in_specs=in_specs, out_specs=out_specs, check_vma=False
    )
```

```python
import functools
import math

import jax
import jax.numpy as jnp
from jax import lax
from jax.experimental import pallas as pl
from jax.experimental.pallas import tpu as pltpu
from jax.sharding import PartitionSpec as P

ITERS = 2
REACH = 6
PLANE = 4
MESH = pl.DeviceIdType.MESH

unnormalized_weights = [math.exp(-(k * k) / 18.0) for k in range(-REACH, REACH + 1)]
weight_total = sum(unnormalized_weights)
gauss_weights = [value / weight_total for value in unnormalized_weights]
shear_time_increment = 20.0


def bits_of(count):
    assert count & (count - 1) == 0
    return [1 << bit for bit in range(count.bit_length() - 1)]


def kernel(
    gx_count,
    gz_count,
    vel_in,
    pres_in,
    old_in,
    plas_in,
    visc_in,
    weak_in,
    VOUT,
    PR,
    TAU,
    PL,
    peak_out,
    V,
    IN,
    WK,
    PLZ,
    PZH,
    ETA,
    INV,
    COH,
    YM,
    GX,
    GXH,
    SM,
    VZE,
    VZH,
    SX,
    TZ,
    SE,
    ZH,
    XS,
    XH,
    CE,
    CH,
    SEL,
    ZHL,
    XHL,
    RF,
    RZF,
    TR,
    DV,
    TB,
    MOST,
    PK,
    in_sem,
    send_sem,
    recv_sem,
    pk_send,
    pk_recv,
    pair_sem,
    hop_sem,
):
    rows, nz, ny = PR.shape
    gx = lax.axis_index("gx")
    gz = lax.axis_index("gz")
    me = gx * gz_count + gz
    total = gx_count * gz_count
    has = {
        "xl": gx > 0,
        "xh": gx < gx_count - 1,
        "zl": gz > 0,
        "zh": gz < gz_count - 1,
    }
    target = {
        "xl": (gx - 1, gz),
        "xh": (gx + 1, gz),
        "zl": (gx, gz - 1),
        "zh": (gx, gz + 1),
    }
    opposite = {"xl": "xh", "xh": "xl", "zl": "zh", "zh": "zl"}
    corners = [(a, b) for a in ("xl", "xh") for b in ("zl", "zh")]
    for a, b in corners:
        has[a + b] = jnp.logical_and(has[a], has[b])
        target[a + b] = (target[a][0], target[b][1])
        opposite[a + b] = opposite[a] + opposite[b]
    barrier = pltpu.get_barrier_semaphore()

    side_of = gz % 2
    odd = side_of == 1
    even = side_of == 0
    lead = gz + 1 - side_of
    couple = gz // 2

    def flipped(index, bit):
        return index + bit * (1 - 2 * ((index // bit) % 2))

    always = gx >= 0
    rounds = [[(flipped(gx, bit), gz, always)] for bit in bits_of(min(PLANE, gx_count))]
    rounds += [
        [(gx - far, gz, gx >= far), (gx + far, gz, gx < gx_count - far)]
        for far in bits_of(gx_count)
        if far >= PLANE
    ]
    rounds += [[(gx, 2 * flipped(couple, bit) + 1, always)] for bit in bits_of(gz_count // 2)]
    along_gx = len(bits_of(gx_count))
    met = [place for far in rounds[1:3] + rounds[max(along_gx, 3) :] for place in far]

    def signal(sem, place):
        pl.semaphore_signal(sem, inc=1, device_id=place, device_id_type=MESH)

    def one_if(flag):
        return jnp.where(flag, 1, 0)

    VI, PIN = IN.at[0], IN.at[1]
    plas_load = pltpu.make_async_copy(plas_in, PLZ, send_sem.at[6])
    vel_load = pltpu.make_async_copy(vel_in, V.at[:, pl.ds(1, rows)], send_sem.at[2])
    weak_load = pltpu.make_async_copy(weak_in, WK, pk_send)
    rest_loads = [
        pltpu.make_async_copy(visc_in, VI, in_sem),
        pltpu.make_async_copy(pres_in, PIN, in_sem),
        pltpu.make_async_copy(old_in, IN.at[pl.ds(2, 6)], in_sem),
    ]
    all_rest = pltpu.make_async_copy(IN, IN, in_sem)

    @pl.when(odd)
    def _():
        signal(barrier, (gx, gz - 1))

        @pl.when(has["zh"])
        def _():
            signal(barrier, (gx, gz + 1))

    for side in ("xl", "xh"):

        @pl.when(has[side])
        def _(side=side):
            signal(barrier, (target[side][0], lead))

    plas_load.start()

    @pl.when(odd)
    def _():
        for x_place, z_place, there in met:

            @pl.when(there)
            def _(x_place=x_place, z_place=z_place):
                signal(barrier, (x_place, z_place))

    def described(side, source, landing, got, sent):
        number = {"xl": 0, "xh": 1, "zl": 0, "zh": 1}.get(side, 0)
        return pltpu.make_async_remote_copy(
            src_ref=source,
            dst_ref=landing,
            send_sem=send_sem.at[2 * sent + number],
            recv_sem=recv_sem.at[2 * got + number],
            device_id=target[side],
            device_id_type=MESH,
        )

    def start(pairs):
        for side, copy in pairs:

            @pl.when(has[side])
            def _(copy=copy):
                copy.start()

    gx_odd = gx % 2 == 1
    gx_even = gx % 2 == 0

    def start_far(pairs):
        for place, side in ((gx_odd, "xh"), (gx_even, "xl")):

            @pl.when(place)
            def _(side=side):
                start([pair for pair in pairs if pair[0] == side])

    def start_near(pairs):
        for place, side in ((gx_odd, "xl"), (gx_even, "xh")):

            @pl.when(place)
            def _(side=side):
                start([pair for pair in pairs if pair[0] == side])

    has_far = jnp.logical_or(
        jnp.logical_and(gx_odd, has["xh"]), jnp.logical_and(gx_even, has["xl"])
    )

    def wait_sent(pairs):
        for side, copy in pairs:

            @pl.when(has[side])
            def _(copy=copy):
                copy.wait_send()

    def wait_got(pairs):
        for side, copy in pairs:

            @pl.when(has[opposite[side]])
            def _(copy=copy):
                copy.wait_recv()

    def zero(ref):
        ref[...] = jnp.zeros(ref.shape, ref.dtype)

    def zero_unless(side, *refs):
        @pl.when(jnp.logical_not(has[side]))
        def _():
            for ref in refs:
                zero(ref)

    @pl.when(even)
    def _():
        pl.semaphore_wait(barrier, 1 + one_if(has["zl"]))
        signal(pair_sem, (gx, gz + 1))

        @pl.when(has["zl"])
        def _():
            signal(pair_sem, (gx, gz - 1))

    @pl.when(odd)
    def _():
        pl.semaphore_wait(pair_sem, 1 + one_if(has["zh"]))

    pz_copies = [
        ("zh", described("zh", plas_in, PZH.at[0], 0, 0)),
        ("zl", described("zl", plas_in, PZH.at[1], 0, 0)),
    ]
    start(pz_copies)
    vel_load.start()
    for copy in rest_loads:
        copy.start()
    weak_load.start()

    places_a = lax.broadcasted_iota(jnp.int32, (ny, ny), 0)
    places_b = lax.broadcasted_iota(jnp.int32, (ny, ny), 1)
    gap = (places_a - places_b).astype(jnp.float32)
    YM[...] = jnp.where(
        jnp.abs(gap) <= float(REACH), jnp.exp(-gap * gap / 18.0) / weight_total, 0.0
    )
    zero_unless("zl", PZH.at[0])
    zero_unless("zh", PZH.at[1])
    zero_unless("xl", V.at[:, pl.ds(0, 1)], GXH.at[0], XH.at[0], XHL.at[0], RF.at[:, pl.ds(0, 1)])
    zero_unless("xh", V.at[:, pl.ds(rows + 1, 1)], GXH.at[1], XH.at[1], XHL.at[1])
    zero_unless("xh", RF.at[:, pl.ds(rows + 1, 1)])
    zero_unless("zl", VZH.at[0], ZH.at[0], ZHL.at[0], RZF.at[0])
    zero_unless("zh", VZH.at[1], ZH.at[1], ZHL.at[1], RZF.at[1])
    for number, (a, b) in enumerate(corners):
        zero_unless(a + b, CH.at[number])
    for it in range(ITERS):
        zero(SX.at[it, :, pl.ds(0, 1)])
        zero(SX.at[it, :, pl.ds(rows + 1, 1)])

    @pl.when(odd)
    def _():
        greeters = 2 * (one_if(has["xl"]) + one_if(has["xh"]))
        for _, _, there in met:
            greeters = greeters + one_if(there)
        pl.semaphore_wait(barrier, greeters)
        signal(pair_sem, (gx, gz - 1))

    @pl.when(even)
    def _():
        pl.semaphore_wait(pair_sem, 1)

    vel_copies = [
        ("xh", described("xh", vel_in.at[:, pl.ds(rows - 1, 1)], V.at[:, pl.ds(0, 1)], 2, 2)),
        ("xl", described("xl", vel_in.at[:, pl.ds(0, 1)], V.at[:, pl.ds(rows + 1, 1)], 2, 2)),
    ]
    start_far(vel_copies)

    @pl.when(jnp.logical_not(has_far))
    def _():
        start_near(vel_copies)


    def hop_send(k):
        if k < len(rounds):

            @pl.when(odd)
            def _():
                for x_place, z_place, there in rounds[k]:

                    @pl.when(there)
                    def _(x_place=x_place, z_place=z_place):
                        signal(hop_sem.at[k], (x_place, z_place))

    def hop_wait(k):
        if k < len(rounds):

            @pl.when(odd)
            def _():
                expected = 0
                for _, _, there in rounds[k]:
                    expected = expected + one_if(there)
                pl.semaphore_wait(hop_sem.at[k], expected)

    hop_send(0)

    block = rows // 2
    many = (block, nz, ny)

    def over_rows(body, carry=0):
        return lax.fori_loop(0, rows // block, lambda i, state: body(i * block, state), carry)

    def at(x):
        return pl.ds(x, block)

    vel_load.wait()

    def vel_edges(x, carry):
        for c in range(3):
            row = V[c, at(x + 1)]
            VZE[0, c, at(x)] = row[:, 0:1]
            VZE[1, c, at(x)] = row[:, nz - 1 : nz]
        return carry

    over_rows(vel_edges)
    plas_load.wait()
    wait_got(pz_copies)
    vz_copies = [
        ("zh", described("zh", VZE.at[1], VZH.at[0], 1, 1)),
        ("zl", described("zl", VZE.at[0], VZH.at[1], 1, 1)),
    ]
    start(vz_copies)

    def smooth_z(x, carry):
        own, low, high = PLZ[at(x)], PZH[0, at(x)], PZH[1, at(x)]
        sub = lax.broadcasted_iota(jnp.int32, many, 1)
        sum_ = gauss_weights[REACH] * own
        for k in range(1, REACH + 1):
            above = pltpu.roll(jnp.where(sub >= k, own, high), nz - k, 1)
            below = pltpu.roll(jnp.where(sub < nz - k, own, low), k, 1)
            sum_ = sum_ + gauss_weights[REACH + k] * (above + below)
        SM[at(x)] = sum_
        return carry

    over_rows(smooth_z)
    GX[...] = jnp.dot(
        SM[...].reshape(rows * nz, ny),
        YM[...],
        precision=lax.Precision.HIGHEST,
        preferred_element_type=jnp.float32,
    ).reshape(rows, nz, ny)
    plas_copies = [
        ("xh", described("xh", GX.at[pl.ds(rows - REACH, REACH)], GXH.at[0], 3, 3)),
        ("xl", described("xl", GX.at[pl.ds(0, REACH)], GXH.at[1], 3, 3)),
    ]
    start_far(plas_copies)

    @pl.when(has_far)
    def _():
        start_near(vel_copies)

    start_near(plas_copies)
    hop_wait(0)
    hop_send(1)

    all_rest.wait()
    weak_load.wait()

    def prepare(x, carry):
        eta = VI[at(x)]
        eta = shear_time_increment * eta / (eta + shear_time_increment)
        ETA[at(x)] = eta
        INV[at(x)] = 1.0 / (eta + 0.5)
        COH[at(x)] = 0.8660254 - (0.8660254 * 0.6) * WK[at(x)].astype(jnp.float32)
        return carry

    over_rows(prepare)
    for row in range(rows):
        sum_ = gauss_weights[REACH] * GX[row]
        for k in range(1, REACH + 1):
            for other in (row - k, row + k):
                if 0 <= other < rows:
                    sum_ = sum_ + gauss_weights[REACH + k] * GX[other]
        SM[row] = sum_
    for k in range(1, len(rounds) - 1):
        hop_wait(k)
        hop_send(k + 1)

    wait_got(vz_copies)

    def dy(f):
        lane = lax.broadcasted_iota(jnp.int32, f.shape, 2)
        up = jnp.where(lane < ny - 1, pltpu.roll(f, ny - 1, 2), 0.0)
        down = jnp.where(lane > 0, pltpu.roll(f, 1, 2), 0.0)
        return (up - down) * 0.5

    def dz(f, low, high):
        sub = lax.broadcasted_iota(jnp.int32, f.shape, 1)
        up = pltpu.roll(jnp.where(sub >= 1, f, jnp.broadcast_to(high, f.shape)), nz - 1, 1)
        down = pltpu.roll(jnp.where(sub < nz - 1, f, jnp.broadcast_to(low, f.shape)), 1, 1)
        return (up - down) * 0.5

    def dz_inside(f):
        sub = lax.broadcasted_iota(jnp.int32, f.shape, 1)
        up = jnp.where(sub < nz - 1, pltpu.roll(f, nz - 1, 1), 0.0)
        down = jnp.where(sub >= 1, pltpu.roll(f, 1, 1), 0.0)
        return (up - down) * 0.5

    def strains(field, halo, x, size):
        v = [field[c, pl.ds(x + 1, size)] for c in range(3)]
        dx_v = [(field[c, pl.ds(x + 2, size)] - field[c, pl.ds(x, size)]) * 0.5 for c in range(3)]
        dz_v = [dz(f, halo[0, c, pl.ds(x, size)], halo[1, c, pl.ds(x, size)]) for c, f in enumerate(v)]
        dy_v = [dy(f) for f in v]
        div = dx_v[0] + dz_v[1] + dy_v[2]
        third = div * (1.0 / 3.0)
        return (
            dx_v[0] - third,
            dz_v[1] - third,
            dy_v[2] - third,
            0.5 * (dx_v[1] + dz_v[0]),
            0.5 * (dx_v[2] + dy_v[0]),
            0.5 * (dz_v[2] + dy_v[1]),
        ), div

    def second_invariant(trial):
        return jnp.sqrt(
            0.5 * (trial[0] * trial[0] + trial[1] * trial[1] + trial[2] * trial[2])
            + trial[3] * trial[3]
            + trial[4] * trial[4]
            + trial[5] * trial[5]
        )

    def first_trial(x):
        strain, div = strains(V, VZH, x, block)
        quarter = 0.25 * div
        pres = PIN[at(x)] - quarter
        PR[at(x)] = pres
        PIN[at(x)] = pres - quarter
        twice = 2.0 * ETA[at(x)]
        trial = [
            twice * (strain[c] + IN[2 + c, at(x)] * (0.5 / shear_time_increment)) for c in range(6)
        ]
        for c in range(6):
            TAU[c, at(x)] = trial[c]
        TB[at(x)] = second_invariant(trial)

    def in_order(act):
        for place, numbers in ((gx_odd, (1, 0)), (gx_even, (0, 1))):

            @pl.when(place)
            def _(numbers=numbers):
                for number in numbers:
                    act(number, number == numbers[0])

    def one_trial(number, far):
        wait_got(vel_copies[number : number + 1])
        first_trial(number * block)

    in_order(one_trial)
    half = ny // 2 if ny % 256 == 0 else ny

    def stress_rows(it, x, size, pres, trial, tau_ii, strength, plas, edge):
        def at(x):
            return pl.ds(x, size)

        last = it == ITERS - 1
        eta, inv = ETA[at(x)], INV[at(x)]
        yield_f = tau_ii - 0.5 * jnp.maximum(pres, 0.0) - strength
        dlam = jnp.maximum(yield_f, 0.0) * inv
        shrink = 1.0 - eta * dlam / jnp.maximum(tau_ii, 0.5)
        tau = [shrink * value for value in trial]
        PL[at(x)] = plas + dlam
        if last:
            for c in range(6):
                TAU[c, at(x)] = tau[c]
        SX[it, 0, at(x + 1)] = tau[0] - pres
        SX[it, 1, at(x + 1)] = tau[3]
        SX[it, 2, at(x + 1)] = tau[4]
        szz = tau[1] - pres
        TZ[0, at(x)] = szz
        TZ[1, at(x)] = tau[5]
        TZ[2, at(x)] = tau[2] - pres
        for c, f in enumerate((tau[3], szz, tau[5])):
            edge[0, c, at(x)] = f[:, 0:1]
            edge[1, c, at(x)] = f[:, nz - 1 : nz]
        return jnp.max(yield_f, axis=0), jnp.max(eta * shrink, axis=0)

    def forces(it, x, size, diff_z):
        s = [SX[it, c, pl.ds(x + 1, size)] for c in range(3)]
        t = [TZ[c, pl.ds(x, size)] for c in range(3)]
        along_x = [0.5 * (SX[it, c, pl.ds(x + 2, size)] - SX[it, c, pl.ds(x, size)]) for c in range(3)]
        along_z = [diff_z(c, f) for c, f in enumerate((s[1], t[0], t[1]))]
        along_y = [dy(f) for f in (s[2], t[1], t[2])]
        return [along_x[c] + along_z[c] + along_y[c] for c in range(3)]

    def folded(most):
        most = jnp.max(most, axis=0, keepdims=True)
        return jnp.maximum(most[:, :half], most[:, ny - half :])

    def tell(it, place):
        pltpu.make_async_remote_copy(
            src_ref=PK.at[it, me],
            dst_ref=PK.at[it, me],
            send_sem=pk_send,
            recv_sem=pk_recv.at[it],
            device_id=place,
            device_id_type=MESH,
        ).start()

    def tell_all(it):
        parts = 3 if it else 2
        most = [folded(functools.reduce(jnp.maximum, [MOST[i, k] for i in range(parts)])) for k in range(2)]
        PK[it, me] = jnp.concatenate(most, axis=0)
        for dz_ in range(gz_count):
            other_z = gz + dz_
            other_z = jnp.where(other_z >= gz_count, other_z - gz_count, other_z)

            def one(dx_, carry, other_z=other_z):
                other_x = gx + dx_
                tell(it, (jnp.where(other_x >= gx_count, other_x - gx_count, other_x), other_z))
                return carry

            first = 0 if dz_ else 1
            if gx_count <= 16 and gz_count <= 2:
                for dx_ in range(first, gx_count):
                    one(dx_, 0)
            else:
                lax.fori_loop(first, gx_count, one, 0)

    def told(it):
        others = PK.at[it, pl.ds(0, total - 1)]
        pltpu.make_async_copy(others, others, pk_recv.at[it]).wait()
        peaks = jnp.max(PK[it], axis=0)
        step = 0.125 / jnp.max(peaks[1:2], axis=1, keepdims=True)
        return step, jnp.max(peaks[0:1], axis=1, keepdims=True)

    def tell_sent():
        others = PK.at[0, pl.ds(0, total - 1)]
        pltpu.make_async_copy(others, others, pk_send).wait()

    def first_stress(x):
        strength = COH[at(x)] / (1.0 + 2.0 * SM[at(x)])
        COH[at(x)] = strength
        trial = [TAU[c, at(x)] for c in range(6)]
        return stress_rows(0, x, block, PR[at(x)], trial, TB[at(x)], strength, PLZ[at(x)], SE)

    x_copies = [
        ("xh", described("xh", XS.at[1], XH.at[0], 4, 2)),
        ("xl", described("xl", XS.at[0], XH.at[1], 4, 2)),
    ]
    corner_copies = []
    for number, (a, b) in enumerate(corners):
        there = corners.index((opposite[a], opposite[b]))
        corner_copies.append(
            (
                a + b,
                pltpu.make_async_remote_copy(
                    src_ref=CE.at[number],
                    dst_ref=CH.at[there],
                    send_sem=send_sem.at[(2, 3, 6, 7)[number]],
                    recv_sem=recv_sem.at[10 + number],
                    device_id=target[a + b],
                    device_id_type=MESH,
                ),
            )
        )

    def one_side(number, far):
        row = (rows - 1) * number
        wait_got(plas_copies[number : number + 1])
        for beside in range(min(REACH, block)):
            here = beside if number == 0 else rows - 1 - beside
            sum_ = SM[here]
            for k in range(beside + 1, REACH + 1):
                place = REACH + beside - k if number == 0 else k - 1 - beside
                sum_ = sum_ + gauss_weights[REACH + k] * GXH[number, place]
            SM[here] = sum_
        MOST[number, 0], MOST[number, 1] = first_stress(number * block)
        force = forces(0, row, 1, lambda c, f: dz_inside(f))
        for c in range(3):
            XS[number, c] = SX[0, c, row + 1]
            XS[number, 3 + c] = force[c][0]
        for layer in range(2):
            where = 2 * number + layer
            place = (nz - 1) * layer
            for c in range(3):
                CE[where, c] = SX[0, c, row + 1, place : place + 1]
                CE[where, 3 + c] = SE[layer, c, row]
        if far:
            wait_sent(vel_copies)
            start(x_copies[1 - number : 2 - number])
        if far:
            if len(rounds) > 1:
                hop_wait(len(rounds) - 1)

            @pl.when(odd)
            def _():
                signal(pair_sem, (gx, gz - 1))

    in_order(one_side)
    @pl.when(even)
    def _():
        pl.semaphore_wait(pair_sem, 1)

    tell_all(0)
    start_near(x_copies)
    wait_sent(vz_copies)
    wait_sent(plas_copies)
    start(corner_copies)

    def own_force(x, carry):
        force = forces(0, x, block, lambda c, f: dz_inside(f))
        for c in range(3):
            RF[c, at(x + 1)] = force[c]
            SE[0, 3 + c, at(x)] = force[c][:, 0:1]
            SE[1, 3 + c, at(x)] = force[c][:, nz - 1 : nz]
        return carry

    over_rows(own_force)
    wait_sent(pz_copies)
    z_copies = [
        ("zh", described("zh", SE.at[1], ZH.at[0], 0, 0)),
        ("zl", described("zl", SE.at[0], ZH.at[1], 0, 0)),
    ]
    start(z_copies)
    wait_got(z_copies)

    def add_z(x, carry):
        sub = lax.broadcasted_iota(jnp.int32, many, 1)
        for c in range(3):
            high = jnp.where(sub == nz - 1, jnp.broadcast_to(ZH[1, c, at(x)], many), 0.0)
            low = jnp.where(sub == 0, jnp.broadcast_to(ZH[0, c, at(x)], many), 0.0)
            RF[c, at(x + 1)] = RF[c, at(x + 1)] + 0.5 * (high - low)
        return carry

    def second_trial(x, size):
        strain, div = strains(RF, RZF, x, size)
        twice = 2.0 * ETA[pl.ds(x, size)]
        for c in range(6):
            TR[c, pl.ds(x, size)] = twice * strain[c]
        DV[pl.ds(x, size)] = 0.25 * div

    over_rows(add_z)

    @pl.when(has["zl"])
    def _():
        RZF[0] = ZH[0, 3:6] + 0.5 * SE[0, 0:3]

    @pl.when(has["zh"])
    def _():
        RZF[1] = ZH[1, 3:6] - 0.5 * SE[1, 0:3]

    inside = rows - 4
    if inside > 0:
        size = next(size for size in (6, 4, 3, 2, 1) if inside % size == 0)

        def inside_trial(i, carry):
            second_trial(2 + i * size, size)
            return carry

        lax.fori_loop(0, inside // size, inside_trial, 0)

    step, top = told(0)
    tell_sent()
    tops = [top]

    def second_stress(x, size):
        here = pl.ds(x, size)
        pres = PIN[here] - step * DV[here]
        PR[here] = pres
        trial = [TAU[c, here] + step * TR[c, here] for c in range(6)]
        return stress_rows(
            1, x, size, pres, trial, second_invariant(trial), COH[here], PL[here], SEL
        )

    lowest = jnp.full((nz, ny), -jnp.inf, jnp.float32)
    most = (lowest, lowest)
    if inside > 0:

        def inside_stress(i, most):
            f, eta = second_stress(2 + i * size, size)
            return jnp.maximum(most[0], f), jnp.maximum(most[1], eta)

        most = lax.fori_loop(0, inside // size, inside_stress, most)
    MOST[2, 0], MOST[2, 1] = most

    wait_got(x_copies)
    wait_got(corner_copies)
    for number, side, row in ((0, "xl", 0), (1, "xh", rows - 1)):
        sign = 0.5 - number
        beyond = row + 2 * number
        for c in range(3):
            RF[c, row + 1] = RF[c, row + 1] - sign * XH[number, c]

        @pl.when(has[side])
        def _(number=number, sign=sign, row=row, beyond=beyond):
            sub = lax.broadcasted_iota(jnp.int32, (nz, ny), 0)
            for c in range(3):
                low = jnp.where(sub == 0, jnp.broadcast_to(CH[2 * number, 3 + c], (nz, ny)), 0.0)
                high = jnp.where(sub == nz - 1, jnp.broadcast_to(CH[2 * number + 1, 3 + c], (nz, ny)), 0.0)
                RF[c, beyond] = XH[number, 3 + c] + sign * SX[0, c, row + 1] + 0.5 * (high - low)

        for layer in range(2):
            for c in range(3):
                RZF[layer, c, row] = RZF[layer, c, row] - sign * CH[2 * number + layer, c]
    if inside > 0:
        second_trial(0, 2)
        second_trial(rows - 2, 2)
    else:
        second_trial(0, rows)

    for i, x in enumerate((0, rows - 2) if inside > 0 else (0,)):
        MOST[i, 0], MOST[i, 1] = second_stress(x, 2 if inside > 0 else rows)
    if inside <= 0:
        MOST[1, 0], MOST[1, 1] = lowest, lowest
    tell_all(1)
    wait_sent(corner_copies)
    sx_copies = [
        ("xh", described("xh", SX.at[1, :, pl.ds(rows, 1)], XHL.at[0], 2, 3)),
        ("xl", described("xl", SX.at[1, :, pl.ds(1, 1)], XHL.at[1], 2, 3)),
    ]
    start(sx_copies[1:])
    start(sx_copies[:1])
    sz_copies = [
        ("zh", described("zh", SEL.at[1], ZHL.at[0], 1, 1)),
        ("zl", described("zl", SEL.at[0], ZHL.at[1], 1, 1)),
    ]
    start(sz_copies)

    def moved(x, carry):
        for c in range(3):
            V[c, at(x + 1)] = V[c, at(x + 1)] + step * RF[c, at(x + 1)]
        return carry

    over_rows(moved)
    wait_got(sz_copies)

    def last_force(x, carry):
        def diff_z(c, f):
            return dz(f, ZHL[0, c, at(x)], ZHL[1, c, at(x)])

        force = forces(1, x, block, diff_z)
        for c in range(3):
            RF[c, at(x + 1)] = force[c]
        return carry

    over_rows(last_force)
    wait_got(sx_copies)
    for c in range(3):
        RF[c, 1] = RF[c, 1] - 0.5 * XHL[0, c, 0]
        RF[c, rows] = RF[c, rows] + 0.5 * XHL[1, c, 0]
    step, top = told(1)
    tops.append(top)

    def last_velocity(x, carry):
        for c in range(3):
            VOUT[c, at(x)] = V[c, at(x + 1)] + step * RF[c, at(x + 1)]
        return carry

    over_rows(last_velocity)
    peak_out[...] = jnp.concatenate(tops, axis=1)[0]
    wait_sent(x_copies + z_copies + sx_copies + sz_copies)
    tell_sent()


def store_kernel(*refs):
    held, out, sem = refs[:5], refs[5:10], refs[10]
    copies = [pltpu.make_async_copy(a, b, sem.at[i]) for i, (a, b) in enumerate(zip(held, out))]
    for copy in copies:
        copy.start()
    for copy in copies:
        copy.wait()


def solution(mesh):
    gx_count, gz_count = mesh.shape["gx"], mesh.shape["gz"]
    total = gx_count * gz_count

    def per_device(velocity, pressure, stress_old, plastic, viscosity, weak_seed):
        rows, nz, ny = pressure.shape
        cells = (rows, nz, ny)
        f32 = jnp.float32
        vm = lambda *shape: pltpu.VMEM(shape, f32)
        hops = len(bits_of(gx_count)) + len(bits_of(gz_count // 2))
        anywhere = pl.BlockSpec(memory_space=pl.ANY)
        shapes = (velocity.shape, pressure.shape, stress_old.shape, plastic.shape)
        held = pl.pallas_call(
            functools.partial(kernel, gx_count, gz_count),
            out_shape=tuple(vm(*shape) for shape in shapes + ((ITERS,),)),
            in_specs=[anywhere] * 6,
            out_specs=(pl.BlockSpec(memory_space=pltpu.VMEM),) * 5,
            scratch_shapes=[
                vm(3, rows + 2, nz, ny),
                vm(8, *cells),
                pltpu.VMEM(cells, jnp.int32),
                vm(*cells),
                vm(2, *cells),
                vm(*cells),
                vm(*cells),
                vm(*cells),
                vm(ny, ny),
                vm(*cells),
                vm(2, REACH, nz, ny),
                vm(*cells),
                vm(2, 3, rows, 1, ny),
                vm(2, 3, rows, 1, ny),
                vm(ITERS, 3, rows + 2, nz, ny),
                vm(3, *cells),
                vm(2, 6, rows, 1, ny),
                vm(2, 6, rows, 1, ny),
                vm(2, 6, nz, ny),
                vm(2, 6, nz, ny),
                vm(4, 6, 1, ny),
                vm(4, 6, 1, ny),
                vm(2, 3, rows, 1, ny),
                vm(2, 3, rows, 1, ny),
                vm(2, 3, 1, nz, ny),
                vm(3, rows + 2, nz, ny),
                vm(2, 3, rows, 1, ny),
                vm(6, *cells),
                vm(*cells),
                vm(*cells),
                vm(3, 2, nz, ny),
                vm(ITERS, total, 2, ny // 2 if ny % 256 == 0 else ny),
                pltpu.SemaphoreType.DMA,
                pltpu.SemaphoreType.DMA((8,)),
                pltpu.SemaphoreType.DMA((14,)),
                pltpu.SemaphoreType.DMA,
                pltpu.SemaphoreType.DMA((ITERS,)),
                pltpu.SemaphoreType.REGULAR,
                pltpu.SemaphoreType.REGULAR((hops,)),
            ],
            compiler_params=pltpu.CompilerParams(collective_id=0, has_side_effects=True),
        )(velocity, pressure, stress_old, plastic, viscosity, weak_seed)
        held = [pltpu.with_memory_space_constraint(array, pltpu.VMEM) for array in held]
        return pl.pallas_call(
            store_kernel,
            out_shape=tuple(jax.ShapeDtypeStruct(shape, f32) for shape in shapes)
            + (jax.ShapeDtypeStruct((ITERS,), f32),),
            in_specs=[anywhere] * 5,
            out_specs=(anywhere,) * 5,
            scratch_shapes=[pltpu.SemaphoreType.DMA((5,))],
        )(*held)

    in_specs = (
        P(None, "gx", "gz", None),
        P("gx", "gz", None),
        P(None, "gx", "gz", None),
        P("gx", "gz", None),
        P("gx", "gz", None),
        P("gx", "gz", None),
    )
    out_specs = (
        P(None, "gx", "gz", None),
        P("gx", "gz", None),
        P(None, "gx", "gz", None),
        P("gx", "gz", None),
        P(),
    )
    return jax.shard_map(
        per_device, mesh=mesh, in_specs=in_specs, out_specs=out_specs, check_vma=False
    )
```

```python
import functools
import math

import jax
import jax.numpy as jnp
from jax import lax
from jax.experimental import pallas as pl
from jax.experimental.pallas import tpu as pltpu
from jax.sharding import PartitionSpec as P

ITERS = 2
REACH = 6
PLANE = 4
MESH = pl.DeviceIdType.MESH

unnormalized_weights = [math.exp(-(k * k) / 18.0) for k in range(-REACH, REACH + 1)]
weight_total = sum(unnormalized_weights)
gauss_weights = [value / weight_total for value in unnormalized_weights]
shear_time_increment = 20.0


def bits_of(count):
    assert count & (count - 1) == 0
    return [1 << bit for bit in range(count.bit_length() - 1)]


def step_of(peaks):
    lane = lax.broadcasted_iota(jnp.int32, peaks.shape, 1)
    return 0.125 / jnp.max(jnp.where(lane < peaks.shape[1] // 2, -jnp.inf, peaks), axis=1, keepdims=True)


def top_of(peaks):
    lane = lax.broadcasted_iota(jnp.int32, peaks.shape, 1)
    return jnp.max(jnp.where(lane < peaks.shape[1] // 2, peaks, -jnp.inf), axis=1, keepdims=True)


def sides_of(count):
    return min(count - 1, 2)


def sems_of(z_sides):
    return 2 * z_sides + 4, 2 * z_sides + 6 + 2 * z_sides


def kernel(
    gx_count,
    gz_count,
    vel_in,
    pres_in,
    old_in,
    plas_in,
    visc_in,
    weak_in,
    MOVED,
    PR,
    TAU,
    PL,
    FORCE,
    PEAKS,
    V,
    IN,
    WK,
    PLZ,
    PZH,
    ETA,
    INV,
    COH,
    YM,
    GX,
    GXH,
    SM,
    VZE,
    VZH,
    SX,
    TZ,
    SE,
    ZH,
    XS,
    XH,
    CE,
    CH,
    SEL,
    ZHL,
    XHL,
    RF,
    RZF,
    TR,
    DV,
    TB,
    MOST,
    PK,
    in_sem,
    send_sem,
    recv_sem,
    pk_send,
    pk_recv,
    pair_sem,
    hop_sem,
):
    rows, nz, ny = PR.shape
    gx = lax.axis_index("gx")
    gz = lax.axis_index("gz")
    me = gx * gz_count + gz
    total = gx_count * gz_count
    has = {
        "xl": gx > 0,
        "xh": gx < gx_count - 1,
        "zl": gz > 0,
        "zh": gz < gz_count - 1,
    }
    target = {
        "xl": (gx - 1, gz),
        "xh": (gx + 1, gz),
        "zl": (gx, gz - 1),
        "zh": (gx, gz + 1),
    }
    opposite = {"xl": "xh", "xh": "xl", "zl": "zh", "zh": "zl"}
    corners = [(a, b) for a in ("xl", "xh") for b in ("zl", "zh")]
    for a, b in corners:
        has[a + b] = jnp.logical_and(has[a], has[b])
        target[a + b] = (target[a][0], target[b][1])
        opposite[a + b] = opposite[a] + opposite[b]
    barrier = pltpu.get_barrier_semaphore()

    side_of = gz % 2
    odd = side_of == 1
    even = side_of == 0
    lead = gz + 1 - side_of
    couple = gz // 2

    def flipped(index, bit):
        return index + bit * (1 - 2 * ((index // bit) % 2))

    always = gx >= 0
    rounds = [[(flipped(gx, bit), gz, always)] for bit in bits_of(min(PLANE, gx_count))]
    rounds += [
        [(gx - far, gz, gx >= far), (gx + far, gz, gx < gx_count - far)]
        for far in bits_of(gx_count)
        if far >= PLANE
    ]
    rounds += [[(gx, 2 * flipped(couple, bit) + 1, always)] for bit in bits_of(gz_count // 2)]
    along_gx = len(bits_of(gx_count))
    met = [place for far in rounds[1:3] + rounds[max(along_gx, 3) :] for place in far]

    def signal(sem, place):
        pl.semaphore_signal(sem, inc=1, device_id=place, device_id_type=MESH)

    def one_if(flag):
        return jnp.where(flag, 1, 0)

    z_sides = sides_of(gz_count)
    VI, PIN = IN.at[0], IN.at[1]
    plas_load = pltpu.make_async_copy(plas_in, PLZ, send_sem.at[sems_of(z_sides)[0] - 2])
    vel_load = pltpu.make_async_copy(vel_in, V.at[:, pl.ds(1, rows)], send_sem.at[z_sides])
    weak_load = pltpu.make_async_copy(weak_in, WK, pk_send)
    rest_loads = [
        pltpu.make_async_copy(visc_in, VI, in_sem),
        pltpu.make_async_copy(pres_in, PIN, in_sem),
        pltpu.make_async_copy(old_in, IN.at[pl.ds(2, 6)], in_sem),
    ]
    all_rest = pltpu.make_async_copy(IN, IN, in_sem)

    for side in ("xl", "xh"):

        @pl.when(has[side])
        def _(side=side):
            signal(barrier, (target[side][0], lead))

    @pl.when(odd)
    def _():
        signal(barrier, (gx, gz - 1))

        @pl.when(has["zh"])
        def _():
            signal(barrier, (gx, gz + 1))

    plas_load.start()

    @pl.when(odd)
    def _():
        for x_place, z_place, there in met:

            @pl.when(there)
            def _(x_place=x_place, z_place=z_place):
                signal(barrier, (x_place, z_place))

    def slot(group):
        return group * z_sides if group < 2 else 2 * z_sides + 2 * (group - 2)

    corner_sent = (slot(1), slot(1) + 1, slot(3), slot(3) + 1) if z_sides == 2 else (slot(1), slot(1), slot(3), slot(3))

    def described(side, source, landing, got, sent):
        number = {"xl": 0, "xh": 1, "zl": 0, "zh": z_sides - 1}[side]
        return pltpu.make_async_remote_copy(
            src_ref=source,
            dst_ref=landing,
            send_sem=send_sem.at[slot(sent) + number],
            recv_sem=recv_sem.at[slot(got) + number],
            device_id=target[side],
            device_id_type=MESH,
        )

    def start(pairs):
        for side, copy in pairs:

            @pl.when(has[side])
            def _(copy=copy):
                copy.start()

    gx_odd = gx % 2 == 1
    gx_even = gx % 2 == 0

    def start_far(pairs):
        for place, side in ((gx_odd, "xh"), (gx_even, "xl")):

            @pl.when(place)
            def _(side=side):
                start([pair for pair in pairs if pair[0] == side])

    def start_near(pairs):
        for place, side in ((gx_odd, "xl"), (gx_even, "xh")):

            @pl.when(place)
            def _(side=side):
                start([pair for pair in pairs if pair[0] == side])

    has_far = jnp.logical_or(
        jnp.logical_and(gx_odd, has["xh"]), jnp.logical_and(gx_even, has["xl"])
    )

    def wait_sent(pairs):
        for side, copy in pairs:

            @pl.when(has[side])
            def _(copy=copy):
                copy.wait_send()

    def wait_got(pairs):
        for side, copy in pairs:

            @pl.when(has[opposite[side]])
            def _(copy=copy):
                copy.wait_recv()

    def zero(ref):
        ref[...] = jnp.zeros(ref.shape, ref.dtype)

    def zero_unless(side, *refs):
        @pl.when(jnp.logical_not(has[side]))
        def _():
            for ref in refs:
                zero(ref)

    @pl.when(even)
    def _():
        pl.semaphore_wait(barrier, 1 + one_if(has["zl"]))
        signal(pair_sem, (gx, gz + 1))

        @pl.when(has["zl"])
        def _():
            signal(pair_sem, (gx, gz - 1))

    @pl.when(odd)
    def _():
        pl.semaphore_wait(pair_sem, 1 + one_if(has["zh"]))

    pz_copies = [
        ("zh", described("zh", plas_in, PZH.at[0], 0, 0)),
        ("zl", described("zl", plas_in, PZH.at[1], 0, 0)),
    ]
    start(pz_copies)
    vel_load.start()
    for copy in rest_loads:
        copy.start()
    weak_load.start()

    places_a = lax.broadcasted_iota(jnp.int32, (ny, ny), 0)
    places_b = lax.broadcasted_iota(jnp.int32, (ny, ny), 1)
    gap = (places_a - places_b).astype(jnp.float32)
    YM[...] = jnp.where(
        jnp.abs(gap) <= float(REACH), jnp.exp(-gap * gap / 18.0) / weight_total, 0.0
    )
    zero_unless("zl", PZH.at[0])
    zero_unless("zh", PZH.at[1])
    zero_unless("xl", V.at[:, pl.ds(0, 1)], GXH.at[0], XH.at[0], XHL.at[0], RF.at[:, pl.ds(0, 1)])
    zero_unless("xh", V.at[:, pl.ds(rows + 1, 1)], GXH.at[1], XH.at[1], XHL.at[1])
    zero_unless("xh", RF.at[:, pl.ds(rows + 1, 1)])
    zero_unless("zl", VZH.at[0], ZH.at[0], ZHL.at[0], RZF.at[0])
    zero_unless("zh", VZH.at[1], ZH.at[1], ZHL.at[1], RZF.at[1])
    for number, (a, b) in enumerate(corners):
        zero_unless(a + b, CH.at[number])
    for it in range(ITERS):
        zero(SX.at[it, :, pl.ds(0, 1)])
        zero(SX.at[it, :, pl.ds(rows + 1, 1)])

    @pl.when(odd)
    def _():
        greeters = 2 * (one_if(has["xl"]) + one_if(has["xh"]))
        for _, _, there in met:
            greeters = greeters + one_if(there)
        pl.semaphore_wait(barrier, greeters)
        signal(pair_sem, (gx, gz - 1))

    @pl.when(even)
    def _():
        pl.semaphore_wait(pair_sem, 1)

    vel_copies = [
        ("xh", described("xh", vel_in.at[:, pl.ds(rows - 1, 1)], V.at[:, pl.ds(0, 1)], 2, 2)),
        ("xl", described("xl", vel_in.at[:, pl.ds(0, 1)], V.at[:, pl.ds(rows + 1, 1)], 2, 2)),
    ]
    start_far(vel_copies)

    @pl.when(jnp.logical_not(has_far))
    def _():
        start_near(vel_copies)


    def hop_send(k):
        if k < len(rounds):

            @pl.when(odd)
            def _():
                for x_place, z_place, there in rounds[k]:

                    @pl.when(there)
                    def _(x_place=x_place, z_place=z_place):
                        signal(hop_sem.at[k], (x_place, z_place))

    def hop_wait(k):
        if k < len(rounds):

            @pl.when(odd)
            def _():
                expected = 0
                for _, _, there in rounds[k]:
                    expected = expected + one_if(there)
                pl.semaphore_wait(hop_sem.at[k], expected)

    hop_send(0)

    block = rows // 2
    many = (block, nz, ny)

    def over_rows(body, carry=0):
        return lax.fori_loop(0, rows // block, lambda i, state: body(i * block, state), carry)

    def at(x):
        return pl.ds(x, block)

    vel_load.wait()

    def vel_edges(x, carry):
        for c in range(3):
            row = V[c, at(x + 1)]
            VZE[0, c, at(x)] = row[:, 0:1]
            VZE[1, c, at(x)] = row[:, nz - 1 : nz]
        return carry

    over_rows(vel_edges)
    plas_load.wait()
    wait_got(pz_copies)
    vz_copies = [
        ("zh", described("zh", VZE.at[1], VZH.at[0], 1, 1)),
        ("zl", described("zl", VZE.at[0], VZH.at[1], 1, 1)),
    ]
    start(vz_copies)

    def smooth_z(x, carry):
        own, low, high = PLZ[at(x)], PZH[0, at(x)], PZH[1, at(x)]
        sub = lax.broadcasted_iota(jnp.int32, many, 1)
        sum_ = gauss_weights[REACH] * own
        for k in range(1, REACH + 1):
            above = pltpu.roll(jnp.where(sub >= k, own, high), nz - k, 1)
            below = pltpu.roll(jnp.where(sub < nz - k, own, low), k, 1)
            sum_ = sum_ + gauss_weights[REACH + k] * (above + below)
        SM[at(x)] = sum_
        return carry

    over_rows(smooth_z)
    GX[...] = jnp.dot(
        SM[...].reshape(rows * nz, ny),
        YM[...],
        precision=lax.Precision.HIGHEST,
        preferred_element_type=jnp.float32,
    ).reshape(rows, nz, ny)
    plas_copies = [
        ("xh", described("xh", GX.at[pl.ds(rows - REACH, REACH)], GXH.at[0], 3, 3)),
        ("xl", described("xl", GX.at[pl.ds(0, REACH)], GXH.at[1], 3, 3)),
    ]
    start_far(plas_copies)

    @pl.when(has_far)
    def _():
        start_near(vel_copies)

    start_near(plas_copies)
    hop_wait(0)
    hop_send(1)

    all_rest.wait()
    weak_load.wait()

    def prepare(x, carry):
        eta = VI[at(x)]
        eta = shear_time_increment * eta / (eta + shear_time_increment)
        ETA[at(x)] = eta
        INV[at(x)] = 1.0 / (eta + 0.5)
        COH[at(x)] = 0.8660254 - (0.8660254 * 0.6) * WK[at(x)].astype(jnp.float32)
        return carry

    over_rows(prepare)
    for row in range(rows):
        sum_ = gauss_weights[REACH] * GX[row]
        for k in range(1, REACH + 1):
            for other in (row - k, row + k):
                if 0 <= other < rows:
                    sum_ = sum_ + gauss_weights[REACH + k] * GX[other]
        SM[row] = sum_
    for k in range(1, len(rounds) - 1):
        hop_wait(k)
        hop_send(k + 1)

    wait_got(vz_copies)

    def dy(f):
        lane = lax.broadcasted_iota(jnp.int32, f.shape, 2)
        up = jnp.where(lane < ny - 1, pltpu.roll(f, ny - 1, 2), 0.0)
        down = jnp.where(lane > 0, pltpu.roll(f, 1, 2), 0.0)
        return (up - down) * 0.5

    def dz(f, low, high):
        sub = lax.broadcasted_iota(jnp.int32, f.shape, 1)
        up = pltpu.roll(jnp.where(sub >= 1, f, jnp.broadcast_to(high, f.shape)), nz - 1, 1)
        down = pltpu.roll(jnp.where(sub < nz - 1, f, jnp.broadcast_to(low, f.shape)), 1, 1)
        return (up - down) * 0.5

    def dz_inside(f):
        sub = lax.broadcasted_iota(jnp.int32, f.shape, 1)
        up = jnp.where(sub < nz - 1, pltpu.roll(f, nz - 1, 1), 0.0)
        down = jnp.where(sub >= 1, pltpu.roll(f, 1, 1), 0.0)
        return (up - down) * 0.5

    def strains(field, halo, x, size):
        v = [field[c, pl.ds(x + 1, size)] for c in range(3)]
        dx_v = [(field[c, pl.ds(x + 2, size)] - field[c, pl.ds(x, size)]) * 0.5 for c in range(3)]
        dz_v = [dz(f, halo[0, c, pl.ds(x, size)], halo[1, c, pl.ds(x, size)]) for c, f in enumerate(v)]
        dy_v = [dy(f) for f in v]
        div = dx_v[0] + dz_v[1] + dy_v[2]
        third = div * (1.0 / 3.0)
        return (
            dx_v[0] - third,
            dz_v[1] - third,
            dy_v[2] - third,
            0.5 * (dx_v[1] + dz_v[0]),
            0.5 * (dx_v[2] + dy_v[0]),
            0.5 * (dz_v[2] + dy_v[1]),
        ), div

    def second_invariant(trial):
        return jnp.sqrt(
            0.5 * (trial[0] * trial[0] + trial[1] * trial[1] + trial[2] * trial[2])
            + trial[3] * trial[3]
            + trial[4] * trial[4]
            + trial[5] * trial[5]
        )

    def first_trial(x):
        strain, div = strains(V, VZH, x, block)
        quarter = 0.25 * div
        pres = PIN[at(x)] - quarter
        PR[at(x)] = pres
        PIN[at(x)] = pres - quarter
        twice = 2.0 * ETA[at(x)]
        trial = [
            twice * (strain[c] + IN[2 + c, at(x)] * (0.5 / shear_time_increment)) for c in range(6)
        ]
        for c in range(6):
            TAU[c, at(x)] = trial[c]
        TB[at(x)] = second_invariant(trial)

    def in_order(act):
        for place, numbers in ((gx_odd, (1, 0)), (gx_even, (0, 1))):

            @pl.when(place)
            def _(numbers=numbers):
                for number in numbers:
                    act(number, number == numbers[0])

    def one_trial(number, far):
        wait_got(vel_copies[number : number + 1])
        first_trial(number * block)

    in_order(one_trial)
    half = ny // 2 if ny % 256 == 0 else ny

    def stress_rows(it, x, size, pres, trial, tau_ii, strength, plas, edge):
        def at(x):
            return pl.ds(x, size)

        last = it == ITERS - 1
        eta, inv = ETA[at(x)], INV[at(x)]
        yield_f = tau_ii - 0.5 * jnp.maximum(pres, 0.0) - strength
        dlam = jnp.maximum(yield_f, 0.0) * inv
        shrink = 1.0 - eta * dlam / jnp.maximum(tau_ii, 0.5)
        tau = [shrink * value for value in trial]
        PL[at(x)] = plas + dlam
        if last:
            for c in range(6):
                TAU[c, at(x)] = tau[c]
        SX[it, 0, at(x + 1)] = tau[0] - pres
        SX[it, 1, at(x + 1)] = tau[3]
        SX[it, 2, at(x + 1)] = tau[4]
        szz = tau[1] - pres
        TZ[0, at(x)] = szz
        TZ[1, at(x)] = tau[5]
        TZ[2, at(x)] = tau[2] - pres
        for c, f in enumerate((tau[3], szz, tau[5])):
            edge[0, c, at(x)] = f[:, 0:1]
            edge[1, c, at(x)] = f[:, nz - 1 : nz]
        return jnp.max(yield_f, axis=0), jnp.max(eta * shrink, axis=0)

    def forces(it, x, size, diff_z):
        s = [SX[it, c, pl.ds(x + 1, size)] for c in range(3)]
        t = [TZ[c, pl.ds(x, size)] for c in range(3)]
        along_x = [0.5 * (SX[it, c, pl.ds(x + 2, size)] - SX[it, c, pl.ds(x, size)]) for c in range(3)]
        along_z = [diff_z(c, f) for c, f in enumerate((s[1], t[0], t[1]))]
        along_y = [dy(f) for f in (s[2], t[1], t[2])]
        return [along_x[c] + along_z[c] + along_y[c] for c in range(3)]

    def folded(most):
        return jnp.maximum(most[:, :half], most[:, ny - half :])

    def tell(it, place):
        pltpu.make_async_remote_copy(
            src_ref=PK.at[it, me],
            dst_ref=PK.at[it, me],
            send_sem=pk_send,
            recv_sem=pk_recv.at[it],
            device_id=place,
            device_id_type=MESH,
        ).start()

    turned = {bit: flipped(gx, bit) - gx for bit in bits_of(gx_count)}

    def tell_all(it):
        parts = 3 if it else 2
        most_f, most_eta = [
            folded(functools.reduce(jnp.maximum, [MOST[i, k] for i in range(parts)])) for k in range(2)
        ]
        lane = lax.broadcasted_iota(jnp.int32, (nz, half), 1)
        most_f = jnp.maximum(most_f, pltpu.roll(most_f, half // 2, 1))
        most_eta = jnp.maximum(most_eta, pltpu.roll(most_eta, half // 2, 1))
        PK[it, me] = jnp.max(jnp.where(lane < half // 2, most_f, most_eta), axis=0, keepdims=True)
        if gx_count <= 16 and gz_count <= 2:
            for flips in reversed(range(1, total)):
                x_place, z_place = gx, gz
                for bit in bits_of(gx_count):
                    if flips // gz_count & bit:
                        x_place = x_place + turned[bit]
                if flips % gz_count:
                    z_place = flipped(gz, 1)
                tell(it, (x_place, z_place))
        else:
            for dz_ in range(gz_count):
                other_z = gz + dz_
                other_z = jnp.where(other_z >= gz_count, other_z - gz_count, other_z)

                def one(dx_, carry, other_z=other_z):
                    other_x = gx + dx_
                    tell(it, (jnp.where(other_x >= gx_count, other_x - gx_count, other_x), other_z))
                    return carry

                lax.fori_loop(0 if dz_ else 1, gx_count, one, 0)

    def told(it):
        others = PK.at[it, pl.ds(0, total - 1)]
        pltpu.make_async_copy(others, others, pk_recv.at[it]).wait()
        PEAKS[it] = jnp.max(PK[it], axis=0)

    def tell_sent():
        others = PK.at[0, pl.ds(0, total - 1)]
        pltpu.make_async_copy(others, others, pk_send).wait()

    def first_stress(x):
        strength = COH[at(x)] / (1.0 + 2.0 * SM[at(x)])
        COH[at(x)] = strength
        trial = [TAU[c, at(x)] for c in range(6)]
        return stress_rows(0, x, block, PR[at(x)], trial, TB[at(x)], strength, PLZ[at(x)], SE)

    x_copies = [
        ("xh", described("xh", XS.at[1], XH.at[0], 4, 2)),
        ("xl", described("xl", XS.at[0], XH.at[1], 4, 2)),
    ]
    corner_copies = []
    for number, (a, b) in enumerate(corners):
        there = corners.index((opposite[a], opposite[b]))
        corner_copies.append(
            (
                a + b,
                pltpu.make_async_remote_copy(
                    src_ref=CE.at[number],
                    dst_ref=CH.at[there],
                    send_sem=send_sem.at[corner_sent[number]],
                    recv_sem=recv_sem.at[slot(5) + (number if z_sides == 2 else number // 2)],
                    device_id=target[a + b],
                    device_id_type=MESH,
                ),
            )
        )

    def one_side(number, far):
        row = (rows - 1) * number
        wait_got(plas_copies[number : number + 1])
        for beside in range(min(REACH, block)):
            here = beside if number == 0 else rows - 1 - beside
            sum_ = SM[here]
            for k in range(beside + 1, REACH + 1):
                place = REACH + beside - k if number == 0 else k - 1 - beside
                sum_ = sum_ + gauss_weights[REACH + k] * GXH[number, place]
            SM[here] = sum_
        MOST[number, 0], MOST[number, 1] = first_stress(number * block)
        force = forces(0, row, 1, lambda c, f: dz_inside(f))
        for c in range(3):
            XS[number, c] = SX[0, c, row + 1]
            XS[number, 3 + c] = force[c][0]
        for layer in range(2):
            where = 2 * number + layer
            place = (nz - 1) * layer
            for c in range(3):
                CE[where, c] = SX[0, c, row + 1, place : place + 1]
                CE[where, 3 + c] = SE[layer, c, row]
        if far:
            wait_sent(vel_copies)
            start(x_copies[1 - number : 2 - number])
        if far:
            if len(rounds) > 1:
                hop_wait(len(rounds) - 1)

            @pl.when(odd)
            def _():
                signal(pair_sem, (gx, gz - 1))

    in_order(one_side)
    @pl.when(even)
    def _():
        pl.semaphore_wait(pair_sem, 1)

    tell_all(0)
    start_near(x_copies)
    wait_sent(vz_copies)
    wait_sent(plas_copies)
    start(corner_copies)

    def own_force(x, carry):
        force = forces(0, x, block, lambda c, f: dz_inside(f))
        for c in range(3):
            RF[c, at(x + 1)] = force[c]
            SE[0, 3 + c, at(x)] = force[c][:, 0:1]
            SE[1, 3 + c, at(x)] = force[c][:, nz - 1 : nz]
        return carry

    over_rows(own_force)
    wait_sent(pz_copies)
    z_copies = [
        ("zh", described("zh", SE.at[1], ZH.at[0], 0, 0)),
        ("zl", described("zl", SE.at[0], ZH.at[1], 0, 0)),
    ]
    start(z_copies)
    wait_got(z_copies)

    def add_z(x, carry):
        sub = lax.broadcasted_iota(jnp.int32, many, 1)
        for c in range(3):
            high = jnp.where(sub == nz - 1, jnp.broadcast_to(ZH[1, c, at(x)], many), 0.0)
            low = jnp.where(sub == 0, jnp.broadcast_to(ZH[0, c, at(x)], many), 0.0)
            RF[c, at(x + 1)] = RF[c, at(x + 1)] + 0.5 * (high - low)
        return carry

    def second_trial(x, size):
        strain, div = strains(RF, RZF, x, size)
        twice = 2.0 * ETA[pl.ds(x, size)]
        for c in range(6):
            TR[c, pl.ds(x, size)] = twice * strain[c]
        DV[pl.ds(x, size)] = 0.25 * div

    over_rows(add_z)

    @pl.when(has["zl"])
    def _():
        RZF[0] = ZH[0, 3:6] + 0.5 * SE[0, 0:3]

    @pl.when(has["zh"])
    def _():
        RZF[1] = ZH[1, 3:6] - 0.5 * SE[1, 0:3]

    inside = rows - 4
    if inside > 0:
        size = next(size for size in (6, 4, 3, 2, 1) if inside % size == 0)

        def inside_trial(i, carry):
            second_trial(2 + i * size, size)
            return carry

        lax.fori_loop(0, inside // size, inside_trial, 0)

    def first_step():
        told(0)
        return step_of(PEAKS[0])

    def second_stress(step, x, size):
        here = pl.ds(x, size)
        pres = PIN[here] - step * DV[here]
        PR[here] = pres
        trial = [TAU[c, here] + step * TR[c, here] for c in range(6)]
        return stress_rows(
            1, x, size, pres, trial, second_invariant(trial), COH[here], PL[here], SEL
        )

    lowest = jnp.full((nz, ny), -jnp.inf, jnp.float32)

    def inside_rows(step):
        most = (lowest, lowest)
        if inside > 0:

            def inside_stress(i, most):
                f, eta = second_stress(step, 2 + i * size, size)
                return jnp.maximum(most[0], f), jnp.maximum(most[1], eta)

            most = lax.fori_loop(0, inside // size, inside_stress, most)
        MOST[2, 0], MOST[2, 1] = most

    def end_trials():
        wait_got(x_copies)
        wait_got(corner_copies)
        for number, side, row in ((0, "xl", 0), (1, "xh", rows - 1)):
            sign = 0.5 - number
            beyond = row + 2 * number
            for c in range(3):
                RF[c, row + 1] = RF[c, row + 1] - sign * XH[number, c]

            @pl.when(has[side])
            def _(number=number, sign=sign, row=row, beyond=beyond):
                sub = lax.broadcasted_iota(jnp.int32, (nz, ny), 0)
                for c in range(3):
                    low = jnp.where(sub == 0, jnp.broadcast_to(CH[2 * number, 3 + c], (nz, ny)), 0.0)
                    high = jnp.where(sub == nz - 1, jnp.broadcast_to(CH[2 * number + 1, 3 + c], (nz, ny)), 0.0)
                    RF[c, beyond] = XH[number, 3 + c] + sign * SX[0, c, row + 1] + 0.5 * (high - low)

            for layer in range(2):
                for c in range(3):
                    RZF[layer, c, row] = RZF[layer, c, row] - sign * CH[2 * number + layer, c]
        if inside > 0:
            second_trial(0, 2)
            second_trial(rows - 2, 2)
        else:
            second_trial(0, rows)

    def end_rows(step):
        for i, x in enumerate((0, rows - 2) if inside > 0 else (0,)):
            MOST[i, 0], MOST[i, 1] = second_stress(step, x, 2 if inside > 0 else rows)
        if inside <= 0:
            MOST[1, 0], MOST[1, 1] = lowest, lowest

    @pl.when(jnp.logical_not(has["xh"]))
    def _():
        step = first_step()
        inside_rows(step)
        end_trials()
        end_rows(step)

    @pl.when(has["xh"])
    def _():
        end_trials()
        step = first_step()
        inside_rows(step)
        end_rows(step)

    tell_sent()
    step = step_of(PEAKS[0])
    tell_all(1)
    wait_sent(corner_copies)
    sx_copies = [
        ("xh", described("xh", SX.at[1, :, pl.ds(rows, 1)], XHL.at[0], 2, 3)),
        ("xl", described("xl", SX.at[1, :, pl.ds(1, 1)], XHL.at[1], 2, 3)),
    ]
    start(sx_copies[1:])
    sz_copies = [
        ("zh", described("zh", SEL.at[1], ZHL.at[0], 1, 1)),
        ("zl", described("zl", SEL.at[0], ZHL.at[1], 1, 1)),
    ]
    start(sz_copies)

    def moved(x, carry):
        for c in range(3):
            MOVED[c, at(x)] = V[c, at(x + 1)] + step * RF[c, at(x + 1)]
        return carry

    over_rows(moved)
    wait_got(sz_copies)
    start(sx_copies[:1])

    def last_force(x, carry):
        def diff_z(c, f):
            return dz(f, ZHL[0, c, at(x)], ZHL[1, c, at(x)])

        force = forces(1, x, block, diff_z)
        for c in range(3):
            FORCE[c, at(x)] = force[c]
        return carry

    over_rows(last_force)
    wait_got(sx_copies)
    for c in range(3):
        FORCE[c, 0] = FORCE[c, 0] - 0.5 * XHL[0, c, 0]
        FORCE[c, rows - 1] = FORCE[c, rows - 1] + 0.5 * XHL[1, c, 0]
    told(1)
    wait_sent(x_copies + z_copies + sx_copies + sz_copies)
    tell_sent()


def store_kernel(moved, pres, tau, plas, force, peaks, v_out, p_out, t_out, l_out, top_out, V, TOP, sem):
    copies = [
        pltpu.make_async_copy(source, place, sem.at[i])
        for i, (source, place) in enumerate(
            ((tau, t_out), (pres, p_out), (plas, l_out), (V, v_out), (TOP, top_out))
        )
    ]
    for copy in copies[:3]:
        copy.start()
    step = step_of(peaks[ITERS - 1])
    for c in range(3):
        V[c] = moved[c] + step * force[c]
    copies[3].start()
    tops = [top_of(peaks[it]) for it in range(ITERS)]
    TOP[...] = jnp.concatenate(tops, axis=1)[0]
    copies[4].start()
    for copy in copies:
        copy.wait()


def solution(mesh):
    gx_count, gz_count = mesh.shape["gx"], mesh.shape["gz"]
    total = gx_count * gz_count

    def per_device(velocity, pressure, stress_old, plastic, viscosity, weak_seed):
        rows, nz, ny = pressure.shape
        cells = (rows, nz, ny)
        f32 = jnp.float32
        vm = lambda *shape: pltpu.VMEM(shape, f32)
        hops = len(bits_of(gx_count)) + len(bits_of(gz_count // 2))
        anywhere = pl.BlockSpec(memory_space=pl.ANY)
        within = pl.BlockSpec(memory_space=pltpu.VMEM)
        half = ny // 2 if ny % 256 == 0 else ny
        shapes = (velocity.shape, pressure.shape, stress_old.shape, plastic.shape)
        inner = (velocity.shape, (ITERS, 1, half))
        held = pl.pallas_call(
            functools.partial(kernel, gx_count, gz_count),
            out_shape=tuple(vm(*shape) for shape in shapes + inner),
            in_specs=[anywhere] * 6,
            out_specs=(within,) * 6,
            scratch_shapes=[
                vm(3, rows + 2, nz, ny),
                vm(8, *cells),
                pltpu.VMEM(cells, jnp.int32),
                vm(*cells),
                vm(2, *cells),
                vm(*cells),
                vm(*cells),
                vm(*cells),
                vm(ny, ny),
                vm(*cells),
                vm(2, REACH, nz, ny),
                vm(*cells),
                vm(2, 3, rows, 1, ny),
                vm(2, 3, rows, 1, ny),
                vm(ITERS, 3, rows + 2, nz, ny),
                vm(3, *cells),
                vm(2, 6, rows, 1, ny),
                vm(2, 6, rows, 1, ny),
                vm(2, 6, nz, ny),
                vm(2, 6, nz, ny),
                vm(4, 6, 1, ny),
                vm(4, 6, 1, ny),
                vm(2, 3, rows, 1, ny),
                vm(2, 3, rows, 1, ny),
                vm(2, 3, 1, nz, ny),
                vm(3, rows + 2, nz, ny),
                vm(2, 3, rows, 1, ny),
                vm(6, *cells),
                vm(*cells),
                vm(*cells),
                vm(3, 2, nz, ny),
                vm(ITERS, total, 1, half),
                pltpu.SemaphoreType.DMA,
                pltpu.SemaphoreType.DMA((sems_of(sides_of(gz_count))[0],)),
                pltpu.SemaphoreType.DMA((sems_of(sides_of(gz_count))[1],)),
                pltpu.SemaphoreType.DMA,
                pltpu.SemaphoreType.DMA((ITERS,)),
                pltpu.SemaphoreType.REGULAR,
                pltpu.SemaphoreType.REGULAR((hops,)),
            ],
            compiler_params=pltpu.CompilerParams(collective_id=0, has_side_effects=True),
        )(velocity, pressure, stress_old, plastic, viscosity, weak_seed)
        held = [pltpu.with_memory_space_constraint(array, pltpu.VMEM) for array in held]
        return pl.pallas_call(
            store_kernel,
            out_shape=tuple(jax.ShapeDtypeStruct(shape, f32) for shape in shapes)
            + (jax.ShapeDtypeStruct((ITERS,), f32),),
            in_specs=[within, anywhere, anywhere, anywhere, within, within],
            out_specs=(anywhere,) * 5,
            scratch_shapes=[vm(*velocity.shape), vm(ITERS), pltpu.SemaphoreType.DMA((5,))],
        )(*held)

    in_specs = (
        P(None, "gx", "gz", None),
        P("gx", "gz", None),
        P(None, "gx", "gz", None),
        P("gx", "gz", None),
        P("gx", "gz", None),
        P("gx", "gz", None),
    )
    out_specs = (
        P(None, "gx", "gz", None),
        P("gx", "gz", None),
        P(None, "gx", "gz", None),
        P("gx", "gz", None),
        P(),
    )
    return jax.shard_map(
        per_device, mesh=mesh, in_specs=in_specs, out_specs=out_specs, check_vma=False
    )
```

```python
import functools
import math

import jax
import jax.numpy as jnp
from jax import lax
from jax.experimental import pallas as pl
from jax.experimental.pallas import tpu as pltpu
from jax.sharding import PartitionSpec as P

ITERS = 2
REACH = 6
PLANE = 4
MESH = pl.DeviceIdType.MESH

unnormalized_weights = [math.exp(-(k * k) / 18.0) for k in range(-REACH, REACH + 1)]
weight_total = sum(unnormalized_weights)
gauss_weights = [value / weight_total for value in unnormalized_weights]
shear_time_increment = 20.0


def bits_of(count):
    assert count & (count - 1) == 0
    return [1 << bit for bit in range(count.bit_length() - 1)]


def step_of(peaks):
    lane = lax.broadcasted_iota(jnp.int32, peaks.shape, 1)
    return 0.125 / jnp.max(jnp.where(lane < peaks.shape[1] // 2, -jnp.inf, peaks), axis=1, keepdims=True)


def top_of(peaks):
    lane = lax.broadcasted_iota(jnp.int32, peaks.shape, 1)
    return jnp.max(jnp.where(lane < peaks.shape[1] // 2, peaks, -jnp.inf), axis=1, keepdims=True)


def sides_of(count):
    return min(count - 1, 2)


def sems_of(z_sides):
    return 2 * z_sides + 4, 2 * z_sides + 6 + 2 * z_sides


def kernel(
    gx_count,
    gz_count,
    vel_in,
    pres_in,
    old_in,
    plas_in,
    visc_in,
    weak_in,
    MOVED,
    PR,
    TAU,
    PL,
    FORCE,
    PEAKS,
    V,
    IN,
    WK,
    PLZ,
    PZH,
    ETA,
    INV,
    COH,
    YM,
    GX,
    GXH,
    SM,
    VZE,
    VZH,
    SX,
    TZ,
    SE,
    ZH,
    XS,
    XH,
    CE,
    CH,
    SEL,
    ZHL,
    XHL,
    RF,
    RZF,
    TR,
    DV,
    TB,
    MOST,
    PK,
    in_sem,
    send_sem,
    recv_sem,
    pk_send,
    pk_recv,
    pair_sem,
    hop_sem,
):
    rows, nz, ny = PR.shape
    gx = lax.axis_index("gx")
    gz = lax.axis_index("gz")
    me = gx * gz_count + gz
    total = gx_count * gz_count
    has = {
        "xl": gx > 0,
        "xh": gx < gx_count - 1,
        "zl": gz > 0,
        "zh": gz < gz_count - 1,
    }
    target = {
        "xl": (gx - 1, gz),
        "xh": (gx + 1, gz),
        "zl": (gx, gz - 1),
        "zh": (gx, gz + 1),
    }
    opposite = {"xl": "xh", "xh": "xl", "zl": "zh", "zh": "zl"}
    corners = [(a, b) for a in ("xl", "xh") for b in ("zl", "zh")]
    for a, b in corners:
        has[a + b] = jnp.logical_and(has[a], has[b])
        target[a + b] = (target[a][0], target[b][1])
        opposite[a + b] = opposite[a] + opposite[b]
    barrier = pltpu.get_barrier_semaphore()

    side_of = gz % 2
    odd = side_of == 1
    even = side_of == 0
    lead = gz + 1 - side_of
    couple = gz // 2

    def flipped(index, bit):
        return index + bit * (1 - 2 * ((index // bit) % 2))

    always = gx >= 0
    rounds = [[(flipped(gx, bit), gz, always)] for bit in bits_of(min(PLANE, gx_count))]
    rounds += [
        [(gx - far, gz, gx >= far), (gx + far, gz, gx < gx_count - far)]
        for far in bits_of(gx_count)
        if far >= PLANE
    ]
    rounds += [[(gx, 2 * flipped(couple, bit) + 1, always)] for bit in bits_of(gz_count // 2)]
    along_gx = len(bits_of(gx_count))
    met = [place for far in rounds[1:3] + rounds[max(along_gx, 3) :] for place in far]

    def signal(sem, place):
        pl.semaphore_signal(sem, inc=1, device_id=place, device_id_type=MESH)

    def one_if(flag):
        return jnp.where(flag, 1, 0)

    z_sides = sides_of(gz_count)
    VI, PIN = IN.at[0], IN.at[1]
    plas_load = pltpu.make_async_copy(plas_in, PLZ, send_sem.at[sems_of(z_sides)[0] - 2])
    vel_load = pltpu.make_async_copy(vel_in, V.at[:, pl.ds(1, rows)], send_sem.at[z_sides])
    weak_load = pltpu.make_async_copy(weak_in, WK, pk_send)
    rest_loads = [
        pltpu.make_async_copy(visc_in, VI, in_sem),
        pltpu.make_async_copy(pres_in, PIN, in_sem),
        pltpu.make_async_copy(old_in, IN.at[pl.ds(2, 6)], in_sem),
    ]
    all_rest = pltpu.make_async_copy(IN, IN, in_sem)

    for side in ("xl", "xh"):

        @pl.when(has[side])
        def _(side=side):
            signal(barrier, (target[side][0], lead))

    @pl.when(odd)
    def _():
        signal(barrier, (gx, gz - 1))

        @pl.when(has["zh"])
        def _():
            signal(barrier, (gx, gz + 1))

    plas_load.start()
    vel_load.start()

    @pl.when(odd)
    def _():
        for x_place, z_place, there in met:

            @pl.when(there)
            def _(x_place=x_place, z_place=z_place):
                signal(barrier, (x_place, z_place))

    def slot(group):
        return group * z_sides if group < 2 else 2 * z_sides + 2 * (group - 2)

    corner_sent = (slot(1), slot(1) + 1, slot(3), slot(3) + 1) if z_sides == 2 else (slot(1), slot(1), slot(3), slot(3))

    def described(side, source, landing, got, sent):
        number = {"xl": 0, "xh": 1, "zl": 0, "zh": z_sides - 1}[side]
        return pltpu.make_async_remote_copy(
            src_ref=source,
            dst_ref=landing,
            send_sem=send_sem.at[slot(sent) + number],
            recv_sem=recv_sem.at[slot(got) + number],
            device_id=target[side],
            device_id_type=MESH,
        )

    def start(pairs):
        for side, copy in pairs:

            @pl.when(has[side])
            def _(copy=copy):
                copy.start()

    gx_odd = gx % 2 == 1
    gx_even = gx % 2 == 0

    def start_far(pairs):
        for place, side in ((gx_odd, "xh"), (gx_even, "xl")):

            @pl.when(place)
            def _(side=side):
                start([pair for pair in pairs if pair[0] == side])

    def start_near(pairs):
        for place, side in ((gx_odd, "xl"), (gx_even, "xh")):

            @pl.when(place)
            def _(side=side):
                start([pair for pair in pairs if pair[0] == side])

    has_far = jnp.logical_or(
        jnp.logical_and(gx_odd, has["xh"]), jnp.logical_and(gx_even, has["xl"])
    )

    def wait_sent(pairs):
        for side, copy in pairs:

            @pl.when(has[side])
            def _(copy=copy):
                copy.wait_send()

    def wait_got(pairs):
        for side, copy in pairs:

            @pl.when(has[opposite[side]])
            def _(copy=copy):
                copy.wait_recv()

    def zero(ref):
        ref[...] = jnp.zeros(ref.shape, ref.dtype)

    def zero_unless(side, *refs):
        @pl.when(jnp.logical_not(has[side]))
        def _():
            for ref in refs:
                zero(ref)

    @pl.when(even)
    def _():
        pl.semaphore_wait(barrier, 1 + one_if(has["zl"]))
        signal(pair_sem, (gx, gz + 1))

        @pl.when(has["zl"])
        def _():
            signal(pair_sem, (gx, gz - 1))

    @pl.when(odd)
    def _():
        pl.semaphore_wait(pair_sem, 1 + one_if(has["zh"]))

    pz_copies = [
        ("zh", described("zh", plas_in, PZH.at[0], 0, 0)),
        ("zl", described("zl", plas_in, PZH.at[1], 0, 0)),
    ]
    start(pz_copies)
    for copy in rest_loads:
        copy.start()
    weak_load.start()

    places_a = lax.broadcasted_iota(jnp.int32, (ny, ny), 0)
    places_b = lax.broadcasted_iota(jnp.int32, (ny, ny), 1)
    gap = (places_a - places_b).astype(jnp.float32)
    YM[...] = jnp.where(
        jnp.abs(gap) <= float(REACH), jnp.exp(-gap * gap / 18.0) / weight_total, 0.0
    )
    zero_unless("zl", PZH.at[0])
    zero_unless("zh", PZH.at[1])
    zero_unless("xl", V.at[:, pl.ds(0, 1)], GXH.at[0], XH.at[0], XHL.at[0], RF.at[:, pl.ds(0, 1)])
    zero_unless("xh", V.at[:, pl.ds(rows + 1, 1)], GXH.at[1], XH.at[1], XHL.at[1])
    zero_unless("xh", RF.at[:, pl.ds(rows + 1, 1)])
    zero_unless("zl", VZH.at[0], ZH.at[0], ZHL.at[0], RZF.at[0])
    zero_unless("zh", VZH.at[1], ZH.at[1], ZHL.at[1], RZF.at[1])
    for number, (a, b) in enumerate(corners):
        zero_unless(a + b, CH.at[number])
    for it in range(ITERS):
        zero(SX.at[it, :, pl.ds(0, 1)])
        zero(SX.at[it, :, pl.ds(rows + 1, 1)])

    vel_load.wait()
    @pl.when(odd)
    def _():
        greeters = 2 * (one_if(has["xl"]) + one_if(has["xh"]))
        for _, _, there in met:
            greeters = greeters + one_if(there)
        pl.semaphore_wait(barrier, greeters)
        signal(pair_sem, (gx, gz - 1))

    @pl.when(even)
    def _():
        pl.semaphore_wait(pair_sem, 1)

    vel_copies = [
        ("xh", described("xh", V.at[:, pl.ds(rows, 1)], V.at[:, pl.ds(0, 1)], 2, 2)),
        ("xl", described("xl", V.at[:, pl.ds(1, 1)], V.at[:, pl.ds(rows + 1, 1)], 2, 2)),
    ]
    start_far(vel_copies)

    @pl.when(jnp.logical_not(has_far))
    def _():
        start_near(vel_copies)


    def hop_send(k):
        if k < len(rounds):

            @pl.when(odd)
            def _():
                for x_place, z_place, there in rounds[k]:

                    @pl.when(there)
                    def _(x_place=x_place, z_place=z_place):
                        signal(hop_sem.at[k], (x_place, z_place))

    def hop_wait(k):
        if k < len(rounds):

            @pl.when(odd)
            def _():
                expected = 0
                for _, _, there in rounds[k]:
                    expected = expected + one_if(there)
                pl.semaphore_wait(hop_sem.at[k], expected)

    hop_send(0)

    block = rows // 2
    many = (block, nz, ny)

    def over_rows(body, carry=0):
        return lax.fori_loop(0, rows // block, lambda i, state: body(i * block, state), carry)

    def at(x):
        return pl.ds(x, block)

    def vel_edges(x, carry):
        for c in range(3):
            row = V[c, at(x + 1)]
            VZE[0, c, at(x)] = row[:, 0:1]
            VZE[1, c, at(x)] = row[:, nz - 1 : nz]
        return carry

    over_rows(vel_edges)
    plas_load.wait()
    wait_got(pz_copies)
    vz_copies = [
        ("zh", described("zh", VZE.at[1], VZH.at[0], 1, 1)),
        ("zl", described("zl", VZE.at[0], VZH.at[1], 1, 1)),
    ]
    start(vz_copies)

    def smooth_z(x, carry):
        own, low, high = PLZ[at(x)], PZH[0, at(x)], PZH[1, at(x)]
        sub = lax.broadcasted_iota(jnp.int32, many, 1)
        sum_ = gauss_weights[REACH] * own
        for k in range(1, REACH + 1):
            above = pltpu.roll(jnp.where(sub >= k, own, high), nz - k, 1)
            below = pltpu.roll(jnp.where(sub < nz - k, own, low), k, 1)
            sum_ = sum_ + gauss_weights[REACH + k] * (above + below)
        SM[at(x)] = sum_
        return carry

    over_rows(smooth_z)
    GX[...] = jnp.dot(
        SM[...].reshape(rows * nz, ny),
        YM[...],
        precision=lax.Precision.HIGHEST,
        preferred_element_type=jnp.float32,
    ).reshape(rows, nz, ny)
    plas_copies = [
        ("xh", described("xh", GX.at[pl.ds(rows - REACH, REACH)], GXH.at[0], 3, 3)),
        ("xl", described("xl", GX.at[pl.ds(0, REACH)], GXH.at[1], 3, 3)),
    ]
    start_far(plas_copies)

    @pl.when(has_far)
    def _():
        start_near(vel_copies)

    start_near(plas_copies)
    hop_wait(0)
    hop_send(1)

    all_rest.wait()
    weak_load.wait()

    def prepare(x, carry):
        eta = VI[at(x)]
        eta = shear_time_increment * eta / (eta + shear_time_increment)
        ETA[at(x)] = eta
        INV[at(x)] = 1.0 / (eta + 0.5)
        COH[at(x)] = 0.8660254 - (0.8660254 * 0.6) * WK[at(x)].astype(jnp.float32)
        return carry

    over_rows(prepare)
    for row in range(rows):
        sum_ = gauss_weights[REACH] * GX[row]
        for k in range(1, REACH + 1):
            for other in (row - k, row + k):
                if 0 <= other < rows:
                    sum_ = sum_ + gauss_weights[REACH + k] * GX[other]
        SM[row] = sum_
    for k in range(1, len(rounds) - 1):
        hop_wait(k)
        hop_send(k + 1)

    wait_got(vz_copies)

    def dy(f):
        lane = lax.broadcasted_iota(jnp.int32, f.shape, 2)
        up = jnp.where(lane < ny - 1, pltpu.roll(f, ny - 1, 2), 0.0)
        down = jnp.where(lane > 0, pltpu.roll(f, 1, 2), 0.0)
        return (up - down) * 0.5

    def dz(f, low, high):
        sub = lax.broadcasted_iota(jnp.int32, f.shape, 1)
        up = pltpu.roll(jnp.where(sub >= 1, f, jnp.broadcast_to(high, f.shape)), nz - 1, 1)
        down = pltpu.roll(jnp.where(sub < nz - 1, f, jnp.broadcast_to(low, f.shape)), 1, 1)
        return (up - down) * 0.5

    def dz_inside(f):
        sub = lax.broadcasted_iota(jnp.int32, f.shape, 1)
        up = jnp.where(sub < nz - 1, pltpu.roll(f, nz - 1, 1), 0.0)
        down = jnp.where(sub >= 1, pltpu.roll(f, 1, 1), 0.0)
        return (up - down) * 0.5

    def strains(field, halo, x, size):
        v = [field[c, pl.ds(x + 1, size)] for c in range(3)]
        dx_v = [(field[c, pl.ds(x + 2, size)] - field[c, pl.ds(x, size)]) * 0.5 for c in range(3)]
        dz_v = [dz(f, halo[0, c, pl.ds(x, size)], halo[1, c, pl.ds(x, size)]) for c, f in enumerate(v)]
        dy_v = [dy(f) for f in v]
        div = dx_v[0] + dz_v[1] + dy_v[2]
        third = div * (1.0 / 3.0)
        return (
            dx_v[0] - third,
            dz_v[1] - third,
            dy_v[2] - third,
            0.5 * (dx_v[1] + dz_v[0]),
            0.5 * (dx_v[2] + dy_v[0]),
            0.5 * (dz_v[2] + dy_v[1]),
        ), div

    def second_invariant(trial):
        return jnp.sqrt(
            0.5 * (trial[0] * trial[0] + trial[1] * trial[1] + trial[2] * trial[2])
            + trial[3] * trial[3]
            + trial[4] * trial[4]
            + trial[5] * trial[5]
        )

    def first_trial(x):
        strain, div = strains(V, VZH, x, block)
        quarter = 0.25 * div
        pres = PIN[at(x)] - quarter
        PR[at(x)] = pres
        PIN[at(x)] = pres - quarter
        twice = 2.0 * ETA[at(x)]
        trial = [
            twice * (strain[c] + IN[2 + c, at(x)] * (0.5 / shear_time_increment)) for c in range(6)
        ]
        for c in range(6):
            TAU[c, at(x)] = trial[c]
        TB[at(x)] = second_invariant(trial)

    def in_order(act):
        for place, numbers in ((gx_odd, (1, 0)), (gx_even, (0, 1))):

            @pl.when(place)
            def _(numbers=numbers):
                for number in numbers:
                    act(number, number == numbers[0])

    def one_trial(number, far):
        wait_got(vel_copies[number : number + 1])
        first_trial(number * block)

    in_order(one_trial)
    half = ny // 2 if ny % 256 == 0 else ny

    def stress_rows(it, x, size, pres, trial, tau_ii, strength, plas, edge):
        def at(x):
            return pl.ds(x, size)

        last = it == ITERS - 1
        eta, inv = ETA[at(x)], INV[at(x)]
        yield_f = tau_ii - 0.5 * jnp.maximum(pres, 0.0) - strength
        dlam = jnp.maximum(yield_f, 0.0) * inv
        shrink = 1.0 - eta * dlam / jnp.maximum(tau_ii, 0.5)
        tau = [shrink * value for value in trial]
        PL[at(x)] = plas + dlam
        if last:
            for c in range(6):
                TAU[c, at(x)] = tau[c]
        SX[it, 0, at(x + 1)] = tau[0] - pres
        SX[it, 1, at(x + 1)] = tau[3]
        SX[it, 2, at(x + 1)] = tau[4]
        szz = tau[1] - pres
        TZ[0, at(x)] = szz
        TZ[1, at(x)] = tau[5]
        TZ[2, at(x)] = tau[2] - pres
        for c, f in enumerate((tau[3], szz, tau[5])):
            edge[0, c, at(x)] = f[:, 0:1]
            edge[1, c, at(x)] = f[:, nz - 1 : nz]
        return jnp.max(yield_f, axis=0), jnp.max(eta * shrink, axis=0)

    def forces(it, x, size, diff_z):
        s = [SX[it, c, pl.ds(x + 1, size)] for c in range(3)]
        t = [TZ[c, pl.ds(x, size)] for c in range(3)]
        along_x = [0.5 * (SX[it, c, pl.ds(x + 2, size)] - SX[it, c, pl.ds(x, size)]) for c in range(3)]
        along_z = [diff_z(c, f) for c, f in enumerate((s[1], t[0], t[1]))]
        along_y = [dy(f) for f in (s[2], t[1], t[2])]
        return [along_x[c] + along_z[c] + along_y[c] for c in range(3)]

    def folded(most):
        return jnp.maximum(most[:, :half], most[:, ny - half :])

    def tell(it, place):
        pltpu.make_async_remote_copy(
            src_ref=PK.at[it, me],
            dst_ref=PK.at[it, me],
            send_sem=pk_send,
            recv_sem=pk_recv.at[it],
            device_id=place,
            device_id_type=MESH,
        ).start()

    turned = {bit: flipped(gx, bit) - gx for bit in bits_of(gx_count)}

    def tell_all(it):
        parts = 3 if it else 2
        most_f, most_eta = [
            folded(functools.reduce(jnp.maximum, [MOST[i, k] for i in range(parts)])) for k in range(2)
        ]
        lane = lax.broadcasted_iota(jnp.int32, (nz, half), 1)
        most_f = jnp.maximum(most_f, pltpu.roll(most_f, half // 2, 1))
        most_eta = jnp.maximum(most_eta, pltpu.roll(most_eta, half // 2, 1))
        PK[it, me] = jnp.max(jnp.where(lane < half // 2, most_f, most_eta), axis=0, keepdims=True)
        if gx_count <= 16 and gz_count <= 2:
            for flips in reversed(range(1, total)):
                x_place, z_place = gx, gz
                for bit in bits_of(gx_count):
                    if flips // gz_count & bit:
                        x_place = x_place + turned[bit]
                if flips % gz_count:
                    z_place = flipped(gz, 1)
                tell(it, (x_place, z_place))
        else:
            for dz_ in range(gz_count):
                other_z = gz + dz_
                other_z = jnp.where(other_z >= gz_count, other_z - gz_count, other_z)

                def one(dx_, carry, other_z=other_z):
                    other_x = gx + dx_
                    tell(it, (jnp.where(other_x >= gx_count, other_x - gx_count, other_x), other_z))
                    return carry

                lax.fori_loop(0 if dz_ else 1, gx_count, one, 0)

    def told(it):
        others = PK.at[it, pl.ds(0, total - 1)]
        pltpu.make_async_copy(others, others, pk_recv.at[it]).wait()
        PEAKS[it] = jnp.max(PK[it], axis=0)

    def tell_sent():
        others = PK.at[0, pl.ds(0, total - 1)]
        pltpu.make_async_copy(others, others, pk_send).wait()

    def first_stress(x):
        strength = COH[at(x)] / (1.0 + 2.0 * SM[at(x)])
        COH[at(x)] = strength
        trial = [TAU[c, at(x)] for c in range(6)]
        return stress_rows(0, x, block, PR[at(x)], trial, TB[at(x)], strength, PLZ[at(x)], SE)

    x_copies = [
        ("xh", described("xh", XS.at[1], XH.at[0], 4, 2)),
        ("xl", described("xl", XS.at[0], XH.at[1], 4, 2)),
    ]
    corner_copies = []
    for number, (a, b) in enumerate(corners):
        there = corners.index((opposite[a], opposite[b]))
        corner_copies.append(
            (
                a + b,
                pltpu.make_async_remote_copy(
                    src_ref=CE.at[number],
                    dst_ref=CH.at[there],
                    send_sem=send_sem.at[corner_sent[number]],
                    recv_sem=recv_sem.at[slot(5) + (number if z_sides == 2 else number // 2)],
                    device_id=target[a + b],
                    device_id_type=MESH,
                ),
            )
        )

    def one_edge(number, far):
        row = (rows - 1) * number
        force = forces(0, row, 1, lambda c, f: dz_inside(f))
        for c in range(3):
            XS[number, c] = SX[0, c, row + 1]
            XS[number, 3 + c] = force[c][0]
        for layer in range(2):
            where = 2 * number + layer
            place = (nz - 1) * layer
            for c in range(3):
                CE[where, c] = SX[0, c, row + 1, place : place + 1]
                CE[where, 3 + c] = SE[layer, c, row]
        if far:
            wait_sent(vel_copies)
        start(x_copies[1 - number : 2 - number])

    def one_side(number, far):
        wait_got(plas_copies[number : number + 1])
        for beside in range(min(REACH, block)):
            here = beside if number == 0 else rows - 1 - beside
            sum_ = SM[here]
            for k in range(beside + 1, REACH + 1):
                place = REACH + beside - k if number == 0 else k - 1 - beside
                sum_ = sum_ + gauss_weights[REACH + k] * GXH[number, place]
            SM[here] = sum_
        MOST[number, 0], MOST[number, 1] = first_stress(number * block)
        if far:
            one_edge(number, far)
        if far:
            if len(rounds) > 1:
                hop_wait(len(rounds) - 1)

            @pl.when(odd)
            def _():
                signal(pair_sem, (gx, gz - 1))

    in_order(one_side)
    @pl.when(even)
    def _():
        pl.semaphore_wait(pair_sem, 1)

    tell_all(0)
    for place, number in ((gx_odd, 0), (gx_even, 1)):

        @pl.when(place)
        def _(number=number):
            one_edge(number, False)

    wait_sent(vz_copies)
    wait_sent(plas_copies)
    start(corner_copies)

    def own_force(x, carry):
        force = forces(0, x, block, lambda c, f: dz_inside(f))
        for c in range(3):
            RF[c, at(x + 1)] = force[c]
            SE[0, 3 + c, at(x)] = force[c][:, 0:1]
            SE[1, 3 + c, at(x)] = force[c][:, nz - 1 : nz]
        return carry

    over_rows(own_force)
    wait_sent(pz_copies)
    z_copies = [
        ("zh", described("zh", SE.at[1], ZH.at[0], 0, 0)),
        ("zl", described("zl", SE.at[0], ZH.at[1], 0, 0)),
    ]
    start(z_copies)
    wait_got(z_copies)

    def add_z(x, carry):
        sub = lax.broadcasted_iota(jnp.int32, many, 1)
        for c in range(3):
            high = jnp.where(sub == nz - 1, jnp.broadcast_to(ZH[1, c, at(x)], many), 0.0)
            low = jnp.where(sub == 0, jnp.broadcast_to(ZH[0, c, at(x)], many), 0.0)
            RF[c, at(x + 1)] = RF[c, at(x + 1)] + 0.5 * (high - low)
        return carry

    def second_trial(x, size):
        strain, div = strains(RF, RZF, x, size)
        twice = 2.0 * ETA[pl.ds(x, size)]
        for c in range(6):
            TR[c, pl.ds(x, size)] = twice * strain[c]
        DV[pl.ds(x, size)] = 0.25 * div

    over_rows(add_z)

    @pl.when(has["zl"])
    def _():
        RZF[0] = ZH[0, 3:6] + 0.5 * SE[0, 0:3]

    @pl.when(has["zh"])
    def _():
        RZF[1] = ZH[1, 3:6] - 0.5 * SE[1, 0:3]

    inside = rows - 4
    if inside > 0:
        size = next(size for size in (6, 4, 3, 2, 1) if inside % size == 0)

        def inside_trial(i, carry):
            second_trial(2 + i * size, size)
            return carry

        lax.fori_loop(0, inside // size, inside_trial, 0)

    def first_step():
        told(0)
        return step_of(PEAKS[0])

    def second_stress(step, x, size):
        here = pl.ds(x, size)
        pres = PIN[here] - step * DV[here]
        PR[here] = pres
        trial = [TAU[c, here] + step * TR[c, here] for c in range(6)]
        return stress_rows(
            1, x, size, pres, trial, second_invariant(trial), COH[here], PL[here], SEL
        )

    lowest = jnp.full((nz, ny), -jnp.inf, jnp.float32)

    def inside_rows(step):
        most = (lowest, lowest)
        if inside > 0:

            def inside_stress(i, most):
                f, eta = second_stress(step, 2 + i * size, size)
                return jnp.maximum(most[0], f), jnp.maximum(most[1], eta)

            most = lax.fori_loop(0, inside // size, inside_stress, most)
        MOST[2, 0], MOST[2, 1] = most

    def end_trials():
        wait_got(x_copies)
        wait_got(corner_copies)
        for number, side, row in ((0, "xl", 0), (1, "xh", rows - 1)):
            sign = 0.5 - number
            beyond = row + 2 * number
            for c in range(3):
                RF[c, row + 1] = RF[c, row + 1] - sign * XH[number, c]

            @pl.when(has[side])
            def _(number=number, sign=sign, row=row, beyond=beyond):
                sub = lax.broadcasted_iota(jnp.int32, (nz, ny), 0)
                for c in range(3):
                    low = jnp.where(sub == 0, jnp.broadcast_to(CH[2 * number, 3 + c], (nz, ny)), 0.0)
                    high = jnp.where(sub == nz - 1, jnp.broadcast_to(CH[2 * number + 1, 3 + c], (nz, ny)), 0.0)
                    RF[c, beyond] = XH[number, 3 + c] + sign * SX[0, c, row + 1] + 0.5 * (high - low)

            for layer in range(2):
                for c in range(3):
                    RZF[layer, c, row] = RZF[layer, c, row] - sign * CH[2 * number + layer, c]
        if inside > 0:
            second_trial(0, 2)
            second_trial(rows - 2, 2)
        else:
            second_trial(0, rows)

    def end_rows(step):
        for i, x in enumerate((0, rows - 2) if inside > 0 else (0,)):
            MOST[i, 0], MOST[i, 1] = second_stress(step, x, 2 if inside > 0 else rows)
        if inside <= 0:
            MOST[1, 0], MOST[1, 1] = lowest, lowest

    @pl.when(gx >= gx_count // 2)
    def _():
        step = first_step()
        inside_rows(step)
        end_trials()
        end_rows(step)

    @pl.when(gx < gx_count // 2)
    def _():
        end_trials()
        step = first_step()
        inside_rows(step)
        end_rows(step)

    tell_sent()
    step = step_of(PEAKS[0])
    tell_all(1)
    wait_sent(corner_copies)
    sx_copies = [
        ("xh", described("xh", SX.at[1, :, pl.ds(rows, 1)], XHL.at[0], 2, 3)),
        ("xl", described("xl", SX.at[1, :, pl.ds(1, 1)], XHL.at[1], 2, 3)),
    ]
    start(sx_copies[1:])
    sz_copies = [
        ("zh", described("zh", SEL.at[1], ZHL.at[0], 1, 1)),
        ("zl", described("zl", SEL.at[0], ZHL.at[1], 1, 1)),
    ]
    start(sz_copies)

    def moved(x, carry):
        for c in range(3):
            MOVED[c, at(x)] = V[c, at(x + 1)] + step * RF[c, at(x + 1)]
        return carry

    over_rows(moved)
    wait_got(sz_copies)
    start(sx_copies[:1])

    def last_force(x, carry):
        def diff_z(c, f):
            return dz(f, ZHL[0, c, at(x)], ZHL[1, c, at(x)])

        force = forces(1, x, block, diff_z)
        for c in range(3):
            FORCE[c, at(x)] = force[c]
        return carry

    over_rows(last_force)
    wait_got(sx_copies)
    for c in range(3):
        FORCE[c, 0] = FORCE[c, 0] - 0.5 * XHL[0, c, 0]
        FORCE[c, rows - 1] = FORCE[c, rows - 1] + 0.5 * XHL[1, c, 0]
    told(1)
    wait_sent(x_copies + z_copies + sx_copies + sz_copies)
    tell_sent()


def store_kernel(moved, pres, tau, plas, force, peaks, v_out, p_out, t_out, l_out, top_out, V, TOP, sem):
    copies = [
        pltpu.make_async_copy(source, place, sem.at[i])
        for i, (source, place) in enumerate(
            ((tau, t_out), (pres, p_out), (plas, l_out), (V, v_out), (TOP, top_out))
        )
    ]
    for copy in copies[:3]:
        copy.start()
    step = step_of(peaks[ITERS - 1])
    for c in range(3):
        V[c] = moved[c] + step * force[c]
    copies[3].start()
    tops = [top_of(peaks[it]) for it in range(ITERS)]
    TOP[...] = jnp.concatenate(tops, axis=1)[0]
    copies[4].start()
    for copy in copies:
        copy.wait()


def solution(mesh):
    gx_count, gz_count = mesh.shape["gx"], mesh.shape["gz"]
    total = gx_count * gz_count

    def per_device(velocity, pressure, stress_old, plastic, viscosity, weak_seed):
        rows, nz, ny = pressure.shape
        cells = (rows, nz, ny)
        f32 = jnp.float32
        vm = lambda *shape: pltpu.VMEM(shape, f32)
        hops = len(bits_of(gx_count)) + len(bits_of(gz_count // 2))
        anywhere = pl.BlockSpec(memory_space=pl.ANY)
        within = pl.BlockSpec(memory_space=pltpu.VMEM)
        half = ny // 2 if ny % 256 == 0 else ny
        shapes = (velocity.shape, pressure.shape, stress_old.shape, plastic.shape)
        inner = (velocity.shape, (ITERS, 1, half))
        held = pl.pallas_call(
            functools.partial(kernel, gx_count, gz_count),
            out_shape=tuple(vm(*shape) for shape in shapes + inner),
            in_specs=[anywhere] * 6,
            out_specs=(within,) * 6,
            scratch_shapes=[
                vm(3, rows + 2, nz, ny),
                vm(8, *cells),
                pltpu.VMEM(cells, jnp.int32),
                vm(*cells),
                vm(2, *cells),
                vm(*cells),
                vm(*cells),
                vm(*cells),
                vm(ny, ny),
                vm(*cells),
                vm(2, REACH, nz, ny),
                vm(*cells),
                vm(2, 3, rows, 1, ny),
                vm(2, 3, rows, 1, ny),
                vm(ITERS, 3, rows + 2, nz, ny),
                vm(3, *cells),
                vm(2, 6, rows, 1, ny),
                vm(2, 6, rows, 1, ny),
                vm(2, 6, nz, ny),
                vm(2, 6, nz, ny),
                vm(4, 6, 1, ny),
                vm(4, 6, 1, ny),
                vm(2, 3, rows, 1, ny),
                vm(2, 3, rows, 1, ny),
                vm(2, 3, 1, nz, ny),
                vm(3, rows + 2, nz, ny),
                vm(2, 3, rows, 1, ny),
                vm(6, *cells),
                vm(*cells),
                vm(*cells),
                vm(3, 2, nz, ny),
                vm(ITERS, total, 1, half),
                pltpu.SemaphoreType.DMA,
                pltpu.SemaphoreType.DMA((sems_of(sides_of(gz_count))[0],)),
                pltpu.SemaphoreType.DMA((sems_of(sides_of(gz_count))[1],)),
                pltpu.SemaphoreType.DMA,
                pltpu.SemaphoreType.DMA((ITERS,)),
                pltpu.SemaphoreType.REGULAR,
                pltpu.SemaphoreType.REGULAR((hops,)),
            ],
            compiler_params=pltpu.CompilerParams(collective_id=0, has_side_effects=True),
        )(velocity, pressure, stress_old, plastic, viscosity, weak_seed)
        held = [pltpu.with_memory_space_constraint(array, pltpu.VMEM) for array in held]
        return pl.pallas_call(
            store_kernel,
            out_shape=tuple(jax.ShapeDtypeStruct(shape, f32) for shape in shapes)
            + (jax.ShapeDtypeStruct((ITERS,), f32),),
            in_specs=[within, anywhere, anywhere, anywhere, within, within],
            out_specs=(anywhere,) * 5,
            scratch_shapes=[vm(*velocity.shape), vm(ITERS), pltpu.SemaphoreType.DMA((5,))],
        )(*held)

    in_specs = (
        P(None, "gx", "gz", None),
        P("gx", "gz", None),
        P(None, "gx", "gz", None),
        P("gx", "gz", None),
        P("gx", "gz", None),
        P("gx", "gz", None),
    )
    out_specs = (
        P(None, "gx", "gz", None),
        P("gx", "gz", None),
        P(None, "gx", "gz", None),
        P("gx", "gz", None),
        P(),
    )
    return jax.shard_map(
        per_device, mesh=mesh, in_specs=in_specs, out_specs=out_specs, check_vma=False
    )
```

```python
import functools
import math

import jax
import jax.numpy as jnp
from jax import lax
from jax.experimental import pallas as pl
from jax.experimental.pallas import tpu as pltpu
from jax.sharding import PartitionSpec as P

ITERS = 2
REACH = 6
PLANE = 4
MESH = pl.DeviceIdType.MESH

unnormalized_weights = [math.exp(-(k * k) / 18.0) for k in range(-REACH, REACH + 1)]
weight_total = sum(unnormalized_weights)
gauss_weights = [value / weight_total for value in unnormalized_weights]
shear_time_increment = 20.0


def bits_of(count):
    assert count & (count - 1) == 0
    return [1 << bit for bit in range(count.bit_length() - 1)]


def step_of(peaks):
    lane = lax.broadcasted_iota(jnp.int32, peaks.shape, 1)
    return 0.125 / jnp.max(jnp.where(lane < peaks.shape[1] // 2, -jnp.inf, peaks), axis=1, keepdims=True)


def top_of(peaks):
    lane = lax.broadcasted_iota(jnp.int32, peaks.shape, 1)
    return jnp.max(jnp.where(lane < peaks.shape[1] // 2, peaks, -jnp.inf), axis=1, keepdims=True)


def sides_of(count):
    return min(count - 1, 2)


def sems_of(z_sides):
    return 2 * z_sides + 4, 2 * z_sides + 6 + 2 * z_sides


def kernel(
    gx_count,
    gz_count,
    vel_in,
    pres_in,
    old_in,
    plas_in,
    visc_in,
    weak_in,
    MOVED,
    PR,
    TAU,
    PL,
    FORCE,
    PEAKS,
    V,
    IN,
    WK,
    PLZ,
    PZH,
    ETA,
    INV,
    COH,
    YM,
    GX,
    GXH,
    SM,
    VZE,
    VZH,
    SX,
    TZ,
    SE,
    ZH,
    XS,
    XH,
    CE,
    CH,
    SEL,
    ZHL,
    XHL,
    RF,
    RZF,
    TR,
    DV,
    TB,
    MOST,
    PK,
    in_sem,
    send_sem,
    recv_sem,
    pk_send,
    pk_recv,
    pair_sem,
    hop_sem,
):
    rows, nz, ny = PR.shape
    gx = lax.axis_index("gx")
    gz = lax.axis_index("gz")
    me = gx * gz_count + gz
    total = gx_count * gz_count
    has = {
        "xl": gx > 0,
        "xh": gx < gx_count - 1,
        "zl": gz > 0,
        "zh": gz < gz_count - 1,
    }
    target = {
        "xl": (gx - 1, gz),
        "xh": (gx + 1, gz),
        "zl": (gx, gz - 1),
        "zh": (gx, gz + 1),
    }
    opposite = {"xl": "xh", "xh": "xl", "zl": "zh", "zh": "zl"}
    corners = [(a, b) for a in ("xl", "xh") for b in ("zl", "zh")]
    for a, b in corners:
        has[a + b] = jnp.logical_and(has[a], has[b])
        target[a + b] = (target[a][0], target[b][1])
        opposite[a + b] = opposite[a] + opposite[b]
    barrier = pltpu.get_barrier_semaphore()

    side_of = gz % 2
    odd = side_of == 1
    even = side_of == 0
    lead = gz + 1 - side_of
    couple = gz // 2

    def flipped(index, bit):
        return index + bit * (1 - 2 * ((index // bit) % 2))

    always = gx >= 0
    rounds = [[(flipped(gx, bit), gz, always)] for bit in bits_of(min(PLANE, gx_count))]
    rounds += [
        [(gx - far, gz, gx >= far), (gx + far, gz, gx < gx_count - far)]
        for far in bits_of(gx_count)
        if far >= PLANE
    ]
    rounds += [[(gx, 2 * flipped(couple, bit) + 1, always)] for bit in bits_of(gz_count // 2)]
    along_gx = len(bits_of(gx_count))
    met = [place for far in rounds[1:3] + rounds[max(along_gx, 3) :] for place in far]

    def signal(sem, place):
        pl.semaphore_signal(sem, inc=1, device_id=place, device_id_type=MESH)

    def one_if(flag):
        return jnp.where(flag, 1, 0)

    z_sides = sides_of(gz_count)
    VI, PIN = IN.at[0], IN.at[1]
    plas_load = pltpu.make_async_copy(plas_in, PLZ, send_sem.at[sems_of(z_sides)[0] - 2])
    vel_load = pltpu.make_async_copy(vel_in, V.at[:, pl.ds(1, rows)], send_sem.at[z_sides])
    weak_load = pltpu.make_async_copy(weak_in, WK, pk_send)
    rest_loads = [
        pltpu.make_async_copy(visc_in, VI, in_sem),
        pltpu.make_async_copy(pres_in, PIN, in_sem),
        pltpu.make_async_copy(old_in, IN.at[pl.ds(2, 6)], in_sem),
    ]
    all_rest = pltpu.make_async_copy(IN, IN, in_sem)

    for side in ("xl", "xh"):

        @pl.when(has[side])
        def _(side=side):
            signal(barrier, (target[side][0], lead))

    @pl.when(odd)
    def _():
        signal(barrier, (gx, gz - 1))

        @pl.when(has["zh"])
        def _():
            signal(barrier, (gx, gz + 1))

    plas_load.start()
    vel_load.start()

    @pl.when(odd)
    def _():
        for x_place, z_place, there in met:

            @pl.when(there)
            def _(x_place=x_place, z_place=z_place):
                signal(barrier, (x_place, z_place))

    def slot(group):
        return group * z_sides if group < 2 else 2 * z_sides + 2 * (group - 2)

    corner_sent = (slot(1), slot(1) + 1, slot(3), slot(3) + 1) if z_sides == 2 else (slot(1), slot(1), slot(3), slot(3))

    def described(side, source, landing, got, sent):
        number = {"xl": 0, "xh": 1, "zl": 0, "zh": z_sides - 1}[side]
        return pltpu.make_async_remote_copy(
            src_ref=source,
            dst_ref=landing,
            send_sem=send_sem.at[slot(sent) + number],
            recv_sem=recv_sem.at[slot(got) + number],
            device_id=target[side],
            device_id_type=MESH,
        )

    def start(pairs):
        for side, copy in pairs:

            @pl.when(has[side])
            def _(copy=copy):
                copy.start()

    gx_odd = gx % 2 == 1
    gx_even = gx % 2 == 0

    def start_far(pairs):
        for place, side in ((gx_odd, "xh"), (gx_even, "xl")):

            @pl.when(place)
            def _(side=side):
                start([pair for pair in pairs if pair[0] == side])

    def start_near(pairs):
        for place, side in ((gx_odd, "xl"), (gx_even, "xh")):

            @pl.when(place)
            def _(side=side):
                start([pair for pair in pairs if pair[0] == side])

    has_far = jnp.logical_or(
        jnp.logical_and(gx_odd, has["xh"]), jnp.logical_and(gx_even, has["xl"])
    )

    def wait_sent(pairs):
        for side, copy in pairs:

            @pl.when(has[side])
            def _(copy=copy):
                copy.wait_send()

    def wait_got(pairs):
        for side, copy in pairs:

            @pl.when(has[opposite[side]])
            def _(copy=copy):
                copy.wait_recv()

    def zero(ref):
        ref[...] = jnp.zeros(ref.shape, ref.dtype)

    def zero_unless(side, *refs):
        @pl.when(jnp.logical_not(has[side]))
        def _():
            for ref in refs:
                zero(ref)

    @pl.when(even)
    def _():
        pl.semaphore_wait(barrier, 1 + one_if(has["zl"]))
        signal(pair_sem, (gx, gz + 1))

        @pl.when(has["zl"])
        def _():
            signal(pair_sem, (gx, gz - 1))

    @pl.when(odd)
    def _():
        pl.semaphore_wait(pair_sem, 1 + one_if(has["zh"]))

    pz_copies = [
        ("zh", described("zh", plas_in, PZH.at[0], 0, 0)),
        ("zl", described("zl", plas_in, PZH.at[1], 0, 0)),
    ]
    start(pz_copies)
    for copy in rest_loads:
        copy.start()
    weak_load.start()

    places_a = lax.broadcasted_iota(jnp.int32, (ny, ny), 0)
    places_b = lax.broadcasted_iota(jnp.int32, (ny, ny), 1)
    gap = (places_a - places_b).astype(jnp.float32)
    YM[...] = jnp.where(
        jnp.abs(gap) <= float(REACH), jnp.exp(-gap * gap / 18.0) / weight_total, 0.0
    )
    zero_unless("zl", PZH.at[0])
    zero_unless("zh", PZH.at[1])
    zero_unless("xl", V.at[:, pl.ds(0, 1)], GXH.at[0], XH.at[0], XHL.at[0], RF.at[:, pl.ds(0, 1)])
    zero_unless("xh", V.at[:, pl.ds(rows + 1, 1)], GXH.at[1], XH.at[1], XHL.at[1])
    zero_unless("xh", RF.at[:, pl.ds(rows + 1, 1)])
    zero_unless("zl", VZH.at[0], ZH.at[0], ZHL.at[0], RZF.at[0])
    zero_unless("zh", VZH.at[1], ZH.at[1], ZHL.at[1], RZF.at[1])
    for number, (a, b) in enumerate(corners):
        zero_unless(a + b, CH.at[number])
    for it in range(ITERS):
        zero(SX.at[it, :, pl.ds(0, 1)])
        zero(SX.at[it, :, pl.ds(rows + 1, 1)])

    vel_load.wait()
    @pl.when(odd)
    def _():
        greeters = 2 * (one_if(has["xl"]) + one_if(has["xh"]))
        for _, _, there in met:
            greeters = greeters + one_if(there)
        pl.semaphore_wait(barrier, greeters)
        signal(pair_sem, (gx, gz - 1))

    @pl.when(even)
    def _():
        pl.semaphore_wait(pair_sem, 1)

    vel_copies = [
        ("xh", described("xh", V.at[:, pl.ds(rows, 1)], V.at[:, pl.ds(0, 1)], 2, 2)),
        ("xl", described("xl", V.at[:, pl.ds(1, 1)], V.at[:, pl.ds(rows + 1, 1)], 2, 2)),
    ]
    start_far(vel_copies)

    @pl.when(jnp.logical_not(has_far))
    def _():
        start_near(vel_copies)


    def hop_send(k):
        if k < len(rounds):

            @pl.when(odd)
            def _():
                for x_place, z_place, there in rounds[k]:

                    @pl.when(there)
                    def _(x_place=x_place, z_place=z_place):
                        signal(hop_sem.at[k], (x_place, z_place))

    def hop_wait(k):
        if k < len(rounds):

            @pl.when(odd)
            def _():
                expected = 0
                for _, _, there in rounds[k]:
                    expected = expected + one_if(there)
                pl.semaphore_wait(hop_sem.at[k], expected)

    hop_send(0)

    block = rows // 2
    many = (block, nz, ny)

    def over_rows(body, carry=0):
        return lax.fori_loop(0, rows // block, lambda i, state: body(i * block, state), carry)

    def at(x):
        return pl.ds(x, block)

    def vel_edges(x, carry):
        for c in range(3):
            row = V[c, at(x + 1)]
            VZE[0, c, at(x)] = row[:, 0:1]
            VZE[1, c, at(x)] = row[:, nz - 1 : nz]
        return carry

    over_rows(vel_edges)
    plas_load.wait()
    wait_got(pz_copies)
    vz_copies = [
        ("zh", described("zh", VZE.at[1], VZH.at[0], 1, 1)),
        ("zl", described("zl", VZE.at[0], VZH.at[1], 1, 1)),
    ]
    start(vz_copies)

    def smooth_z(x, carry):
        own, low, high = PLZ[at(x)], PZH[0, at(x)], PZH[1, at(x)]
        sub = lax.broadcasted_iota(jnp.int32, many, 1)
        sum_ = gauss_weights[REACH] * own
        for k in range(1, REACH + 1):
            above = pltpu.roll(jnp.where(sub >= k, own, high), nz - k, 1)
            below = pltpu.roll(jnp.where(sub < nz - k, own, low), k, 1)
            sum_ = sum_ + gauss_weights[REACH + k] * (above + below)
        SM[at(x)] = sum_
        return carry

    over_rows(smooth_z)
    GX[...] = jnp.dot(
        SM[...].reshape(rows * nz, ny),
        YM[...],
        precision=lax.Precision.HIGHEST,
        preferred_element_type=jnp.float32,
    ).reshape(rows, nz, ny)
    plas_copies = [
        ("xh", described("xh", GX.at[pl.ds(rows - REACH, REACH)], GXH.at[0], 3, 3)),
        ("xl", described("xl", GX.at[pl.ds(0, REACH)], GXH.at[1], 3, 3)),
    ]
    start_far(plas_copies)

    @pl.when(has_far)
    def _():
        start_near(vel_copies)

    start_near(plas_copies)
    hop_wait(0)
    hop_send(1)

    all_rest.wait()
    weak_load.wait()

    def prepare(x, carry):
        eta = VI[at(x)]
        eta = shear_time_increment * eta / (eta + shear_time_increment)
        ETA[at(x)] = eta
        INV[at(x)] = 1.0 / (eta + 0.5)
        COH[at(x)] = 0.8660254 - (0.8660254 * 0.6) * WK[at(x)].astype(jnp.float32)
        return carry

    over_rows(prepare)
    for row in range(rows):
        sum_ = gauss_weights[REACH] * GX[row]
        for k in range(1, REACH + 1):
            for other in (row - k, row + k):
                if 0 <= other < rows:
                    sum_ = sum_ + gauss_weights[REACH + k] * GX[other]
        SM[row] = sum_
    for k in range(1, len(rounds) - 1):
        hop_wait(k)
        hop_send(k + 1)

    wait_got(vz_copies)

    def dy(f):
        lane = lax.broadcasted_iota(jnp.int32, f.shape, 2)
        up = jnp.where(lane < ny - 1, pltpu.roll(f, ny - 1, 2), 0.0)
        down = jnp.where(lane > 0, pltpu.roll(f, 1, 2), 0.0)
        return (up - down) * 0.5

    def dz(f, low, high):
        sub = lax.broadcasted_iota(jnp.int32, f.shape, 1)
        up = pltpu.roll(jnp.where(sub >= 1, f, jnp.broadcast_to(high, f.shape)), nz - 1, 1)
        down = pltpu.roll(jnp.where(sub < nz - 1, f, jnp.broadcast_to(low, f.shape)), 1, 1)
        return (up - down) * 0.5

    def dz_inside(f):
        sub = lax.broadcasted_iota(jnp.int32, f.shape, 1)
        up = jnp.where(sub < nz - 1, pltpu.roll(f, nz - 1, 1), 0.0)
        down = jnp.where(sub >= 1, pltpu.roll(f, 1, 1), 0.0)
        return (up - down) * 0.5

    def strains(field, halo, x, size):
        v = [field[c, pl.ds(x + 1, size)] for c in range(3)]
        dx_v = [(field[c, pl.ds(x + 2, size)] - field[c, pl.ds(x, size)]) * 0.5 for c in range(3)]
        dz_v = [dz(f, halo[0, c, pl.ds(x, size)], halo[1, c, pl.ds(x, size)]) for c, f in enumerate(v)]
        dy_v = [dy(f) for f in v]
        div = dx_v[0] + dz_v[1] + dy_v[2]
        third = div * (1.0 / 3.0)
        return (
            dx_v[0] - third,
            dz_v[1] - third,
            dy_v[2] - third,
            0.5 * (dx_v[1] + dz_v[0]),
            0.5 * (dx_v[2] + dy_v[0]),
            0.5 * (dz_v[2] + dy_v[1]),
        ), div

    def second_invariant(trial):
        return jnp.sqrt(
            0.5 * (trial[0] * trial[0] + trial[1] * trial[1] + trial[2] * trial[2])
            + trial[3] * trial[3]
            + trial[4] * trial[4]
            + trial[5] * trial[5]
        )

    def first_trial(x):
        strain, div = strains(V, VZH, x, block)
        quarter = 0.25 * div
        pres = PIN[at(x)] - quarter
        PR[at(x)] = pres
        PIN[at(x)] = pres - quarter
        twice = 2.0 * ETA[at(x)]
        trial = [
            twice * (strain[c] + IN[2 + c, at(x)] * (0.5 / shear_time_increment)) for c in range(6)
        ]
        for c in range(6):
            TAU[c, at(x)] = trial[c]
        TB[at(x)] = second_invariant(trial)

    def in_order(act):
        for place, numbers in ((gx_odd, (1, 0)), (gx_even, (0, 1))):

            @pl.when(place)
            def _(numbers=numbers):
                for number in numbers:
                    act(number, number == numbers[0])

    def one_trial(number, far):
        wait_got(vel_copies[number : number + 1])
        first_trial(number * block)

    in_order(one_trial)
    half = ny // 2 if ny % 256 == 0 else ny

    def stress_rows(it, x, size, pres, trial, tau_ii, strength, plas, edge):
        def at(x):
            return pl.ds(x, size)

        last = it == ITERS - 1
        eta, inv = ETA[at(x)], INV[at(x)]
        yield_f = tau_ii - 0.5 * jnp.maximum(pres, 0.0) - strength
        dlam = jnp.maximum(yield_f, 0.0) * inv
        shrink = 1.0 - eta * dlam / jnp.maximum(tau_ii, 0.5)
        tau = [shrink * value for value in trial]
        PL[at(x)] = plas + dlam
        if last:
            for c in range(6):
                TAU[c, at(x)] = tau[c]
        SX[it, 0, at(x + 1)] = tau[0] - pres
        SX[it, 1, at(x + 1)] = tau[3]
        SX[it, 2, at(x + 1)] = tau[4]
        szz = tau[1] - pres
        TZ[0, at(x)] = szz
        TZ[1, at(x)] = tau[5]
        TZ[2, at(x)] = tau[2] - pres
        for c, f in enumerate((tau[3], szz, tau[5])):
            edge[0, c, at(x)] = f[:, 0:1]
            edge[1, c, at(x)] = f[:, nz - 1 : nz]
        return jnp.max(yield_f, axis=0), jnp.max(eta * shrink, axis=0)

    def forces(it, x, size, diff_z):
        s = [SX[it, c, pl.ds(x + 1, size)] for c in range(3)]
        t = [TZ[c, pl.ds(x, size)] for c in range(3)]
        along_x = [0.5 * (SX[it, c, pl.ds(x + 2, size)] - SX[it, c, pl.ds(x, size)]) for c in range(3)]
        along_z = [diff_z(c, f) for c, f in enumerate((s[1], t[0], t[1]))]
        along_y = [dy(f) for f in (s[2], t[1], t[2])]
        return [along_x[c] + along_z[c] + along_y[c] for c in range(3)]

    def folded(most):
        return jnp.maximum(most[:, :half], most[:, ny - half :])

    def tell(it, place):
        pltpu.make_async_remote_copy(
            src_ref=PK.at[it, me],
            dst_ref=PK.at[it, me],
            send_sem=pk_send,
            recv_sem=pk_recv.at[it],
            device_id=place,
            device_id_type=MESH,
        ).start()

    turned = {bit: flipped(gx, bit) - gx for bit in bits_of(gx_count)}

    def tell_all(it):
        parts = 3 if it else 2
        most_f, most_eta = [
            folded(functools.reduce(jnp.maximum, [MOST[i, k] for i in range(parts)])) for k in range(2)
        ]
        lane = lax.broadcasted_iota(jnp.int32, (nz, half), 1)
        most_f = jnp.maximum(most_f, pltpu.roll(most_f, half // 2, 1))
        most_eta = jnp.maximum(most_eta, pltpu.roll(most_eta, half // 2, 1))
        PK[it, me] = jnp.max(jnp.where(lane < half // 2, most_f, most_eta), axis=0, keepdims=True)
        if gx_count <= 16 and gz_count <= 2:
            for flips in reversed(range(1, total)):
                x_place, z_place = gx, gz
                for bit in bits_of(gx_count):
                    if flips // gz_count & bit:
                        x_place = x_place + turned[bit]
                if flips % gz_count:
                    z_place = flipped(gz, 1)
                tell(it, (x_place, z_place))
        else:
            for dz_ in range(gz_count):
                other_z = gz + dz_
                other_z = jnp.where(other_z >= gz_count, other_z - gz_count, other_z)

                def one(dx_, carry, other_z=other_z):
                    other_x = gx + dx_
                    tell(it, (jnp.where(other_x >= gx_count, other_x - gx_count, other_x), other_z))
                    return carry

                lax.fori_loop(0 if dz_ else 1, gx_count, one, 0)

    def told(it):
        others = PK.at[it, pl.ds(0, total - 1)]
        pltpu.make_async_copy(others, others, pk_recv.at[it]).wait()
        PEAKS[it] = jnp.max(PK[it], axis=0)

    def tell_sent():
        others = PK.at[0, pl.ds(0, total - 1)]
        pltpu.make_async_copy(others, others, pk_send).wait()

    def first_stress(x):
        strength = COH[at(x)] / (1.0 + 2.0 * SM[at(x)])
        COH[at(x)] = strength
        trial = [TAU[c, at(x)] for c in range(6)]
        return stress_rows(0, x, block, PR[at(x)], trial, TB[at(x)], strength, PLZ[at(x)], SE)

    x_copies = [
        ("xh", described("xh", XS.at[1], XH.at[0], 4, 2)),
        ("xl", described("xl", XS.at[0], XH.at[1], 4, 2)),
    ]
    corner_copies = []
    for number, (a, b) in enumerate(corners):
        there = corners.index((opposite[a], opposite[b]))
        corner_copies.append(
            (
                a + b,
                pltpu.make_async_remote_copy(
                    src_ref=CE.at[number],
                    dst_ref=CH.at[there],
                    send_sem=send_sem.at[corner_sent[number]],
                    recv_sem=recv_sem.at[slot(5) + (number if z_sides == 2 else number // 2)],
                    device_id=target[a + b],
                    device_id_type=MESH,
                ),
            )
        )

    def one_edge(number, far):
        row = (rows - 1) * number
        force = forces(0, row, 1, lambda c, f: dz_inside(f))
        for c in range(3):
            XS[number, c] = SX[0, c, row + 1]
            XS[number, 3 + c] = force[c][0]
        for layer in range(2):
            where = 2 * number + layer
            place = (nz - 1) * layer
            for c in range(3):
                CE[where, c] = SX[0, c, row + 1, place : place + 1]
                CE[where, 3 + c] = SE[layer, c, row]
        if far:
            wait_sent(vel_copies)
        start(x_copies[1 - number : 2 - number])

    def one_side(number, far):
        wait_got(plas_copies[number : number + 1])
        for beside in range(min(REACH, block)):
            here = beside if number == 0 else rows - 1 - beside
            sum_ = SM[here]
            for k in range(beside + 1, REACH + 1):
                place = REACH + beside - k if number == 0 else k - 1 - beside
                sum_ = sum_ + gauss_weights[REACH + k] * GXH[number, place]
            SM[here] = sum_
        MOST[number, 0], MOST[number, 1] = first_stress(number * block)
        if far:
            one_edge(number, far)
        if far:
            if len(rounds) > 1:
                hop_wait(len(rounds) - 1)

            @pl.when(odd)
            def _():
                signal(pair_sem, (gx, gz - 1))

    in_order(one_side)
    @pl.when(even)
    def _():
        pl.semaphore_wait(pair_sem, 1)

    tell_all(0)
    for place, number in ((gx_odd, 0), (gx_even, 1)):

        @pl.when(place)
        def _(number=number):
            one_edge(number, False)

    wait_sent(vz_copies)
    wait_sent(plas_copies)
    start(corner_copies)

    def own_force(x, carry):
        force = forces(0, x, block, lambda c, f: dz_inside(f))
        for c in range(3):
            RF[c, at(x + 1)] = force[c]
            SE[0, 3 + c, at(x)] = force[c][:, 0:1]
            SE[1, 3 + c, at(x)] = force[c][:, nz - 1 : nz]
        return carry

    over_rows(own_force)
    wait_sent(pz_copies)
    z_copies = [
        ("zh", described("zh", SE.at[1], ZH.at[0], 0, 0)),
        ("zl", described("zl", SE.at[0], ZH.at[1], 0, 0)),
    ]
    start(z_copies)
    wait_got(z_copies)

    def add_z(x, carry):
        sub = lax.broadcasted_iota(jnp.int32, many, 1)
        for c in range(3):
            high = jnp.where(sub == nz - 1, jnp.broadcast_to(ZH[1, c, at(x)], many), 0.0)
            low = jnp.where(sub == 0, jnp.broadcast_to(ZH[0, c, at(x)], many), 0.0)
            RF[c, at(x + 1)] = RF[c, at(x + 1)] + 0.5 * (high - low)
        return carry

    def second_trial(x, size):
        strain, div = strains(RF, RZF, x, size)
        twice = 2.0 * ETA[pl.ds(x, size)]
        for c in range(6):
            TR[c, pl.ds(x, size)] = twice * strain[c]
        DV[pl.ds(x, size)] = 0.25 * div

    over_rows(add_z)

    @pl.when(has["zl"])
    def _():
        RZF[0] = ZH[0, 3:6] + 0.5 * SE[0, 0:3]

    @pl.when(has["zh"])
    def _():
        RZF[1] = ZH[1, 3:6] - 0.5 * SE[1, 0:3]

    inside = rows - 4
    if inside > 0:
        size = next(size for size in (6, 4, 3, 2, 1) if inside % size == 0)

        def inside_trial(i, carry):
            second_trial(2 + i * size, size)
            return carry

        lax.fori_loop(0, inside // size, inside_trial, 0)

    def first_step():
        told(0)
        return step_of(PEAKS[0])

    def second_stress(step, x, size):
        here = pl.ds(x, size)
        pres = PIN[here] - step * DV[here]
        PR[here] = pres
        trial = [TAU[c, here] + step * TR[c, here] for c in range(6)]
        return stress_rows(
            1, x, size, pres, trial, second_invariant(trial), COH[here], PL[here], SEL
        )

    lowest = jnp.full((nz, ny), -jnp.inf, jnp.float32)

    def inside_rows(step):
        most = (lowest, lowest)
        if inside > 0:

            def inside_stress(i, most):
                f, eta = second_stress(step, 2 + i * size, size)
                return jnp.maximum(most[0], f), jnp.maximum(most[1], eta)

            if inside // size <= 2:
                for i in range(inside // size):
                    most = inside_stress(i, most)
            else:
                most = lax.fori_loop(0, inside // size, inside_stress, most)
        MOST[2, 0], MOST[2, 1] = most

    def end_trials():
        wait_got(x_copies)
        wait_got(corner_copies)
        for number, side, row in ((0, "xl", 0), (1, "xh", rows - 1)):
            sign = 0.5 - number
            beyond = row + 2 * number
            for c in range(3):
                RF[c, row + 1] = RF[c, row + 1] - sign * XH[number, c]

            @pl.when(has[side])
            def _(number=number, sign=sign, row=row, beyond=beyond):
                sub = lax.broadcasted_iota(jnp.int32, (nz, ny), 0)
                for c in range(3):
                    low = jnp.where(sub == 0, jnp.broadcast_to(CH[2 * number, 3 + c], (nz, ny)), 0.0)
                    high = jnp.where(sub == nz - 1, jnp.broadcast_to(CH[2 * number + 1, 3 + c], (nz, ny)), 0.0)
                    RF[c, beyond] = XH[number, 3 + c] + sign * SX[0, c, row + 1] + 0.5 * (high - low)

            for layer in range(2):
                for c in range(3):
                    RZF[layer, c, row] = RZF[layer, c, row] - sign * CH[2 * number + layer, c]
        if inside > 0:
            second_trial(0, 2)
            second_trial(rows - 2, 2)
        else:
            second_trial(0, rows)

    def end_rows(step):
        for i, x in enumerate((0, rows - 2) if inside > 0 else (0,)):
            MOST[i, 0], MOST[i, 1] = second_stress(step, x, 2 if inside > 0 else rows)
        if inside <= 0:
            MOST[1, 0], MOST[1, 1] = lowest, lowest

    @pl.when(gx >= gx_count // 2)
    def _():
        step = first_step()
        inside_rows(step)
        end_trials()
        end_rows(step)

    @pl.when(gx < gx_count // 2)
    def _():
        end_trials()
        step = first_step()
        inside_rows(step)
        end_rows(step)

    tell_sent()
    step = step_of(PEAKS[0])
    tell_all(1)
    wait_sent(corner_copies)
    sx_copies = [
        ("xh", described("xh", SX.at[1, :, pl.ds(rows, 1)], XHL.at[0], 2, 3)),
        ("xl", described("xl", SX.at[1, :, pl.ds(1, 1)], XHL.at[1], 2, 3)),
    ]
    start(sx_copies[1:])
    sz_copies = [
        ("zh", described("zh", SEL.at[1], ZHL.at[0], 1, 1)),
        ("zl", described("zl", SEL.at[0], ZHL.at[1], 1, 1)),
    ]
    start(sz_copies)

    def moved(x, carry):
        for c in range(3):
            MOVED[c, at(x)] = V[c, at(x + 1)] + step * RF[c, at(x + 1)]
        return carry

    over_rows(moved)
    wait_got(sz_copies)
    start(sx_copies[:1])

    def last_force(x, carry):
        def diff_z(c, f):
            return dz(f, ZHL[0, c, at(x)], ZHL[1, c, at(x)])

        force = forces(1, x, block, diff_z)
        for c in range(3):
            FORCE[c, at(x)] = force[c]
        return carry

    over_rows(last_force)
    wait_got(sx_copies)
    for c in range(3):
        FORCE[c, 0] = FORCE[c, 0] - 0.5 * XHL[0, c, 0]
        FORCE[c, rows - 1] = FORCE[c, rows - 1] + 0.5 * XHL[1, c, 0]
    told(1)
    wait_sent(x_copies + z_copies + sx_copies + sz_copies)
    tell_sent()


def store_kernel(moved, pres, tau, plas, force, peaks, v_out, p_out, t_out, l_out, top_out, V, TOP, sem):
    copies = [
        pltpu.make_async_copy(source, place, sem.at[i])
        for i, (source, place) in enumerate(
            ((tau, t_out), (pres, p_out), (plas, l_out), (V, v_out), (TOP, top_out))
        )
    ]
    for copy in copies[:3]:
        copy.start()
    step = step_of(peaks[ITERS - 1])
    for c in range(3):
        V[c] = moved[c] + step * force[c]
    copies[3].start()
    tops = [top_of(peaks[it]) for it in range(ITERS)]
    TOP[...] = jnp.concatenate(tops, axis=1)[0]
    copies[4].start()
    for copy in copies:
        copy.wait()


def solution(mesh):
    gx_count, gz_count = mesh.shape["gx"], mesh.shape["gz"]
    total = gx_count * gz_count

    def per_device(velocity, pressure, stress_old, plastic, viscosity, weak_seed):
        rows, nz, ny = pressure.shape
        cells = (rows, nz, ny)
        f32 = jnp.float32
        vm = lambda *shape: pltpu.VMEM(shape, f32)
        hops = len(bits_of(gx_count)) + len(bits_of(gz_count // 2))
        anywhere = pl.BlockSpec(memory_space=pl.ANY)
        within = pl.BlockSpec(memory_space=pltpu.VMEM)
        half = ny // 2 if ny % 256 == 0 else ny
        shapes = (velocity.shape, pressure.shape, stress_old.shape, plastic.shape)
        inner = (velocity.shape, (ITERS, 1, half))
        held = pl.pallas_call(
            functools.partial(kernel, gx_count, gz_count),
            out_shape=tuple(vm(*shape) for shape in shapes + inner),
            in_specs=[anywhere] * 6,
            out_specs=(within,) * 6,
            scratch_shapes=[
                vm(3, rows + 2, nz, ny),
                vm(8, *cells),
                pltpu.VMEM(cells, jnp.int32),
                vm(*cells),
                vm(2, *cells),
                vm(*cells),
                vm(*cells),
                vm(*cells),
                vm(ny, ny),
                vm(*cells),
                vm(2, REACH, nz, ny),
                vm(*cells),
                vm(2, 3, rows, 1, ny),
                vm(2, 3, rows, 1, ny),
                vm(ITERS, 3, rows + 2, nz, ny),
                vm(3, *cells),
                vm(2, 6, rows, 1, ny),
                vm(2, 6, rows, 1, ny),
                vm(2, 6, nz, ny),
                vm(2, 6, nz, ny),
                vm(4, 6, 1, ny),
                vm(4, 6, 1, ny),
                vm(2, 3, rows, 1, ny),
                vm(2, 3, rows, 1, ny),
                vm(2, 3, 1, nz, ny),
                vm(3, rows + 2, nz, ny),
                vm(2, 3, rows, 1, ny),
                vm(6, *cells),
                vm(*cells),
                vm(*cells),
                vm(3, 2, nz, ny),
                vm(ITERS, total, 1, half),
                pltpu.SemaphoreType.DMA,
                pltpu.SemaphoreType.DMA((sems_of(sides_of(gz_count))[0],)),
                pltpu.SemaphoreType.DMA((sems_of(sides_of(gz_count))[1],)),
                pltpu.SemaphoreType.DMA,
                pltpu.SemaphoreType.DMA((ITERS,)),
                pltpu.SemaphoreType.REGULAR,
                pltpu.SemaphoreType.REGULAR((hops,)),
            ],
            compiler_params=pltpu.CompilerParams(
                collective_id=0,
                has_side_effects=True,
            ),
        )(velocity, pressure, stress_old, plastic, viscosity, weak_seed)
        held = [pltpu.with_memory_space_constraint(array, pltpu.VMEM) for array in held]
        return pl.pallas_call(
            store_kernel,
            out_shape=tuple(jax.ShapeDtypeStruct(shape, f32) for shape in shapes)
            + (jax.ShapeDtypeStruct((ITERS,), f32),),
            in_specs=[within, anywhere, anywhere, anywhere, within, within],
            out_specs=(anywhere,) * 5,
            scratch_shapes=[vm(*velocity.shape), vm(ITERS), pltpu.SemaphoreType.DMA((5,))],
        )(*held)

    in_specs = (
        P(None, "gx", "gz", None),
        P("gx", "gz", None),
        P(None, "gx", "gz", None),
        P("gx", "gz", None),
        P("gx", "gz", None),
        P("gx", "gz", None),
    )
    out_specs = (
        P(None, "gx", "gz", None),
        P("gx", "gz", None),
        P(None, "gx", "gz", None),
        P("gx", "gz", None),
        P(),
    )
    return jax.shard_map(
        per_device, mesh=mesh, in_specs=in_specs, out_specs=out_specs, check_vma=False
    )
```
